128 devices in a mesh: dp: 128 (over x, z, y, core).
Axes of the slice: x: 4, y: 4, z: 4, core: 2. Of those that a mesh axis runs over, the one named last changes fastest.
Arguments:
- query_features: bfloat16 [32768, 768], P('dp'), may hold values from -24 to 24
- passage_features: bfloat16 [32768, 768], P('dp'), may hold values from -24 to 24
- counts: int32 [128], replicated, may hold values from 128 to 256, as said below
- positives: int32 [32768], P('dp'), may hold values from 0 to 17407
- w_first: bfloat16 [768, 1536], replicated, may hold values from -0.21875 to 0.21875
- w_second: bfloat16 [1536, 384], replicated, may hold values from -0.15625 to 0.15625
Outputs:
- mean_loss: float32 [], replicated
- grad_first: float32 [768, 1536], P(None, 'dp')
- grad_second: float32 [1536, 384], P('dp')
The draws below stay inside these ranges and needn't reach their ends.
Inputs may be any that keep to these rules, and one draw needn't show every extreme that they name: Device i holds counts[i] pairs in the first slots of its 256 slots. Each entry is 128 or 256; among the 16 devices whose indices agree modulo 128 // 16 exactly one entry is 256, so the entries sum to 17408. `positives`: only entries of occupied slots are used; an entry is the index of a passage in the order of occupied slots, device by device.
All inputs are finite; a program needn't handle non-finite values.
Results may differ from the reference program's by a relative error of at most 0.0043.
The reference program's roundings to bfloat16 on the way count: a program that leaves them out, or rounds other values in their place, can miss the bound.
Values may be sent and summed in bfloat16 or wider, within the bound.
No kernel may reach another device: no remote copies, remote signals or barrier semaphores. Data moves between devices by JAX's collectives and lax.ppermute only.
A program may use at most 128 MiB of HBM per device.

```python
import jax
import jax.numpy as jnp
from jax import lax

D = 768
FF = 1536
E = 384
LOW = 128
BLOCK = 136
CAP = 256
PAIRS = 17408
N_DP = 128


def feature_pair(key):
    pass_key = jax.random.fold_in(key, 11)
    query_key = jax.random.fold_in(key, 12)
    shape = (N_DP * CAP, D)
    passages = jax.random.truncated_normal(pass_key, -4.0, 4.0, shape, jnp.float32)
    queries = jax.random.truncated_normal(query_key, -4.0, 4.0, shape, jnp.float32)
    return (queries, passages)


def draw_query_features(key, part):
    return feature_pair(key)[0].astype(jnp.bfloat16)


def draw_passage_features(key, part):
    return feature_pair(key)[1].astype(jnp.bfloat16)


def draw_counts(key, part):
    stride = N_DP // 16
    heavy_pos = jax.random.randint(key, (stride,), 0, 16)
    device_ids = jnp.arange(N_DP, dtype=jnp.int32)
    heavy = device_ids // stride == heavy_pos[device_ids % stride]
    return (LOW + LOW * heavy.astype(jnp.int32)).astype(jnp.int32)


def place_ends(values, rng, smallest, high):
    shape = values.shape
    index_at = [jax.random.randint(jax.random.fold_in(rng, axis), (), 0, shape[axis]) for axis in range(len(shape))]
    values = values.at[tuple(index_at)].set(smallest)
    longest = shape.index(max(shape))
    index_at[longest] = (index_at[longest] + 1) % shape[longest]
    return values.at[tuple(index_at)].set(high)


def normal_values(key, shape, spread, most, held_as=jnp.bfloat16):
    result = spread * jax.random.normal(key, shape, jnp.float32)
    return jnp.clip(result, min=-most, max=most).astype(held_as)


def setup_inputs(seed: int = 0) -> dict:
    keys = jax.random.split(jax.random.key(seed), 7)
    return {
        "query_features": draw_query_features(jax.random.fold_in(keys[6], 71), 0),
        "passage_features": draw_passage_features(jax.random.fold_in(keys[6], 71), 0),
        "counts": draw_counts(jax.random.fold_in(keys[6], 71), 0),
        "positives": place_ends(jax.random.randint(keys[3], (N_DP * CAP,), 0, PAIRS), jax.random.fold_in(keys[3], 1), 0, PAIRS - 1).astype(jnp.int32),
        "w_first": normal_values(keys[4], (D, FF), D ** -0.5, 0.21875),
        "w_second": normal_values(keys[5], (FF, E), FF ** -0.5, 0.15625),
    }


def gelu_tanh(values):
    return jax.nn.gelu(values, approximate=True)

def tower_pass(features, w_first, w_second):
    pre_act = jnp.dot(features, w_first, preferred_element_type=jnp.float32)
    hidden = gelu_tanh(pre_act).astype(jnp.bfloat16)
    embedded = jnp.dot(hidden, w_second, preferred_element_type=jnp.float32).astype(jnp.bfloat16)
    return (pre_act, hidden, embedded)

def weight_terms(features, pre_act, hidden, grads, w_second):
    grad_second = lax.dot_general(hidden, grads, (((0,), (0,)), ((), ())), preferred_element_type=jnp.float32)
    back_act = lax.dot_general(grads, w_second, (((1,), (1,)), ((), ())), preferred_element_type=jnp.float32)
    pull_back = jax.vjp(gelu_tanh, pre_act)[1]
    pre_grad = pull_back(back_act)[0].astype(jnp.bfloat16)
    grad_first = lax.dot_general(features, pre_grad, (((0,), (0,)), ((), ())), preferred_element_type=jnp.float32)
    return (grad_first, grad_second)

def reference(query_features, passage_features, counts, positives, w_first, w_second):
    slot_ids = jnp.arange(N_DP * CAP, dtype=jnp.int32)
    owner_dev = slot_ids // CAP
    row_in = slot_ids % CAP
    offsets = (jnp.cumsum(counts) - counts).astype(jnp.int32)
    occupied = row_in < counts[owner_dev]
    dest_row = jnp.where(occupied, offsets[owner_dev] + row_in, PAIRS).astype(jnp.int32)
    width = query_features.shape[1]
    queries_in = jnp.zeros((PAIRS, width), query_features.dtype).at[dest_row].set(query_features, mode='drop')
    passages_in = jnp.zeros((PAIRS, width), passage_features.dtype).at[dest_row].set(passage_features, mode='drop')
    positive_ids = jnp.zeros((PAIRS,), jnp.int32).at[dest_row].set(positives, mode='drop')
    pre_q, hidden_q, query_emb = tower_pass(queries_in, w_first, w_second)
    pre_p, hidden_p, passage_emb = tower_pass(passages_in, w_first, w_second)
    score_scale = 2.5 * E ** (-0.5)
    step_rows = BLOCK * 16
    step_count = PAIRS // step_rows
    columns = jnp.arange(PAIRS, dtype=jnp.int32)

    def one_step(grad_sum, step_index):
        query_rows = lax.dynamic_slice_in_dim(query_emb, step_index * step_rows, step_rows, 0)
        pos_rows = lax.dynamic_slice_in_dim(positive_ids, step_index * step_rows, step_rows, 0)
        scores = lax.dot_general(query_rows, passage_emb, (((1,), (1,)), ((), ())), preferred_element_type=jnp.float32) * score_scale
        row_top = lax.optimization_barrier(jnp.max(scores, axis=1))
        log_norm = row_top + jnp.log(lax.optimization_barrier(jnp.sum(jnp.exp(scores - row_top[:, None]), axis=1)))
        is_positive = pos_rows[:, None] == columns[None, :]
        pos_score = lax.optimization_barrier(jnp.sum(jnp.where(is_positive, scores, jnp.zeros_like(scores)), axis=1))
        weights = (jnp.exp(scores - log_norm[:, None]) - is_positive.astype(jnp.float32)).astype(jnp.bfloat16)
        query_grad = (score_scale * jnp.dot(weights, passage_emb, preferred_element_type=jnp.float32)).astype(jnp.bfloat16)
        grad_sum = grad_sum + lax.dot_general(weights, query_rows, (((0,), (0,)), ((), ())), preferred_element_type=jnp.float32)
        return (grad_sum, (query_grad, jnp.sum(log_norm - pos_score)))
    start_sum = jnp.zeros((PAIRS, query_emb.shape[1]), jnp.float32)
    grad_sum, (query_parts, loss_parts) = lax.scan(one_step, start_sum, jnp.arange(step_count, dtype=jnp.int32))
    query_grads = query_parts.reshape(PAIRS, query_emb.shape[1])
    passage_grads = (score_scale * grad_sum).astype(jnp.bfloat16)
    mean_loss = jnp.sum(loss_parts) / PAIRS
    first_q, second_q = weight_terms(queries_in, pre_q, hidden_q, query_grads, w_second)
    first_p, second_p = weight_terms(passages_in, pre_p, hidden_p, passage_grads, w_second)
    return (mean_loss, first_q + first_p, second_q + second_p)
```

```python
import functools

import jax
import jax.numpy as jnp
from jax import lax
from jax.experimental import pallas as pl
from jax.experimental.pallas import tpu as pltpu
from jax.sharding import Mesh
from jax.sharding import PartitionSpec as P

DP = ("dp_0", "dp_1", "dp_2", "dp_3")
PLANE = ("dp_0", "dp_1")
LINE = "dp_2"
CORE = "dp_3"
F32 = jnp.float32
BF16 = jnp.bfloat16

LOW = 128
UNIT = 8
BLOCK = LOW + UNIT
CHUNK = 144
TILE = 256
LOG2E = 1.4426950408889634


def gelu_tanh(values):
    return jax.nn.gelu(values, approximate=True)


def swap_core(x):
    return lax.ppermute(x, CORE, [(0, 1), (1, 0)])


def plane_exchange(x):
    return lax.all_to_all(x, PLANE, 0, 0, tiled=True)


def line_exchange(x):
    return lax.all_to_all(x, (LINE, CORE), 0, 0, tiled=True)


def chip_exchange(x):
    return lax.all_to_all(x, (*PLANE, LINE), 0, 0, tiled=True)


def place_of(pos, sc):
    over = pos - sc[17]
    slot = jnp.bitwise_and(lax.shift_right_logical(over, 3) + sc[16], 15)
    place = jnp.where(
        (over >= 0) & (over < LOW), 16 * LOW + slot * UNIT + jnp.bitwise_and(over, 7), -1
    )
    for s in range(16):
        at = pos - sc[s]
        place = jnp.where((at >= 0) & (at < LOW), at + s * LOW, place)
    return place


def nt_dot(a, b):
    return lax.dot_general(a, b, (((1,), (1,)), ((), ())), preferred_element_type=F32)


def row_tiles(base, tail):
    tiles = [(base, k * TILE, TILE) for k in range(base.shape[0] // TILE)]
    return tiles + [(tail, 0, tail.shape[0])]


def stats_kernel(sc, qb, qt, pb, pt, q_out, turned_out, place_out, stats_out, *, scale):
    blocks = qb.shape[0] // LOW
    codes = []
    spread = None
    for b in range(blocks):
        q_out[b * LOW : (b + 1) * LOW] = qb[b * LOW : (b + 1) * LOW]
        q_out[blocks * LOW + b * UNIT : blocks * LOW + (b + 1) * UNIT] = qt[
            2 * b * UNIT : (2 * b + 1) * UNIT
        ]
        code = qt[(2 * b + 1) * UNIT : (2 * b + 2) * UNIT, :LOW].astype(F32)
        codes.append(code[0:1] * 128.0 + code[1:2])
        part = code[2:3] * 128.0 + code[3:4]
        spread = part if spread is None else spread + part
    codes.append(spread[:, : blocks * UNIT])
    place_out[...] = place_of(jnp.concatenate(codes, axis=1).astype(jnp.int32), sc)
    rows = q_out.shape[0]
    pull = scale * LOG2E
    top = jnp.full((1, rows), -1e30, F32)
    total = jnp.zeros((1, rows), F32)
    found = jnp.zeros((1, rows), F32)
    at = 0
    for ref, first, size in row_tiles(pb, pt):
        tile = ref[first : first + size]
        turned_out[:, at : at + size] = tile.T
        s = nt_dot(tile, q_out[...])
        row = lax.broadcasted_iota(jnp.int32, s.shape, 0)
        found += jnp.sum(jnp.where(row == place_out[...] - at, s, 0.0), axis=0, keepdims=True)
        new_top = jnp.maximum(top, jnp.max(s, axis=0, keepdims=True))
        total = total * jnp.exp2((top - new_top) * pull) + jnp.sum(
            jnp.exp2(s * pull - new_top * pull), axis=0, keepdims=True
        )
        top = new_top
        at += size
    line = lax.broadcasted_iota(jnp.int32, (8, rows), 0)
    stats = jnp.where(line == 0, top, jnp.where(line == 1, total, jnp.where(line == 2, found, 0.0)))
    for b in range(blocks):
        stats_out[b * 8 : (b + 1) * 8] = stats


def grads_kernel(stats, q, pb, pt, turned, place, dp_out, dq_out, g_ref, *, scale):
    blocks = dq_out.shape[0] // CHUNK
    units = dp_out.shape[0] // CHUNK
    rows = q.shape[0]
    width = q.shape[1]
    pull = scale * LOG2E
    tops = [stats[b * 8 : b * 8 + 1] for b in range(blocks)]
    top = functools.reduce(jnp.maximum, tops)
    total = jnp.zeros((1, rows), F32)
    found = jnp.zeros((1, rows), F32)
    for b in range(blocks):
        total += stats[b * 8 + 1 : b * 8 + 2] * jnp.exp2((tops[b] - top) * pull)
        found += stats[b * 8 + 2 : b * 8 + 3]
    norm = top * scale + jnp.log(total)
    loss = jnp.sum(norm - found * scale, axis=1, keepdims=True)
    norm = norm * LOG2E
    loss_high = loss.astype(BF16).astype(F32)
    loss_mid = (loss - loss_high).astype(BF16).astype(F32)
    loss_low = loss - loss_high - loss_mid
    line = lax.broadcasted_iota(jnp.int32, (UNIT, width), 0)
    loss_tile = jnp.where(
        line == 0,
        loss_high,
        jnp.where(line == 1, loss_mid, jnp.where(line == 2, loss_low, 0.0)),
    ).astype(BF16)
    at = 0
    for ref, first, size in row_tiles(pb, pt):
        s = nt_dot(ref[first : first + size], q[...])
        row = lax.broadcasted_iota(jnp.int32, s.shape, 0)
        e = jnp.exp2(s * pull - norm)
        g_ref[at : at + size] = jnp.where(row == place[...] - at, e - 1.0, e).astype(BF16)
        at += size
    for k in range(units * LOW // TILE):
        dp = scale * jnp.dot(g_ref[k * TILE : (k + 1) * TILE], q[...], preferred_element_type=F32)
        dp = dp.astype(BF16)
        for half in range(TILE // LOW):
            to = (k * (TILE // LOW) + half) * CHUNK
            dp_out[to : to + LOW] = dp[half * LOW : (half + 1) * LOW]
    dp = scale * jnp.dot(g_ref[units * LOW :], q[...], preferred_element_type=F32)
    dp = dp.astype(BF16)
    for k in range(units):
        dp_out[k * CHUNK + LOW : k * CHUNK + BLOCK] = dp[k * UNIT : (k + 1) * UNIT]
        dp_out[k * CHUNK + BLOCK : (k + 1) * CHUNK] = loss_tile
    for k in range(blocks * LOW // TILE):
        dq = jnp.dot(
            turned[...], g_ref[:, k * TILE : (k + 1) * TILE], preferred_element_type=F32
        )
        dq = (scale * dq).T.astype(BF16)
        for half in range(TILE // LOW):
            to = (k * (TILE // LOW) + half) * CHUNK
            dq_out[to : to + LOW] = dq[half * LOW : (half + 1) * LOW]
    dq = jnp.dot(turned[...], g_ref[:, blocks * LOW :], preferred_element_type=F32)
    dq = (scale * dq).T.astype(BF16)
    for k in range(blocks):
        dq_out[k * CHUNK + LOW : k * CHUNK + BLOCK] = dq[k * UNIT : (k + 1) * UNIT]
        dq_out[k * CHUNK + BLOCK : (k + 1) * CHUNK] = jnp.zeros((CHUNK - BLOCK, width), BF16)


def weights_kernel(de_q, de_q_other, de_p, de_p_other, rows, hidden, slope, second, out, de):
    for k, part in enumerate((de_q, de_q_other, de_p, de_p_other)):
        de[k * BLOCK : (k + 1) * BLOCK] = part[...]
    many = out.shape[0]
    wide = rows.shape[1] + de.shape[1]
    for first in range(0, hidden.shape[0], TILE):
        span = slice(first, first + TILE)
        grad_second = jnp.dot(hidden[span], de[...], preferred_element_type=F32)
        back = nt_dot(second[span], de[...])
        dpre = (slope[span] * back).astype(BF16)
        grad_first = jnp.dot(dpre, rows[...], preferred_element_type=F32)
        if first < many:
            out[span, : rows.shape[1]] = grad_first.astype(BF16)
            out[span, rows.shape[1] : wide] = grad_second.astype(BF16)
        else:
            x = jnp.concatenate(
                [grad_first, grad_second, jnp.zeros((TILE, 128), F32)], axis=1
            )
            near, far = x[:, :640], x[:, 640:]
            line = jnp.bitwise_and(lax.broadcasted_iota(jnp.int32, near.shape, 0), 7)
            even = jnp.where(line < 4, near, pltpu.roll(far, 4, 0)).astype(BF16)
            odd = jnp.where(line < 4, pltpu.roll(near, TILE - 4, 0), far).astype(BF16)
            for b in range(TILE // 8):
                to = (first - many) * 2 + b * 16
                out[to : to + 8, wide:] = even[b * 8 : (b + 1) * 8]
                out[to + 8 : to + 16, wide:] = odd[b * 8 : (b + 1) * 8]


def score_stats(sc, qb, qt, pb, pt, scale):
    blocks = qb.shape[0] // LOW
    rows = blocks * BLOCK
    columns = pb.shape[0] + pt.shape[0]
    width = qb.shape[1]
    vmem = pl.BlockSpec(memory_space=pltpu.VMEM)
    return pl.pallas_call(
        functools.partial(stats_kernel, scale=scale),
        in_specs=[pl.BlockSpec(memory_space=pltpu.SMEM)] + [vmem] * 4,
        out_specs=[vmem] * 4,
        out_shape=[
            jax.ShapeDtypeStruct((rows, width), BF16),
            jax.ShapeDtypeStruct((width, columns), BF16),
            jax.ShapeDtypeStruct((1, rows), jnp.int32),
            jax.ShapeDtypeStruct((8 * blocks, rows), F32),
        ],
        name="score_stats",
    )(sc, qb, qt, pb, pt)


def score_grads(stats, q, pb, pt, turned, place, scale):
    rows, width = q.shape
    columns = pb.shape[0] + pt.shape[0]
    vmem = pl.BlockSpec(memory_space=pltpu.VMEM)
    return pl.pallas_call(
        functools.partial(grads_kernel, scale=scale),
        in_specs=[vmem] * 6,
        out_specs=[vmem] * 2,
        out_shape=[
            jax.ShapeDtypeStruct((columns // BLOCK * CHUNK, width), BF16),
            jax.ShapeDtypeStruct((rows // BLOCK * CHUNK, width), BF16),
        ],
        scratch_shapes=[pltpu.VMEM((columns, rows), BF16)],
        name="score_grads",
    )(stats, q, pb, pt, turned, place)


def weight_grads(de_parts, rows, hidden, slope, second):
    vmem = pl.BlockSpec(memory_space=pltpu.VMEM)
    return pl.pallas_call(
        weights_kernel,
        in_specs=[vmem] * 8,
        out_specs=vmem,
        out_shape=jax.ShapeDtypeStruct((512, 1792), BF16),
        scratch_shapes=[pltpu.VMEM((4 * BLOCK, second.shape[1]), BF16)],
        name="weight_grads",
    )(*de_parts, rows, hidden, slope, second)


def body(query_features, passage_features, counts, positives, w_first, w_second):
    width = query_features.shape[1]
    hidden_width, emb_width = w_second.shape
    scale = 2.5 * emb_width ** (-0.5)
    group = lax.axis_index((LINE, CORE))
    core = lax.axis_index(CORE)
    pairs = BLOCK * lax.axis_size(DP)

    heavy = (counts > LOW).astype(jnp.int32)
    offsets = jnp.cumsum(counts) - counts
    devices = jnp.arange(counts.shape[0], dtype=jnp.int32)
    mine = heavy * (devices % 8 == group)
    heavy_at = jnp.sum(mine * (devices // 8))
    over_start = jnp.sum(mine * offsets) + LOW
    group_start = lax.dynamic_slice_in_dim(offsets.reshape(16, 8), group, 1, 1)[:, 0]
    sc = jnp.concatenate([group_start, heavy_at[None], over_start[None]]).astype(jnp.int32)

    pos_high = jnp.right_shift(positives, 7).astype(BF16)
    pos_low = jnp.bitwise_and(positives, 127).astype(BF16)
    lane = jnp.arange(LOW, dtype=jnp.int32)
    line = jnp.arange(UNIT, dtype=jnp.int32)[None, :, None]
    at_group = (lane // UNIT == group)[None, None, :]
    spread_high = jnp.tile(pos_high[LOW:].reshape(16, 1, UNIT), (1, 1, 16))
    spread_low = jnp.tile(pos_low[LOW:].reshape(16, 1, UNIT), (1, 1, 16))
    coded = jnp.where(
        at_group & (line == 2),
        spread_high,
        jnp.where(at_group & (line == 3), spread_low, jnp.zeros((), BF16)),
    ).reshape(LOW, LOW)
    over = jnp.concatenate([query_features[LOW:], passage_features[LOW:], coded], axis=1)
    over = jnp.concatenate([over, over], axis=0)
    over = lax.dynamic_slice_in_dim(over, (16 - heavy_at) * UNIT, LOW, 0)
    arrived = plane_exchange(over)
    tail = lax.dynamic_slice_in_dim(arrived, heavy_at * UNIT, UNIT, 0)

    def tower(x):
        pre = jnp.dot(x, w_first, preferred_element_type=F32)
        hidden = gelu_tanh(pre).astype(BF16)
        return jnp.dot(hidden, w_second, preferred_element_type=F32).astype(BF16)

    base = tower(jnp.concatenate([query_features[:LOW], passage_features[:LOW]], axis=0))
    pb = plane_exchange(jnp.concatenate([base[LOW:]] * 16, axis=0))
    qb = line_exchange(jnp.concatenate([base[:LOW]] * 8, axis=0))

    tail_q, tail_p = tail[:, :width], tail[:, width : 2 * width]
    tail_emb = tower(jnp.concatenate([tail_q, tail_p], axis=0))
    line = line[0]
    codes = jnp.where(
        line == 0, pos_high[None, :LOW], jnp.where(line == 1, pos_low[None, :LOW], tail[:, 2 * width :])
    )
    codes = jnp.pad(codes, ((0, 0), (0, emb_width - LOW)))
    pt = plane_exchange(jnp.concatenate([tail_emb[UNIT:]] * 16, axis=0))
    qt = line_exchange(jnp.concatenate([tail_emb[:UNIT], codes] * 8, axis=0))

    q_all, turned, place, stats = score_stats(sc, qb, qt, pb, pt, scale)
    stats = line_exchange(stats)
    dp_part, dq_part = score_grads(stats, q_all, pb, pt, turned, place, scale)
    dp_sum = jnp.sum(plane_exchange(dp_part).reshape(16, CHUNK, emb_width).astype(F32), axis=0)
    dq_sum = jnp.sum(line_exchange(dq_part).reshape(8, CHUNK, emb_width).astype(F32), axis=0)
    mean_loss = (dp_sum[BLOCK, 0] + dp_sum[BLOCK + 1, 0] + dp_sum[BLOCK + 2, 0]) / pairs
    de_q = dq_sum[:BLOCK].astype(BF16)
    de_p = dp_sum[:BLOCK].astype(BF16)

    late_core, _ = lax.optimization_barrier((core, base))
    each = hidden_width // lax.axis_size(DP)
    half = hidden_width // 2
    unit = jnp.arange(half, dtype=jnp.int32)
    rest = unit - 512
    unit_of = jnp.where(
        unit < 512,
        (unit // 8) * (2 * each) + unit % 8,
        (rest // 4) * (2 * each) + 8 + rest % 4,
    )
    unit_of = unit_of + late_core * each
    pick = (unit_of[:, None] == jnp.arange(hidden_width, dtype=jnp.int32)[None, :]).astype(BF16)
    first_half = lax.dot_general(
        pick, w_first, (((1,), (1,)), ((), ())), preferred_element_type=F32
    ).astype(BF16)
    second_half = jnp.dot(pick, w_second, preferred_element_type=F32).astype(BF16)
    own = jnp.concatenate(
        [query_features[:LOW], tail_q, passage_features[:LOW], tail_p], axis=0
    )
    other = swap_core(own)
    rows = jnp.concatenate([own[:BLOCK], other[:BLOCK], own[BLOCK:], other[BLOCK:]], axis=0)
    pre_half = lax.dot_general(
        first_half, rows, (((1,), (1,)), ((), ())), preferred_element_type=F32
    )
    act, pull_back = jax.vjp(gelu_tanh, pre_half)
    hidden = act.astype(BF16)
    slope = pull_back(jnp.ones_like(pre_half))[0]

    grads = weight_grads(
        (de_q, swap_core(de_q), de_p, swap_core(de_p)), rows, hidden, slope, second_half
    )
    out = jnp.sum(chip_exchange(grads).reshape(64, 8, -1).astype(F32), axis=0)
    wide = width + emb_width
    tail_out = jnp.concatenate([out[:4, wide:], out[4:, wide : 2 * wide - 640]], axis=1)
    out = jnp.concatenate([out[:, :wide], tail_out], axis=0)
    return (mean_loss, out[:, :width].T, out[:, width:])


def solution(mesh):
    finer = Mesh(mesh.devices.reshape(4, 4, 4, 2), DP)
    placed = (P(DP, None), P(DP, None), P(), P(DP), P(), P())
    return jax.shard_map(
        body,
        mesh=finer,
        in_specs=placed,
        out_specs=(P(), P(None, DP), P(DP, None)),
        check_vma=False,
    )
```

```python
import functools

import jax
import jax.numpy as jnp
from jax import lax
from jax.experimental import pallas as pl
from jax.experimental.pallas import tpu as pltpu
from jax.sharding import Mesh
from jax.sharding import PartitionSpec as P

DP = ("dp_0", "dp_1", "dp_2", "dp_3")
PLANE = ("dp_0", "dp_1")
LINE = "dp_2"
CORE = "dp_3"
F32 = jnp.float32
BF16 = jnp.bfloat16

LOW = 128
UNIT = 8
BLOCK = LOW + UNIT
CHUNK = 144
PAIR = 2 * BLOCK
TILE = 256
LOG2E = 1.4426950408889634


def gelu_tanh(values):
    return jax.nn.gelu(values, approximate=True)


def swap_core(x):
    return lax.ppermute(x, CORE, [(0, 1), (1, 0)])


def plane_exchange(x):
    return lax.all_to_all(x, PLANE, 0, 0, tiled=True)


def stats_exchange(x):
    return lax.all_to_all(x, (LINE, CORE), 0, 0, tiled=True)


def from_line(x, k):
    return lax.ppermute(x, LINE, [((i + k) % 4, i) for i in range(4)])


def to_line(x, k):
    return lax.ppermute(x, LINE, [(i, (i + k) % 4) for i in range(4)])


def along_line(pair):
    return [pair] + [from_line(pair, k) for k in (1, 2, 3)]


def place_of(pos, sc):
    over = pos - sc[17]
    slot = jnp.bitwise_and(lax.shift_right_logical(over, 3) + sc[16], 15)
    place = jnp.where(
        (over >= 0) & (over < LOW), slot * BLOCK + LOW + jnp.bitwise_and(over, 7), -1
    )
    for s in range(16):
        at = pos - sc[s]
        place = jnp.where((at >= 0) & (at < LOW), at + s * BLOCK, place)
    return place


def near_index(sc, j):
    return jnp.bitwise_and(j // 2 - sc[18], 3) * 2 + jnp.bitwise_xor(j % 2, sc[19])


def nt_dot(a, b):
    return lax.dot_general(a, b, (((1,), (1,)), ((), ())), preferred_element_type=F32)


def stats_kernel(
    sc, q0, q1, q2, q3, t0, t1, t2, t3, p, q_out, turned_out, place_out, stats_out, qs, ts, *, scale
):
    width = p.shape[1]
    for k, ref in enumerate((q0, q1, q2, q3)):
        for b in range(2):
            qs[2 * k + b] = ref[b * LOW : (b + 1) * LOW]
    for k, ref in enumerate((t0, t1, t2, t3)):
        for b in range(2):
            ts[2 * k + b] = ref[b * 16 : (b + 1) * 16, :width]
    codes = []
    spread = None
    for j in range(8):
        b = near_index(sc, j)
        q_out[j * LOW : (j + 1) * LOW] = qs[b]
        tail = ts[b]
        q_out[8 * LOW + j * UNIT : 8 * LOW + (j + 1) * UNIT] = tail[:UNIT]
        code = tail[UNIT:, :LOW].astype(F32)
        codes.append(code[0:1] * 128.0 + code[1:2])
        part = code[2:3] * 128.0 + code[3:4]
        spread = part if spread is None else spread + part
    codes.append(spread[:, : 8 * UNIT])
    place_out[...] = place_of(jnp.concatenate(codes, axis=1).astype(jnp.int32), sc)
    rows = q_out.shape[0]
    pull = scale * LOG2E
    top = jnp.full((1, rows), -1e30, F32)
    total = jnp.zeros((1, rows), F32)
    found = jnp.zeros((1, rows), F32)
    for at in range(0, p.shape[0], PAIR):
        tile = p[at : at + PAIR]
        s = nt_dot(tile, q_out[...])
        row = lax.broadcasted_iota(jnp.int32, s.shape, 0)
        found += jnp.sum(jnp.where(row == place_out[...] - at, s, 0.0), axis=0, keepdims=True)
        new_top = jnp.maximum(top, jnp.max(s, axis=0, keepdims=True))
        total = total * jnp.exp2((top - new_top) * pull) + jnp.sum(
            jnp.exp2(s * pull - new_top * pull), axis=0, keepdims=True
        )
        top = new_top
    for at in range(0, p.shape[0], LOW):
        turned_out[:, at : at + LOW] = p[at : at + LOW].T
    line = lax.broadcasted_iota(jnp.int32, (8, rows), 0)
    stats = jnp.where(line == 0, top, jnp.where(line == 1, total, jnp.where(line == 2, found, 0.0)))
    for b in range(8):
        stats_out[b * 8 : (b + 1) * 8] = stats


def grads_kernel(sc, stats, q, p, turned, place, dp_out, dq_out, g_ref, *, scale):
    rows, width = q.shape
    pull = scale * LOG2E
    tops = [stats[b * 8 : b * 8 + 1] for b in range(8)]
    top = functools.reduce(jnp.maximum, tops)
    total = jnp.zeros((1, rows), F32)
    found = jnp.zeros((1, rows), F32)
    for b in range(8):
        total += stats[b * 8 + 1 : b * 8 + 2] * jnp.exp2((tops[b] - top) * pull)
        found += stats[b * 8 + 2 : b * 8 + 3]
    norm = top * scale + jnp.log(total)
    loss = jnp.sum(norm - found * scale, axis=1, keepdims=True)
    norm = norm * LOG2E
    loss_high = loss.astype(BF16).astype(F32)
    loss_mid = (loss - loss_high).astype(BF16).astype(F32)
    loss_low = loss - loss_high - loss_mid
    line = lax.broadcasted_iota(jnp.int32, (UNIT, width), 0)
    loss_tile = jnp.where(
        line == 0,
        loss_high,
        jnp.where(line == 1, loss_mid, jnp.where(line == 2, loss_low, 0.0)),
    ).astype(BF16)
    for at in range(0, p.shape[0], PAIR):
        s = nt_dot(p[at : at + PAIR], q[...])
        row = lax.broadcasted_iota(jnp.int32, s.shape, 0)
        e = jnp.exp2(s * pull - norm)
        g_ref[at : at + PAIR] = jnp.where(row == place[...] - at, e - 1.0, e).astype(BF16)
    for k in range(p.shape[0] // PAIR):
        dp = scale * jnp.dot(g_ref[k * PAIR : (k + 1) * PAIR], q[...], preferred_element_type=F32)
        dp = dp.astype(BF16)
        for half in range(2):
            to = (2 * k + half) * CHUNK
            dp_out[to : to + BLOCK] = dp[half * BLOCK : (half + 1) * BLOCK]
            dp_out[to + BLOCK : to + CHUNK] = loss_tile
    for k in range(4):
        dq = jnp.dot(
            turned[...], g_ref[:, k * TILE : (k + 1) * TILE], preferred_element_type=F32
        )
        dq = (scale * dq).T.astype(BF16)
        for half in range(2):
            dq_out[near_index(sc, 2 * k + half), :LOW] = dq[half * LOW : (half + 1) * LOW]
    dq = jnp.dot(turned[...], g_ref[:, 8 * LOW :], preferred_element_type=F32)
    dq = (scale * dq).T.astype(BF16)
    for j in range(8):
        dq_out[near_index(sc, j), LOW:BLOCK] = dq[j * UNIT : (j + 1) * UNIT]


def weights_kernel(q0, q1, q2, q3, p0, p1, p2, p3, rows, hidden, slope, second, out, de):
    for k, (dq, dp) in enumerate(zip((q0, q1, q2, q3), (p0, p1, p2, p3))):
        for b in range(2):
            to = (2 * k + b) * 2 * LOW
            de[to : to + LOW] = dq[b * BLOCK : b * BLOCK + LOW]
            de[to + LOW : to + 2 * LOW] = dp[b * BLOCK : b * BLOCK + LOW]
            to = 16 * LOW + (2 * k + b) * 2 * UNIT
            de[to : to + UNIT] = dq[b * BLOCK + LOW : (b + 1) * BLOCK]
            de[to + UNIT : to + 2 * UNIT] = dp[b * BLOCK + LOW : (b + 1) * BLOCK]
    many = out.shape[0]
    wide = rows.shape[1] + de.shape[1]
    grad_second = jnp.dot(hidden[...], de[...], preferred_element_type=F32)
    back = nt_dot(second[...], de[...])
    dpre = (slope[...] * back).astype(BF16)
    grad_first = jnp.dot(dpre, rows[...], preferred_element_type=F32)
    out[:, : rows.shape[1]] = grad_first[:many].astype(BF16)
    out[:, rows.shape[1] : wide] = grad_second[:many].astype(BF16)
    rest = grad_first.shape[0] - many
    x = jnp.concatenate(
        [grad_first[many:], grad_second[many:], jnp.zeros((rest, 128), F32)], axis=1
    )
    near, far = x[:, :640], x[:, 640:]
    line = jnp.bitwise_and(lax.broadcasted_iota(jnp.int32, near.shape, 0), 7)
    even = jnp.where(line < 4, near, pltpu.roll(far, 4, 0)).astype(BF16)
    odd = jnp.where(line < 4, pltpu.roll(near, rest - 4, 0), far).astype(BF16)
    for b in range(rest // 8):
        out[b * 16 : b * 16 + 8, wide:] = even[b * 8 : (b + 1) * 8]
        out[b * 16 + 8 : b * 16 + 16, wide:] = odd[b * 8 : (b + 1) * 8]


VMEM = pl.BlockSpec(memory_space=pltpu.VMEM)
SMEM = pl.BlockSpec(memory_space=pltpu.SMEM)


def score_stats(sc, qs, ts, p, scale):
    columns, width = p.shape
    rows = 8 * BLOCK
    return pl.pallas_call(
        functools.partial(stats_kernel, scale=scale),
        in_specs=[SMEM] + [VMEM] * 9,
        out_specs=[VMEM] * 4,
        out_shape=[
            jax.ShapeDtypeStruct((rows, width), BF16),
            jax.ShapeDtypeStruct((width, columns), BF16),
            jax.ShapeDtypeStruct((1, rows), jnp.int32),
            jax.ShapeDtypeStruct((64, rows), F32),
        ],
        scratch_shapes=[pltpu.VMEM((8, LOW, width), BF16), pltpu.VMEM((8, 16, width), BF16)],
        name="score_stats",
    )(sc, *qs, *ts, p)


def score_grads(sc, stats, q, p, turned, place, scale):
    columns, width = p.shape
    rows = q.shape[0]
    return pl.pallas_call(
        functools.partial(grads_kernel, scale=scale),
        in_specs=[SMEM] + [VMEM] * 5,
        out_specs=[VMEM] * 2,
        out_shape=[
            jax.ShapeDtypeStruct((columns // BLOCK * CHUNK, width), BF16),
            jax.ShapeDtypeStruct((8, BLOCK, width), BF16),
        ],
        scratch_shapes=[pltpu.VMEM((columns, rows), BF16)],
        name="score_grads",
    )(sc, stats, q, p, turned, place)


def weight_grads(dqs, dps, rows, hidden, slope, second):
    return pl.pallas_call(
        weights_kernel,
        in_specs=[VMEM] * 12,
        out_specs=VMEM,
        out_shape=jax.ShapeDtypeStruct((128, 1792), BF16),
        scratch_shapes=[pltpu.VMEM((16 * BLOCK, second.shape[1]), BF16)],
        name="weight_grads",
    )(*dqs, *dps, rows, hidden, slope, second)


def body(query_features, passage_features, counts, positives, w_first, w_second):
    width = query_features.shape[1]
    hidden_width, emb_width = w_second.shape
    scale = 2.5 * emb_width ** (-0.5)
    group = lax.axis_index((LINE, CORE))
    pairs = BLOCK * lax.axis_size(DP)

    heavy = (counts > LOW).astype(jnp.int32)
    offsets = jnp.cumsum(counts) - counts
    devices = jnp.arange(counts.shape[0], dtype=jnp.int32)
    mine = heavy * (devices % 8 == group)
    heavy_at = jnp.sum(mine * (devices // 8))
    over_start = jnp.sum(mine * offsets) + LOW
    group_start = lax.dynamic_slice_in_dim(offsets.reshape(16, 8), group, 1, 1)[:, 0]
    scalars = [heavy_at, over_start, lax.axis_index(LINE), lax.axis_index(CORE)]
    sc = jnp.concatenate([group_start, jnp.stack(scalars)]).astype(jnp.int32)

    pos_high = jnp.right_shift(positives, 7).astype(BF16)
    pos_low = jnp.bitwise_and(positives, 127).astype(BF16)
    lane = jnp.arange(LOW, dtype=jnp.int32)
    line = jnp.arange(UNIT, dtype=jnp.int32)[None, :, None]
    at_group = (lane // UNIT == group)[None, None, :]
    spread_high = jnp.tile(pos_high[LOW:].reshape(16, 1, UNIT), (1, 1, 16))
    spread_low = jnp.tile(pos_low[LOW:].reshape(16, 1, UNIT), (1, 1, 16))
    coded = jnp.where(
        at_group & (line == 2),
        spread_high,
        jnp.where(at_group & (line == 3), spread_low, jnp.zeros((), BF16)),
    ).reshape(LOW, LOW)
    over = jnp.concatenate([query_features[LOW:], passage_features[LOW:], coded], axis=1)
    over = jnp.concatenate([over, over], axis=0)
    over = lax.dynamic_slice_in_dim(over, (16 - heavy_at) * UNIT, LOW, 0)
    arrived = plane_exchange(over)
    tail = lax.dynamic_slice_in_dim(arrived, heavy_at * UNIT, UNIT, 0)

    def tower(x):
        pre = jnp.dot(x, w_first, preferred_element_type=F32)
        hidden = gelu_tanh(pre).astype(BF16)
        return jnp.dot(hidden, w_second, preferred_element_type=F32).astype(BF16)

    feats = jnp.concatenate([query_features[:LOW], passage_features[:LOW]], axis=0)
    base = tower(feats)
    q_base = base[:LOW]
    q_pair = jnp.concatenate([q_base, swap_core(q_base)], axis=0)

    feats_tail = jnp.concatenate([tail[:, :width], tail[:, width : 2 * width]], axis=0)
    tail_emb = tower(feats_tail)
    p_send = jnp.concatenate([base[LOW:], tail_emb[UNIT:]], axis=0)
    p_send, q_pair = lax.optimization_barrier((p_send, q_pair))
    qs = along_line(q_pair)
    p_send = jnp.broadcast_to(p_send[None], (16, BLOCK, emb_width))
    p_all = plane_exchange(p_send.reshape(16 * BLOCK, emb_width))

    line = line[0]
    codes = jnp.where(
        line == 0,
        pos_high[None, :LOW],
        jnp.where(line == 1, pos_low[None, :LOW], tail[:, 2 * width :]),
    )
    codes = jnp.pad(codes, ((0, 0), (0, emb_width - LOW)))
    pack = jnp.concatenate(
        [jnp.concatenate([tail_emb[:UNIT], codes], axis=0), feats_tail], axis=1
    )
    ts = along_line(jnp.concatenate([pack, swap_core(pack)], axis=0))

    feats_pair = jnp.concatenate([feats, swap_core(feats)], axis=0)
    feats_pair, _ = lax.optimization_barrier((feats_pair, (qs[1], ts[0])))
    rows = jnp.concatenate(along_line(feats_pair) + [t[:, emb_width:] for t in ts], axis=0)

    late_group, _ = lax.optimization_barrier((group, base))
    each = hidden_width // lax.axis_size(DP)
    unit = jnp.arange(16 * each, dtype=jnp.int32)
    rest = unit - LOW
    unit_of = jnp.where(
        unit < LOW, (unit // 8) * (8 * each) + unit % 8, (rest // 4) * (8 * each) + 8 + rest % 4
    )
    unit_of = unit_of + late_group * each
    pick = (unit_of[:, None] == jnp.arange(hidden_width, dtype=jnp.int32)[None, :]).astype(BF16)
    first_part = lax.dot_general(
        pick, w_first, (((1,), (1,)), ((), ())), preferred_element_type=F32
    ).astype(BF16)
    second_part = jnp.dot(pick, w_second, preferred_element_type=F32).astype(BF16)
    p_all, first_part, second_part = lax.optimization_barrier((p_all, first_part, second_part))

    q_all, turned, place, stats = score_stats(sc, qs, ts, p_all, scale)
    stats = stats_exchange(stats)
    dp_part, dq_part = score_grads(sc, stats, q_all, p_all, turned, place, scale)
    dp_all = plane_exchange(dp_part)

    dq_part = dq_part.reshape(4, 2 * BLOCK, emb_width)
    dq_pair = dq_part[0].astype(F32)
    for k in (1, 2, 3):
        dq_pair = dq_pair + to_line(dq_part[k], k).astype(F32)
    dq_far = swap_core(dq_pair)
    dq_far = jnp.concatenate([dq_far[BLOCK:], dq_far[:BLOCK]], axis=0)
    dqs = along_line((dq_pair + dq_far).astype(BF16))
    pre = lax.dot_general(first_part, rows, (((1,), (1,)), ((), ())), preferred_element_type=F32)
    act, pull_back = jax.vjp(gelu_tanh, pre)
    hidden = act.astype(BF16)
    slope = pull_back(jnp.ones_like(pre))[0]
    dp_all, dqs, hidden, slope = lax.optimization_barrier((dp_all, dqs, hidden, slope))

    dp_sum = jnp.sum(dp_all.reshape(16, CHUNK, emb_width).astype(F32), axis=0)
    mean_loss = (dp_sum[BLOCK, 0] + dp_sum[BLOCK + 1, 0] + dp_sum[BLOCK + 2, 0]) / pairs
    de_p = dp_sum[:BLOCK].astype(BF16)
    dps = along_line(jnp.concatenate([de_p, swap_core(de_p)], axis=0))
    grads = weight_grads(dqs, dps, rows, hidden, slope, second_part)
    out = jnp.sum(plane_exchange(grads).reshape(16, 8, -1).astype(F32), axis=0)
    wide = width + emb_width
    tail_out = jnp.concatenate([out[:4, wide:], out[4:, wide : 2 * wide - 640]], axis=1)
    out = jnp.concatenate([out[:, :wide], tail_out], axis=0)
    return (mean_loss, out[:, :width].T, out[:, width:])


def solution(mesh):
    finer = Mesh(mesh.devices.reshape(4, 4, 4, 2), DP)
    placed = (P(DP, None), P(DP, None), P(), P(DP), P(), P())
    return jax.shard_map(
        body,
        mesh=finer,
        in_specs=placed,
        out_specs=(P(), P(None, DP), P(DP, None)),
        check_vma=False,
    )
```

```python
import functools

import jax
import jax.numpy as jnp
from jax import lax
from jax.experimental import pallas as pl
from jax.experimental.pallas import tpu as pltpu
from jax.sharding import Mesh
from jax.sharding import PartitionSpec as P

DP = ("dp_0", "dp_1", "dp_2", "dp_3")
PLANE = ("dp_0", "dp_1")
LINE = "dp_2"
CORE = "dp_3"
F32 = jnp.float32
BF16 = jnp.bfloat16

LOW = 128
UNIT = 8
BLOCK = LOW + UNIT
CHUNK = 144
PAIR = 2 * BLOCK
TILE = 256
LOG2E = 1.4426950408889634


def gelu_tanh(values):
    return jax.nn.gelu(values, approximate=True)


def swap_core(x):
    return lax.ppermute(x, CORE, [(0, 1), (1, 0)])


def plane_exchange(x):
    return lax.all_to_all(x, PLANE, 0, 0, tiled=True)


def stats_exchange(x):
    return lax.all_to_all(x, (LINE, CORE), 0, 0, tiled=True)


def from_line(x, k):
    return lax.ppermute(x, LINE, [((i + k) % 4, i) for i in range(4)])


def to_line(x, k):
    return lax.ppermute(x, LINE, [(i, (i + k) % 4) for i in range(4)])


def along_line(x):
    return [x] + [from_line(x, k) for k in (1, 2, 3)]


def gathered(x):
    own = jnp.concatenate(along_line(x), axis=0)
    return (own, swap_core(own))


def place_of(pos, sc):
    over = pos - sc[17]
    slot = jnp.bitwise_and(lax.shift_right_logical(over, 3) + sc[16], 15)
    place = jnp.where(
        (over >= 0) & (over < LOW), slot * BLOCK + LOW + jnp.bitwise_and(over, 7), -1
    )
    for s in range(16):
        at = pos - sc[s]
        place = jnp.where((at >= 0) & (at < LOW), at + s * BLOCK, place)
    return place


def near_index(sc, j):
    return jnp.bitwise_and(j // 2 - sc[18], 3) + 4 * jnp.bitwise_xor(j % 2, sc[19])


def nt_dot(a, b):
    return lax.dot_general(a, b, (((1,), (1,)), ((), ())), preferred_element_type=F32)


def stats_kernel(
    sc, q_own, q_far, t_own, t_far, p, q_out, place_out, stats_out, qs, ts, *, scale
):
    for k, (q, t) in enumerate(((q_own, t_own), (q_far, t_far))):
        for b in range(4):
            qs[4 * k + b] = q[b * LOW : (b + 1) * LOW]
            ts[4 * k + b] = t[b * 16 : (b + 1) * 16]
    lane = lax.broadcasted_iota(jnp.int32, (1, LOW), 1) // UNIT
    codes = []
    spread = jnp.zeros((1, LOW), F32)
    for j in range(8):
        b = near_index(sc, j)
        q_out[j * LOW : (j + 1) * LOW] = qs[b]
        tail = ts[b]
        q_out[8 * LOW + j * UNIT : 8 * LOW + (j + 1) * UNIT] = tail[:UNIT]
        code = tail[UNIT:, :LOW].astype(F32)
        codes.append(code[0:1] * 128.0 + code[1:2])
        unit = jnp.bitwise_and(sc[20] - sc[21 + j], 15)
        part = pltpu.roll(code, jnp.bitwise_and(j - unit, 15) * UNIT, 1)
        spread = jnp.where(lane == j, part[2:3] * 128.0 + part[3:4], spread)
    codes.append(spread[:, : 8 * UNIT])
    place_out[...] = place_of(jnp.concatenate(codes, axis=1).astype(jnp.int32), sc)
    rows = q_out.shape[0]
    pull = scale * LOG2E
    top = jnp.full((1, rows), -1e30, F32)
    total = jnp.zeros((1, rows), F32)
    found = jnp.zeros((1, rows), F32)
    for at in range(0, p.shape[0], PAIR):
        tile = p[at : at + PAIR]
        s = nt_dot(tile, q_out[...])
        row = lax.broadcasted_iota(jnp.int32, s.shape, 0)
        found += jnp.sum(jnp.where(row == place_out[...] - at, s, 0.0), axis=0, keepdims=True)
        new_top = jnp.maximum(top, jnp.max(s, axis=0, keepdims=True))
        total = total * jnp.exp2((top - new_top) * pull) + jnp.sum(
            jnp.exp2(s * pull - new_top * pull), axis=0, keepdims=True
        )
        top = new_top
    line = lax.broadcasted_iota(jnp.int32, (8, rows), 0)
    stats = jnp.where(line == 0, top, jnp.where(line == 1, total, jnp.where(line == 2, found, 0.0)))
    for b in range(8):
        stats_out[b * 8 : (b + 1) * 8] = stats


def grads_kernel(stats, q, p, place, dp_out, g_ref, *, scale):
    rows, width = q.shape
    pull = scale * LOG2E
    tops = [stats[b * 8 : b * 8 + 1] for b in range(8)]
    top = functools.reduce(jnp.maximum, tops)
    total = jnp.zeros((1, rows), F32)
    found = jnp.zeros((1, rows), F32)
    for b in range(8):
        total += stats[b * 8 + 1 : b * 8 + 2] * jnp.exp2((tops[b] - top) * pull)
        found += stats[b * 8 + 2 : b * 8 + 3]
    norm = top * scale + jnp.log(total)
    loss = jnp.sum(norm - found * scale, axis=1, keepdims=True)
    norm = norm * LOG2E
    loss_high = loss.astype(BF16).astype(F32)
    loss_mid = (loss - loss_high).astype(BF16).astype(F32)
    loss_low = loss - loss_high - loss_mid
    line = lax.broadcasted_iota(jnp.int32, (UNIT, width), 0)
    loss_tile = jnp.where(
        line == 0,
        loss_high,
        jnp.where(line == 1, loss_mid, jnp.where(line == 2, loss_low, 0.0)),
    ).astype(BF16)
    for at in range(0, p.shape[0], PAIR):
        s = nt_dot(p[at : at + PAIR], q[...])
        row = lax.broadcasted_iota(jnp.int32, s.shape, 0)
        e = jnp.exp2(s * pull - norm)
        g_ref[at : at + PAIR] = jnp.where(row == place[...] - at, e - 1.0, e).astype(BF16)
    for k in range(p.shape[0] // PAIR):
        dp = scale * jnp.dot(g_ref[k * PAIR : (k + 1) * PAIR], q[...], preferred_element_type=F32)
        dp = dp.astype(BF16)
        for half in range(2):
            to = (2 * k + half) * CHUNK
            dp_out[to : to + BLOCK] = dp[half * BLOCK : (half + 1) * BLOCK]
            dp_out[to + BLOCK : to + CHUNK] = loss_tile


def query_kernel(sc, p, g, own, far, turned, *, scale):
    for at in range(0, p.shape[0], LOW):
        turned[:, at : at + LOW] = p[at : at + LOW].T

    def put(j, rows, part):
        b = near_index(sc, j)

        @pl.when(b < 4)
        def _():
            own[b, rows] = part

        @pl.when(b >= 4)
        def _():
            far[b - 4, rows] = part

    for k in range(4):
        dq = jnp.dot(turned[...], g[:, k * TILE : (k + 1) * TILE], preferred_element_type=F32)
        dq = (scale * dq).T
        for half in range(2):
            put(2 * k + half, slice(0, LOW), dq[half * LOW : (half + 1) * LOW])
    dq = jnp.dot(turned[...], g[:, 8 * LOW :], preferred_element_type=F32)
    dq = (scale * dq).T
    for j in range(8):
        put(j, slice(LOW, BLOCK), dq[j * UNIT : (j + 1) * UNIT])


def weight_parts(de_own, de_far, rows, hidden, slope, second, de):
    half = de_own.shape[0]
    de[:half] = de_own[...]
    de[half:] = de_far[...]
    grad_second = jnp.dot(hidden[...], de[...], preferred_element_type=F32)
    dpre = (slope[...] * nt_dot(second[...], de[...])).astype(BF16)
    grad_first = jnp.dot(dpre, rows[...], preferred_element_type=F32)
    return (grad_first, grad_second)


def first_weights_kernel(de_own, de_far, rows, hidden, slope, second, out, de):
    grad_first, grad_second = weight_parts(de_own, de_far, rows, hidden, slope, second, de)
    out[:, : rows.shape[1]] = grad_first
    out[:, rows.shape[1] :] = grad_second


def last_weights_kernel(sums, de_own, de_far, rows, hidden, slope, second, out, de):
    grad_first, grad_second = weight_parts(de_own, de_far, rows, hidden, slope, second, de)
    grad_first += sums[:, : rows.shape[1]]
    grad_second += sums[:, rows.shape[1] :]
    many = out.shape[0]
    wide = sums.shape[1]
    out[:, : rows.shape[1]] = grad_first[:many].astype(BF16)
    out[:, rows.shape[1] : wide] = grad_second[:many].astype(BF16)
    rest = grad_first.shape[0] - many
    x = jnp.concatenate(
        [grad_first[many:], grad_second[many:], jnp.zeros((rest, 128), F32)], axis=1
    )
    near, far = x[:, :640], x[:, 640:]
    line = jnp.bitwise_and(lax.broadcasted_iota(jnp.int32, near.shape, 0), 7)
    even = jnp.where(line < 4, near, pltpu.roll(far, 4, 0)).astype(BF16)
    odd = jnp.where(line < 4, pltpu.roll(near, rest - 4, 0), far).astype(BF16)
    for b in range(rest // 8):
        out[b * 16 : b * 16 + 8, wide:] = even[b * 8 : (b + 1) * 8]
        out[b * 16 + 8 : b * 16 + 16, wide:] = odd[b * 8 : (b + 1) * 8]


VMEM = pl.BlockSpec(memory_space=pltpu.VMEM)
SMEM = pl.BlockSpec(memory_space=pltpu.SMEM)


def score_stats(sc, qs, ts, p, scale):
    width = p.shape[1]
    rows = 8 * BLOCK
    return pl.pallas_call(
        functools.partial(stats_kernel, scale=scale),
        in_specs=[SMEM] + [VMEM] * 5,
        out_specs=[VMEM] * 3,
        out_shape=[
            jax.ShapeDtypeStruct((rows, width), BF16),
            jax.ShapeDtypeStruct((1, rows), jnp.int32),
            jax.ShapeDtypeStruct((64, rows), F32),
        ],
        scratch_shapes=[pltpu.VMEM((8, LOW, width), BF16), pltpu.VMEM((8, 16, width), BF16)],
        name="score_stats",
    )(sc, *qs, *ts, p)


def score_grads(stats, q, p, place, scale):
    columns, width = p.shape
    rows = q.shape[0]
    return pl.pallas_call(
        functools.partial(grads_kernel, scale=scale),
        in_specs=[VMEM] * 4,
        out_specs=[VMEM] * 2,
        out_shape=[
            jax.ShapeDtypeStruct((columns // BLOCK * CHUNK, width), BF16),
            jax.ShapeDtypeStruct((columns, rows), BF16),
        ],
        name="score_grads",
    )(stats, q, p, place)


def query_grads(sc, p, g, scale):
    columns, width = p.shape
    return pl.pallas_call(
        functools.partial(query_kernel, scale=scale),
        in_specs=[SMEM] + [VMEM] * 2,
        out_specs=[VMEM] * 2,
        out_shape=[jax.ShapeDtypeStruct((4, BLOCK, width), F32)] * 2,
        scratch_shapes=[pltpu.VMEM((width, columns), BF16)],
        name="query_grads",
    )(sc, p, g)


def weight_grads(sums, des, rows, hidden, slope, second):
    scratch = [pltpu.VMEM((8 * BLOCK, second.shape[1]), BF16)]
    operands = (*des, rows, hidden, slope, second)
    if sums is None:
        shape = (second.shape[0], rows.shape[1] + second.shape[1])
        return pl.pallas_call(
            first_weights_kernel,
            in_specs=[VMEM] * 6,
            out_specs=VMEM,
            out_shape=jax.ShapeDtypeStruct(shape, F32),
            scratch_shapes=scratch,
            name="first_weights",
        )(*operands)
    return pl.pallas_call(
        last_weights_kernel,
        in_specs=[VMEM] * 7,
        out_specs=VMEM,
        out_shape=jax.ShapeDtypeStruct((128, 1792), BF16),
        scratch_shapes=scratch,
        name="last_weights",
    )(sums, *operands)


def body(query_features, passage_features, counts, positives, w_first, w_second):
    width = query_features.shape[1]
    hidden_width, emb_width = w_second.shape
    scale = 2.5 * emb_width ** (-0.5)
    group = lax.axis_index((LINE, CORE))
    pairs = BLOCK * lax.axis_size(DP)

    heavy = (counts > LOW).astype(jnp.int32)
    devices = jnp.arange(counts.shape[0], dtype=jnp.int32)
    mine = heavy * (devices % 8 == group)
    heavy_at = jnp.sum(mine * (devices // 8))
    pos_high = jnp.right_shift(positives, 7).astype(BF16)
    pos_low = jnp.bitwise_and(positives, 127).astype(BF16)
    line = jnp.arange(LOW, dtype=jnp.int32)[:, None] % UNIT
    coded = jnp.where(
        line == 2, pos_high[LOW:], jnp.where(line == 3, pos_low[LOW:], jnp.zeros((), BF16))
    )
    over = jnp.concatenate([query_features[LOW:], passage_features[LOW:], coded], axis=1)
    over = jnp.concatenate([over, over], axis=0)
    over = lax.dynamic_slice_in_dim(over, (16 - heavy_at) * UNIT, LOW, 0)
    arrived = plane_exchange(over)
    tail = lax.dynamic_slice_in_dim(arrived, heavy_at * UNIT, UNIT, 0)

    def tower(x):
        pre = jnp.dot(x, w_first, preferred_element_type=F32)
        hidden = gelu_tanh(pre).astype(BF16)
        return jnp.dot(hidden, w_second, preferred_element_type=F32).astype(BF16)

    base = tower(jnp.concatenate([query_features[:LOW], passage_features[:LOW]], axis=0))
    qs = gathered(base[:LOW])

    tail_q, tail_p = tail[:, :width], tail[:, width : 2 * width]
    tail_emb = tower(jnp.concatenate([tail_q, tail_p], axis=0))
    p_send = jnp.concatenate([base[LOW:], tail_emb[UNIT:]], axis=0)
    p_send = jnp.broadcast_to(p_send[None], (16, BLOCK, emb_width))
    p_all = plane_exchange(p_send.reshape(16 * BLOCK, emb_width))

    line = line[:UNIT]
    codes = jnp.where(
        line == 0,
        pos_high[None, :LOW],
        jnp.where(line == 1, pos_low[None, :LOW], tail[:, 2 * width :]),
    )
    codes = jnp.pad(codes, ((0, 0), (0, emb_width - LOW)))
    ts = gathered(jnp.concatenate([tail_emb[:UNIT], codes], axis=0))

    late_counts, group, _ = lax.optimization_barrier((counts, group, base))
    heavy = (late_counts > LOW).astype(jnp.int32)
    mine = heavy * (devices % 8 == group)
    offsets = jnp.cumsum(late_counts) - late_counts
    over_start = jnp.sum(mine * offsets) + LOW
    group_start = lax.dynamic_slice_in_dim(offsets.reshape(16, 8), group, 1, 1)[:, 0]
    scalars = [heavy_at, over_start, lax.axis_index(LINE), lax.axis_index(CORE)]
    scalars = jnp.stack(scalars + [lax.axis_index(PLANE)])
    heavies = jnp.sum(heavy.reshape(16, 8) * jnp.arange(16, dtype=jnp.int32)[:, None], axis=0)
    sc = jnp.concatenate([group_start, scalars, heavies]).astype(jnp.int32)

    feats = jnp.concatenate(
        [query_features[:LOW], tail_q, passage_features[:LOW], tail_p], axis=0
    )
    feats, _ = lax.optimization_barrier((feats, (qs[1], ts[1])))
    feats = along_line(feats)

    each = hidden_width // lax.axis_size(DP)
    unit = jnp.arange(16 * each, dtype=jnp.int32)
    rest = unit - LOW
    unit_of = jnp.where(
        unit < LOW, (unit // 8) * (8 * each) + unit % 8, (rest // 4) * (8 * each) + 8 + rest % 4
    )
    unit_of = unit_of + group * each
    pick = (unit_of[:, None] == jnp.arange(hidden_width, dtype=jnp.int32)[None, :]).astype(BF16)
    first_part = lax.dot_general(
        pick, w_first, (((1,), (1,)), ((), ())), preferred_element_type=F32
    ).astype(BF16)
    second_part = jnp.dot(pick, w_second, preferred_element_type=F32).astype(BF16)
    p_all, first_part, second_part = lax.optimization_barrier((p_all, first_part, second_part))

    q_all, place, stats = score_stats(sc, qs, ts, p_all, scale)
    stats = stats_exchange(stats)
    dp_part, g = score_grads(stats, q_all, p_all, place, scale)
    dp_all = plane_exchange(dp_part)
    dq_own, dq_far = query_grads(sc, p_all, g, scale)

    dq = dq_own + swap_core(dq_far)
    dq_sum = dq[0].astype(BF16).astype(F32)
    for k in (1, 2, 3):
        dq_sum = dq_sum + to_line(dq[k].astype(BF16), k).astype(F32)
    dqs = gathered(dq_sum.astype(BF16))
    feats, _ = lax.optimization_barrier((feats, dq_far))
    feats_own = jnp.concatenate(
        [x[:BLOCK] for x in feats] + [x[BLOCK:] for x in feats], axis=0
    )
    feats_far = swap_core(feats_own)
    half = 4 * BLOCK

    def units_of(rows):
        pre = lax.dot_general(
            first_part, rows, (((1,), (1,)), ((), ())), preferred_element_type=F32
        )
        act, pull_back = jax.vjp(gelu_tanh, pre)
        return (rows, act.astype(BF16), pull_back(jnp.ones_like(pre))[0])

    q_units = units_of(jnp.concatenate([feats_own[:half], feats_far[:half]], axis=0))
    p_units = units_of(jnp.concatenate([feats_own[half:], feats_far[half:]], axis=0))
    dp_all, dqs, q_units, p_units = lax.optimization_barrier((dp_all, dqs, q_units, p_units))

    dp_sum = jnp.sum(dp_all.reshape(16, CHUNK, emb_width).astype(F32), axis=0)
    mean_loss = (dp_sum[BLOCK, 0] + dp_sum[BLOCK + 1, 0] + dp_sum[BLOCK + 2, 0]) / pairs
    dps = gathered(dp_sum[:BLOCK].astype(BF16))
    sums = weight_grads(None, dqs, *q_units, second_part)
    grads = weight_grads(sums, dps, *p_units, second_part)
    out = jnp.sum(plane_exchange(grads).reshape(16, 8, -1).astype(F32), axis=0)
    wide = width + emb_width
    tail_out = jnp.concatenate([out[:4, wide:], out[4:, wide : 2 * wide - 640]], axis=1)
    out = jnp.concatenate([out[:, :wide], tail_out], axis=0)
    return (mean_loss, out[:, :width].T, out[:, width:])


def solution(mesh):
    finer = Mesh(mesh.devices.reshape(4, 4, 4, 2), DP)
    placed = (P(DP, None), P(DP, None), P(), P(DP), P(), P())
    return jax.shard_map(
        body,
        mesh=finer,
        in_specs=placed,
        out_specs=(P(), P(None, DP), P(DP, None)),
        check_vma=False,
    )
```

```python
import functools

import jax
import jax.numpy as jnp
from jax import lax
from jax.experimental import pallas as pl
from jax.experimental.pallas import tpu as pltpu
from jax.sharding import Mesh
from jax.sharding import PartitionSpec as P

DP = ("dp_0", "dp_1", "dp_2", "dp_3")
PLANE = ("dp_0", "dp_1")
LINE = "dp_2"
CORE = "dp_3"
F32 = jnp.float32
BF16 = jnp.bfloat16

LOW = 128
UNIT = 8
BLOCK = LOW + UNIT
CHUNK = 144
PAIR = 2 * BLOCK
LOG2E = 1.4426950408889634


def gelu_tanh(values):
    return jax.nn.gelu(values, approximate=True)


def swap_core(x):
    return lax.ppermute(x, CORE, [(0, 1), (1, 0)])


def plane_exchange(x):
    return lax.all_to_all(x, PLANE, 0, 0, tiled=True)


def stats_exchange(x):
    return lax.all_to_all(x, (LINE, CORE), 0, 0, tiled=True)


def from_line(x, k):
    return lax.ppermute(x, LINE, [((i + k) % 4, i) for i in range(4)])


def to_line(x, k):
    return lax.ppermute(x, LINE, [(i, (i + k) % 4) for i in range(4)])


def along_line(x):
    return [x] + [from_line(x, k) for k in (1, 2, 3)]


def gathered(x):
    own = jnp.concatenate(along_line(x), axis=0)
    return (own, swap_core(own))


def place_of(pos, sc):
    over = pos - sc[17]
    slot = jnp.bitwise_and(lax.shift_right_logical(over, 3) + sc[16], 15)
    place = jnp.where(
        (over >= 0) & (over < LOW), slot * BLOCK + LOW + jnp.bitwise_and(over, 7), -1
    )
    for s in range(16):
        at = pos - sc[s]
        place = jnp.where((at >= 0) & (at < LOW), at + s * BLOCK, place)
    return place


def near_index(sc, j):
    return jnp.bitwise_and(j // 2 - sc[18], 3) + 4 * jnp.bitwise_xor(j % 2, sc[19])


def nt_dot(a, b):
    return lax.dot_general(a, b, (((1,), (1,)), ((), ())), preferred_element_type=F32)


def pack_kernel(counts, where, q, p, pos, out, heavy_out):
    heavy_at = jnp.int32(0)
    for s in range(16):
        heavy_at += jnp.where(counts[s * 8 + where[0]] > LOW, s, 0)
    heavy_out[0] = heavy_at
    width = q.shape[1]
    high = lax.shift_right_logical(pos[1:2], 7).astype(F32)
    low = jnp.bitwise_and(pos[1:2], 127).astype(F32)
    line = lax.broadcasted_iota(jnp.int32, (UNIT, LOW), 0)
    code = jnp.where(line == 2, high, jnp.where(line == 3, low, 0.0)).astype(BF16)
    for u in range(16):
        slot = jnp.bitwise_and(heavy_at + u, 15)
        out[slot, :, :width] = q[u * UNIT : (u + 1) * UNIT]
        out[slot, :, width : 2 * width] = p[u * UNIT : (u + 1) * UNIT]
        out[slot, :, 2 * width :] = code


def gelu_parts(v):
    square = v * v
    t = jnp.tanh(0.7978845608028654 * (v + 0.044715 * (square * v)))
    grown = 0.5 * (1.0 + t)
    slope = grown + (0.5 * v) * (1.0 - t * t) * (
        0.7978845608028654 * (1.0 + 3 * 0.044715 * square)
    )
    return (v * grown, slope)


def tail_kernel(heavy_at, arrived, base_p, pos, w_first, w_second, p_out, q_out, feats_out):
    width = w_first.shape[0]
    tail = arrived[heavy_at[0]]
    feats = jnp.concatenate([tail[:, :width], tail[:, width : 2 * width]], axis=0)
    feats_out[...] = feats
    pre = jnp.dot(feats, w_first[...], preferred_element_type=F32)
    hidden = gelu_parts(pre)[0].astype(BF16)
    emb = jnp.dot(hidden, w_second[...], preferred_element_type=F32).astype(BF16)
    for s in range(p_out.shape[0]):
        p_out[s, :LOW] = base_p[...]
        p_out[s, LOW:] = emb[UNIT:]
    high = lax.shift_right_logical(pos[0:1], 7).astype(F32)
    low = jnp.bitwise_and(pos[0:1], 127).astype(F32)
    line = lax.broadcasted_iota(jnp.int32, (UNIT, LOW), 0)
    code = tail[:, 2 * width :].astype(F32)
    code = jnp.where(line == 0, high, jnp.where(line == 1, low, code)).astype(BF16)
    q_out[:UNIT] = emb[:UNIT]
    q_out[UNIT:] = jnp.zeros((UNIT, q_out.shape[1]), BF16)
    q_out[UNIT:, :LOW] = code


def units_kernel(*refs):
    blocks, (first, rows_q, rows_p, hidden_q, hidden_p, slope_q, slope_p) = refs[:8], refs[8:]
    for k, block in enumerate(blocks):
        rows_q[k * BLOCK : (k + 1) * BLOCK] = block[:BLOCK]
        rows_p[k * BLOCK : (k + 1) * BLOCK] = block[BLOCK:]
    for rows, hidden, slope in ((rows_q, hidden_q, slope_q), (rows_p, hidden_p, slope_p)):
        value, gain = gelu_parts(nt_dot(first[...], rows[...]))
        hidden[...] = value.astype(BF16)
        slope[...] = gain


def stats_kernel(
    sc, q_own, q_far, t_own, t_far, p, q_out, place_out, stats_out, qs, ts, *, scale
):
    for k, (q, t) in enumerate(((q_own, t_own), (q_far, t_far))):
        for b in range(4):
            qs[4 * k + b] = q[b * LOW : (b + 1) * LOW]
            ts[4 * k + b] = t[b * 16 : (b + 1) * 16]
    lane = lax.broadcasted_iota(jnp.int32, (1, LOW), 1) // UNIT
    codes = []
    spread = jnp.zeros((1, LOW), F32)
    for j in range(8):
        b = near_index(sc, j)
        q_out[j * LOW : (j + 1) * LOW] = qs[b]
        tail = ts[b]
        q_out[8 * LOW + j * UNIT : 8 * LOW + (j + 1) * UNIT] = tail[:UNIT]
        code = tail[UNIT:, :LOW].astype(F32)
        codes.append(code[0:1] * 128.0 + code[1:2])
        unit = jnp.bitwise_and(sc[20] - sc[21 + j], 15)
        part = pltpu.roll(code, jnp.bitwise_and(j - unit, 15) * UNIT, 1)
        spread = jnp.where(lane == j, part[2:3] * 128.0 + part[3:4], spread)
    codes.append(spread[:, : 8 * UNIT])
    place_out[...] = place_of(jnp.concatenate(codes, axis=1).astype(jnp.int32), sc)
    rows = q_out.shape[0]
    pull = scale * LOG2E
    top = jnp.full((1, rows), -1e30, F32)
    total = jnp.zeros((1, rows), F32)
    found = jnp.zeros((1, rows), F32)
    for at in range(0, p.shape[0], PAIR):
        tile = p[at : at + PAIR]
        s = nt_dot(tile, q_out[...])
        row = lax.broadcasted_iota(jnp.int32, s.shape, 0)
        found += jnp.sum(jnp.where(row == place_out[...] - at, s, 0.0), axis=0, keepdims=True)
        new_top = jnp.maximum(top, jnp.max(s, axis=0, keepdims=True))
        total = total * jnp.exp2((top - new_top) * pull) + jnp.sum(
            jnp.exp2(s * pull - new_top * pull), axis=0, keepdims=True
        )
        top = new_top
    line = lax.broadcasted_iota(jnp.int32, (8, rows), 0)
    stats = jnp.where(line == 0, top, jnp.where(line == 1, total, jnp.where(line == 2, found, 0.0)))
    for b in range(8):
        stats_out[b * 8 : (b + 1) * 8] = stats


def grads_kernel(stats, q, p, place, dp_out, g_ref, *, scale):
    rows, width = q.shape
    pull = scale * LOG2E
    tops = [stats[b * 8 : b * 8 + 1] for b in range(8)]
    top = functools.reduce(jnp.maximum, tops)
    total = jnp.zeros((1, rows), F32)
    found = jnp.zeros((1, rows), F32)
    for b in range(8):
        total += stats[b * 8 + 1 : b * 8 + 2] * jnp.exp2((tops[b] - top) * pull)
        found += stats[b * 8 + 2 : b * 8 + 3]
    norm = top * scale + jnp.log(total)
    loss = jnp.sum(norm - found * scale, axis=1, keepdims=True)
    norm = norm * LOG2E
    loss_high = loss.astype(BF16).astype(F32)
    loss_mid = (loss - loss_high).astype(BF16).astype(F32)
    loss_low = loss - loss_high - loss_mid
    line = lax.broadcasted_iota(jnp.int32, (UNIT, width), 0)
    loss_tile = jnp.where(
        line == 0,
        loss_high,
        jnp.where(line == 1, loss_mid, jnp.where(line == 2, loss_low, 0.0)),
    ).astype(BF16)
    for at in range(0, p.shape[0], PAIR):
        s = nt_dot(p[at : at + PAIR], q[...])
        row = lax.broadcasted_iota(jnp.int32, s.shape, 0)
        e = jnp.exp2(s * pull - norm)
        g_ref[at : at + PAIR] = jnp.where(row == place[...] - at, e - 1.0, e).astype(BF16)
    for k in range(p.shape[0] // PAIR):
        dp = scale * jnp.dot(g_ref[k * PAIR : (k + 1) * PAIR], q[...], preferred_element_type=F32)
        dp = dp.astype(BF16)
        for half in range(2):
            to = (2 * k + half) * CHUNK
            dp_out[to : to + BLOCK] = dp[half * BLOCK : (half + 1) * BLOCK]
            dp_out[to + BLOCK : to + CHUNK] = loss_tile


def query_kernel(sc, p, g, own, far, turned, *, scale):
    for at in range(0, p.shape[0], LOW):
        turned[:, at : at + LOW] = p[at : at + LOW].T

    def put(j, rows, part):
        b = near_index(sc, j)

        @pl.when(b < 4)
        def _():
            own[b, rows] = part

        @pl.when(b >= 4)
        def _():
            far[b - 4, rows] = part

    for first, size in ((0, 4 * LOW), (4 * LOW, 4 * LOW + 8 * UNIT)):
        dq = jnp.dot(turned[...], g[:, first : first + size], preferred_element_type=F32)
        dq = (scale * dq).T
        for k in range(4):
            put(first // LOW + k, slice(0, LOW), dq[k * LOW : (k + 1) * LOW])
    dq = dq[4 * LOW :]
    for j in range(8):
        put(j, slice(LOW, BLOCK), dq[j * UNIT : (j + 1) * UNIT])


def weight_parts(de_own, de_far, rows, hidden, slope, second, de):
    half = de_own.shape[0]
    de[:half] = de_own[...]
    de[half:] = de_far[...]
    grad_second = jnp.dot(hidden[...], de[...], preferred_element_type=F32)
    dpre = (slope[...] * nt_dot(second[...], de[...])).astype(BF16)
    grad_first = jnp.dot(dpre, rows[...], preferred_element_type=F32)
    return (grad_first, grad_second)


def first_weights_kernel(de_own, de_far, rows, hidden, slope, second, out, de):
    grad_first, grad_second = weight_parts(de_own, de_far, rows, hidden, slope, second, de)
    out[:, : rows.shape[1]] = grad_first
    out[:, rows.shape[1] :] = grad_second


def last_weights_kernel(sums, de_own, de_far, rows, hidden, slope, second, out, de):
    grad_first, grad_second = weight_parts(de_own, de_far, rows, hidden, slope, second, de)
    grad_first += sums[:, : rows.shape[1]]
    grad_second += sums[:, rows.shape[1] :]
    many = out.shape[0]
    wide = sums.shape[1]
    out[:, : rows.shape[1]] = grad_first[:many].astype(BF16)
    out[:, rows.shape[1] : wide] = grad_second[:many].astype(BF16)
    rest = grad_first.shape[0] - many
    x = jnp.concatenate(
        [grad_first[many:], grad_second[many:], jnp.zeros((rest, 128), F32)], axis=1
    )
    near, far = x[:, :640], x[:, 640:]
    line = jnp.bitwise_and(lax.broadcasted_iota(jnp.int32, near.shape, 0), 7)
    even = jnp.where(line < 4, near, pltpu.roll(far, 4, 0)).astype(BF16)
    odd = jnp.where(line < 4, pltpu.roll(near, rest - 4, 0), far).astype(BF16)
    for b in range(rest // 8):
        out[b * 16 : b * 16 + 8, wide:] = even[b * 8 : (b + 1) * 8]
        out[b * 16 + 8 : b * 16 + 16, wide:] = odd[b * 8 : (b + 1) * 8]


VMEM = pl.BlockSpec(memory_space=pltpu.VMEM)
SMEM = pl.BlockSpec(memory_space=pltpu.SMEM)


def pack_overflow(counts, where, q, p, pos):
    width = q.shape[1]
    half = pl.BlockSpec((LOW, width), lambda i: (1, 0))
    return pl.pallas_call(
        pack_kernel,
        grid=(1,),
        in_specs=[SMEM, SMEM, half, half, pl.BlockSpec((2, LOW), lambda i: (0, 0))],
        out_specs=[pl.BlockSpec((16, UNIT, 2 * width + LOW), lambda i: (0, 0, 0)), SMEM],
        out_shape=[
            jax.ShapeDtypeStruct((16, UNIT, 2 * width + LOW), BF16),
            jax.ShapeDtypeStruct((1,), jnp.int32),
        ],
        name="pack_overflow",
    )(counts, where, q, p, pos)


def tail_rows(heavy_at, arrived, base_p, pos, w_first, w_second):
    emb_width = w_second.shape[1]
    return pl.pallas_call(
        tail_kernel,
        in_specs=[SMEM] + [VMEM] * 5,
        out_specs=[VMEM] * 3,
        out_shape=[
            jax.ShapeDtypeStruct((16, BLOCK, emb_width), BF16),
            jax.ShapeDtypeStruct((2 * UNIT, emb_width), BF16),
            jax.ShapeDtypeStruct((2 * UNIT, w_first.shape[0]), BF16),
        ],
        name="tail_rows",
    )(heavy_at, arrived, base_p, pos, w_first, w_second)


def hidden_units(blocks, first):
    rows = jax.ShapeDtypeStruct((8 * BLOCK, first.shape[1]), BF16)
    hidden = jax.ShapeDtypeStruct((first.shape[0], 8 * BLOCK), BF16)
    slope = jax.ShapeDtypeStruct((first.shape[0], 8 * BLOCK), F32)
    rows_q, rows_p, hidden_q, hidden_p, slope_q, slope_p = pl.pallas_call(
        units_kernel,
        in_specs=[VMEM] * 9,
        out_specs=[VMEM] * 6,
        out_shape=[rows, rows, hidden, hidden, slope, slope],
        name="hidden_units",
    )(*blocks, first)
    return ((rows_q, hidden_q, slope_q), (rows_p, hidden_p, slope_p))


def score_stats(sc, qs, ts, p, scale):
    width = p.shape[1]
    rows = 8 * BLOCK
    return pl.pallas_call(
        functools.partial(stats_kernel, scale=scale),
        in_specs=[SMEM] + [VMEM] * 5,
        out_specs=[VMEM] * 3,
        out_shape=[
            jax.ShapeDtypeStruct((rows, width), BF16),
            jax.ShapeDtypeStruct((1, rows), jnp.int32),
            jax.ShapeDtypeStruct((64, rows), F32),
        ],
        scratch_shapes=[pltpu.VMEM((8, LOW, width), BF16), pltpu.VMEM((8, 16, width), BF16)],
        name="score_stats",
    )(sc, *qs, *ts, p)


def score_grads(stats, q, p, place, scale):
    columns, width = p.shape
    rows = q.shape[0]
    return pl.pallas_call(
        functools.partial(grads_kernel, scale=scale),
        in_specs=[VMEM] * 4,
        out_specs=[VMEM] * 2,
        out_shape=[
            jax.ShapeDtypeStruct((columns // BLOCK * CHUNK, width), BF16),
            jax.ShapeDtypeStruct((columns, rows), BF16),
        ],
        name="score_grads",
    )(stats, q, p, place)


def query_grads(sc, p, g, scale):
    columns, width = p.shape
    return pl.pallas_call(
        functools.partial(query_kernel, scale=scale),
        in_specs=[SMEM] + [VMEM] * 2,
        out_specs=[VMEM] * 2,
        out_shape=[jax.ShapeDtypeStruct((4, BLOCK, width), F32)] * 2,
        scratch_shapes=[pltpu.VMEM((width, columns), BF16)],
        name="query_grads",
    )(sc, p, g)


def weight_grads(sums, des, rows, hidden, slope, second):
    scratch = [pltpu.VMEM((8 * BLOCK, second.shape[1]), BF16)]
    operands = (*des, rows, hidden, slope, second)
    if sums is None:
        shape = (second.shape[0], rows.shape[1] + second.shape[1])
        return pl.pallas_call(
            first_weights_kernel,
            in_specs=[VMEM] * 6,
            out_specs=VMEM,
            out_shape=jax.ShapeDtypeStruct(shape, F32),
            scratch_shapes=scratch,
            name="first_weights",
        )(*operands)
    return pl.pallas_call(
        last_weights_kernel,
        in_specs=[VMEM] * 7,
        out_specs=VMEM,
        out_shape=jax.ShapeDtypeStruct((128, 1792), BF16),
        scratch_shapes=scratch,
        name="last_weights",
    )(sums, *operands)


def body(query_features, passage_features, counts, positives, w_first, w_second):
    width = query_features.shape[1]
    hidden_width, emb_width = w_second.shape
    scale = 2.5 * emb_width ** (-0.5)
    group = lax.axis_index((LINE, CORE))
    pairs = BLOCK * lax.axis_size(DP)

    pos = positives.reshape(2, LOW)
    where = jnp.reshape(group, (1,)).astype(jnp.int32)
    over, heavy_at = pack_overflow(counts, where, query_features, passage_features, pos)
    over = over.reshape(16 * UNIT, -1)
    arrived = plane_exchange(over)

    def tower(x):
        pre = jnp.dot(x, w_first, preferred_element_type=F32)
        hidden = gelu_tanh(pre).astype(BF16)
        return jnp.dot(hidden, w_second, preferred_element_type=F32).astype(BF16)

    base = tower(jnp.concatenate([query_features[:LOW], passage_features[:LOW]], axis=0))
    qs = gathered(base[:LOW])

    p_send, q_tail, tail = tail_rows(
        heavy_at, arrived.reshape(16, UNIT, -1), base[LOW:], pos, w_first, w_second
    )
    p_all = plane_exchange(p_send.reshape(16 * BLOCK, emb_width))
    ts = gathered(q_tail)

    late_counts, group, _ = lax.optimization_barrier((counts, group, q_tail))
    heavy = (late_counts > LOW).astype(jnp.int32)
    devices = jnp.arange(counts.shape[0], dtype=jnp.int32)
    mine = heavy * (devices % 8 == group)
    offsets = jnp.cumsum(late_counts) - late_counts
    over_start = jnp.sum(mine * offsets) + LOW
    group_start = lax.dynamic_slice_in_dim(offsets.reshape(16, 8), group, 1, 1)[:, 0]
    scalars = [heavy_at[0], over_start, lax.axis_index(LINE), lax.axis_index(CORE)]
    scalars = jnp.stack(scalars + [lax.axis_index(PLANE)])
    heavies = jnp.sum(heavy.reshape(16, 8) * jnp.arange(16, dtype=jnp.int32)[:, None], axis=0)
    sc = jnp.concatenate([group_start, scalars, heavies]).astype(jnp.int32)

    feats = jnp.concatenate(
        [query_features[:LOW], tail[:UNIT], passage_features[:LOW], tail[UNIT:]], axis=0
    )
    feats, _ = lax.optimization_barrier((feats, (qs[1], ts[1])))
    feats = along_line(feats)
    feats = feats + [swap_core(x) for x in feats]

    each = hidden_width // lax.axis_size(DP)
    unit = jnp.arange(16 * each, dtype=jnp.int32)
    rest = unit - LOW
    unit_of = jnp.where(
        unit < LOW, (unit // 8) * (8 * each) + unit % 8, (rest // 4) * (8 * each) + 8 + rest % 4
    )
    unit_of = unit_of + group * each
    pick = (unit_of[:, None] == jnp.arange(hidden_width, dtype=jnp.int32)[None, :]).astype(BF16)
    first_part = lax.dot_general(
        pick, w_first, (((1,), (1,)), ((), ())), preferred_element_type=F32
    ).astype(BF16)
    second_part = jnp.dot(pick, w_second, preferred_element_type=F32).astype(BF16)
    p_all, first_part, second_part = lax.optimization_barrier((p_all, first_part, second_part))

    q_all, place, stats = score_stats(sc, qs, ts, p_all, scale)
    stats = stats_exchange(stats)
    dp_part, g = score_grads(stats, q_all, p_all, place, scale)
    dp_all = plane_exchange(dp_part)
    dq_own, dq_far = query_grads(sc, p_all, g, scale)

    dq = dq_own + swap_core(dq_far)
    dq_sum = dq[0].astype(BF16).astype(F32)
    for k in (1, 2, 3):
        dq_sum = dq_sum + to_line(dq[k].astype(BF16), k).astype(F32)
    dqs = gathered(dq_sum.astype(BF16))
    feats, _ = lax.optimization_barrier((feats, dq_far))
    q_units, p_units = hidden_units(feats, first_part)
    dp_all, dqs, q_units, p_units = lax.optimization_barrier((dp_all, dqs, q_units, p_units))

    dp_sum = jnp.sum(dp_all.reshape(16, CHUNK, emb_width).astype(F32), axis=0)
    mean_loss = (dp_sum[BLOCK, 0] + dp_sum[BLOCK + 1, 0] + dp_sum[BLOCK + 2, 0]) / pairs
    dps = gathered(dp_sum[:BLOCK].astype(BF16))
    sums = weight_grads(None, dqs, *q_units, second_part)
    grads = weight_grads(sums, dps, *p_units, second_part)
    out = jnp.sum(plane_exchange(grads).reshape(16, 8, -1).astype(F32), axis=0)
    wide = width + emb_width
    tail_out = jnp.concatenate([out[:4, wide:], out[4:, wide : 2 * wide - 640]], axis=1)
    out = jnp.concatenate([out[:, :wide], tail_out], axis=0)
    return (mean_loss, out[:, :width].T, out[:, width:])


def solution(mesh):
    finer = Mesh(mesh.devices.reshape(4, 4, 4, 2), DP)
    placed = (P(DP, None), P(DP, None), P(), P(DP), P(), P())
    return jax.shard_map(
        body,
        mesh=finer,
        in_specs=placed,
        out_specs=(P(), P(None, DP), P(DP, None)),
        check_vma=False,
    )
```

```python
import functools

import jax
import jax.numpy as jnp
from jax import lax
from jax.experimental import pallas as pl
from jax.experimental.pallas import tpu as pltpu
from jax.sharding import Mesh
from jax.sharding import PartitionSpec as P

DP = ("dp_0", "dp_1", "dp_2", "dp_3")
PLANE = ("dp_0", "dp_1")
LINE = "dp_2"
CORE = "dp_3"
F32 = jnp.float32
BF16 = jnp.bfloat16

LOW = 128
UNIT = 8
BLOCK = LOW + UNIT
CHUNK = 144
PAIR = 2 * BLOCK
LOG2E = 1.4426950408889634


def gelu_tanh(values):
    return jax.nn.gelu(values, approximate=True)


def swap_core(x):
    return lax.ppermute(x, CORE, [(0, 1), (1, 0)])


def plane_exchange(x):
    return lax.all_to_all(x, PLANE, 0, 0, tiled=True)


def stats_exchange(x):
    return lax.all_to_all(x, (LINE, CORE), 0, 0, tiled=True)


def from_line(x, k):
    return lax.ppermute(x, LINE, [((i + k) % 4, i) for i in range(4)])


def to_line(x, k):
    return lax.ppermute(x, LINE, [(i, (i + k) % 4) for i in range(4)])


def along_line(x):
    return [x] + [from_line(x, k) for k in (1, 2, 3)]


def gathered(x):
    own = jnp.concatenate(along_line(x), axis=0)
    return (own, swap_core(own))


def place_of(pos, sc):
    over = pos - sc[17]
    slot = jnp.bitwise_and(lax.shift_right_logical(over, 3) + sc[16], 15)
    place = jnp.where(
        (over >= 0) & (over < LOW), slot * BLOCK + LOW + jnp.bitwise_and(over, 7), -1
    )
    for s in range(16):
        at = pos - sc[s]
        place = jnp.where((at >= 0) & (at < LOW), at + s * BLOCK, place)
    return place


def near_index(sc, j):
    return jnp.bitwise_and(j // 2 - sc[18], 3) + 4 * jnp.bitwise_xor(j % 2, sc[19])


def nt_dot(a, b):
    return lax.dot_general(a, b, (((1,), (1,)), ((), ())), preferred_element_type=F32)


def pack_kernel(counts, where, q, p, pos, out, heavy_out):
    heavy_at = jnp.int32(0)
    for s in range(16):
        heavy_at += jnp.where(counts[s * 8 + where[0]] > LOW, s, 0)
    heavy_out[0] = heavy_at
    width = q.shape[1]
    high = lax.shift_right_logical(pos[1:2], 7).astype(F32)
    low = jnp.bitwise_and(pos[1:2], 127).astype(F32)
    line = lax.broadcasted_iota(jnp.int32, (UNIT, LOW), 0)
    code = jnp.where(line == 2, high, jnp.where(line == 3, low, 0.0)).astype(BF16)
    for u in range(16):
        slot = jnp.bitwise_and(heavy_at + u, 15)
        out[slot, :, :width] = q[u * UNIT : (u + 1) * UNIT]
        out[slot, :, width : 2 * width] = p[u * UNIT : (u + 1) * UNIT]
        out[slot, :, 2 * width :] = code


def gelu_parts(v):
    square = v * v
    t = jnp.tanh(0.7978845608028654 * (v + 0.044715 * (square * v)))
    grown = 0.5 * (1.0 + t)
    slope = grown + (0.5 * v) * (1.0 - t * t) * (
        0.7978845608028654 * (1.0 + 3 * 0.044715 * square)
    )
    return (v * grown, slope)


def tail_kernel(heavy_at, arrived, base_p, pos, w_first, w_second, p_out, q_out):
    width, emb_width = w_first.shape[0], w_second.shape[1]
    tail = arrived[heavy_at[0]]
    feats = jnp.concatenate([tail[:, :width], tail[:, width : 2 * width]], axis=0)
    q_out[:, emb_width:] = feats
    pre = jnp.dot(feats, w_first[...], preferred_element_type=F32)
    hidden = gelu_parts(pre)[0].astype(BF16)
    emb = jnp.dot(hidden, w_second[...], preferred_element_type=F32).astype(BF16)
    for s in range(p_out.shape[0]):
        p_out[s, :LOW] = base_p[...]
        p_out[s, LOW:] = emb[UNIT:]
    high = lax.shift_right_logical(pos[0:1], 7).astype(F32)
    low = jnp.bitwise_and(pos[0:1], 127).astype(F32)
    line = lax.broadcasted_iota(jnp.int32, (UNIT, LOW), 0)
    code = tail[:, 2 * width :].astype(F32)
    code = jnp.where(line == 0, high, jnp.where(line == 1, low, code)).astype(BF16)
    q_out[:UNIT, :emb_width] = emb[:UNIT]
    q_out[UNIT:, LOW:emb_width] = jnp.zeros((UNIT, emb_width - LOW), BF16)
    q_out[UNIT:, :LOW] = code


def units_kernel(*refs):
    blocks, tails, (first, rows_q, rows_p, hidden_q, hidden_p, slope_q, slope_p) = (
        refs[:8],
        refs[8:10],
        refs[10:],
    )
    skip = tails[0].shape[1] - rows_q.shape[1]
    for k, block in enumerate(blocks):
        tail = tails[k // 4][(k % 4) * 2 * UNIT : (k % 4 + 1) * 2 * UNIT, skip:]
        at = k * BLOCK
        rows_q[at : at + LOW] = block[:LOW]
        rows_q[at + LOW : at + BLOCK] = tail[:UNIT]
        rows_p[at : at + LOW] = block[LOW:]
        rows_p[at + LOW : at + BLOCK] = tail[UNIT:]
    for rows, hidden, slope in ((rows_q, hidden_q, slope_q), (rows_p, hidden_p, slope_p)):
        value, gain = gelu_parts(nt_dot(first[...], rows[...]))
        hidden[...] = value.astype(BF16)
        slope[...] = gain


def stats_kernel(
    sc, q_own, q_far, t_own, t_far, p, q_out, place_out, stats_out, qs, ts, *, scale
):
    for k, (q, t) in enumerate(((q_own, t_own), (q_far, t_far))):
        for b in range(4):
            qs[4 * k + b] = q[b * LOW : (b + 1) * LOW]
            ts[4 * k + b] = t[b * 16 : (b + 1) * 16, : p.shape[1]]
    lane = lax.broadcasted_iota(jnp.int32, (1, LOW), 1) // UNIT
    codes = []
    spread = jnp.zeros((1, LOW), F32)
    for j in range(8):
        b = near_index(sc, j)
        q_out[j * LOW : (j + 1) * LOW] = qs[b]
        tail = ts[b]
        q_out[8 * LOW + j * UNIT : 8 * LOW + (j + 1) * UNIT] = tail[:UNIT]
        code = tail[UNIT:, :LOW].astype(F32)
        codes.append(code[0:1] * 128.0 + code[1:2])
        unit = jnp.bitwise_and(sc[20] - sc[21 + j], 15)
        part = pltpu.roll(code, jnp.bitwise_and(j - unit, 15) * UNIT, 1)
        spread = jnp.where(lane == j, part[2:3] * 128.0 + part[3:4], spread)
    codes.append(spread[:, : 8 * UNIT])
    place_out[...] = place_of(jnp.concatenate(codes, axis=1).astype(jnp.int32), sc)
    rows = q_out.shape[0]
    pull = scale * LOG2E
    top = jnp.full((1, rows), -1e30, F32)
    total = jnp.zeros((1, rows), F32)
    found = jnp.zeros((1, rows), F32)
    for at in range(0, p.shape[0], PAIR):
        tile = p[at : at + PAIR]
        s = nt_dot(tile, q_out[...])
        row = lax.broadcasted_iota(jnp.int32, s.shape, 0)
        found += jnp.sum(jnp.where(row == place_out[...] - at, s, 0.0), axis=0, keepdims=True)
        new_top = jnp.maximum(top, jnp.max(s, axis=0, keepdims=True))
        total = total * jnp.exp2((top - new_top) * pull) + jnp.sum(
            jnp.exp2(s * pull - new_top * pull), axis=0, keepdims=True
        )
        top = new_top
    line = lax.broadcasted_iota(jnp.int32, (8, rows), 0)
    stats = jnp.where(line == 0, top, jnp.where(line == 1, total, jnp.where(line == 2, found, 0.0)))
    for b in range(8):
        stats_out[b * 8 : (b + 1) * 8] = stats


def grads_kernel(stats, q, p, place, dp_out, g_ref, *, scale):
    rows, width = q.shape
    pull = scale * LOG2E
    tops = [stats[b * 8 : b * 8 + 1] for b in range(8)]
    top = functools.reduce(jnp.maximum, tops)
    total = jnp.zeros((1, rows), F32)
    found = jnp.zeros((1, rows), F32)
    for b in range(8):
        total += stats[b * 8 + 1 : b * 8 + 2] * jnp.exp2((tops[b] - top) * pull)
        found += stats[b * 8 + 2 : b * 8 + 3]
    norm = top * scale + jnp.log(total)
    loss = jnp.sum(norm - found * scale, axis=1, keepdims=True)
    norm = norm * LOG2E
    loss_high = loss.astype(BF16).astype(F32)
    loss_mid = (loss - loss_high).astype(BF16).astype(F32)
    loss_low = loss - loss_high - loss_mid
    line = lax.broadcasted_iota(jnp.int32, (UNIT, width), 0)
    loss_tile = jnp.where(
        line == 0,
        loss_high,
        jnp.where(line == 1, loss_mid, jnp.where(line == 2, loss_low, 0.0)),
    ).astype(BF16)
    for at in range(0, p.shape[0], PAIR):
        s = nt_dot(p[at : at + PAIR], q[...])
        row = lax.broadcasted_iota(jnp.int32, s.shape, 0)
        e = jnp.exp2(s * pull - norm)
        g_ref[at : at + PAIR] = jnp.where(row == place[...] - at, e - 1.0, e).astype(BF16)
    for k in range(p.shape[0] // PAIR):
        dp = scale * jnp.dot(g_ref[k * PAIR : (k + 1) * PAIR], q[...], preferred_element_type=F32)
        dp = dp.astype(BF16)
        for half in range(2):
            to = (2 * k + half) * CHUNK
            dp_out[to : to + BLOCK] = dp[half * BLOCK : (half + 1) * BLOCK]
            dp_out[to + BLOCK : to + CHUNK] = loss_tile


def query_kernel(sc, p, g, own, far, turned, *, scale):
    for at in range(0, p.shape[0], LOW):
        turned[:, at : at + LOW] = p[at : at + LOW].T

    def put(j, rows, part):
        b = near_index(sc, j)

        @pl.when(b < 4)
        def _():
            own[b, rows] = part

        @pl.when(b >= 4)
        def _():
            far[b - 4, rows] = part

    for first, size in ((0, 4 * LOW), (4 * LOW, 4 * LOW + 8 * UNIT)):
        dq = jnp.dot(turned[...], g[:, first : first + size], preferred_element_type=F32)
        dq = (scale * dq).T
        for k in range(4):
            put(first // LOW + k, slice(0, LOW), dq[k * LOW : (k + 1) * LOW])
    dq = dq[4 * LOW :]
    for j in range(8):
        put(j, slice(LOW, BLOCK), dq[j * UNIT : (j + 1) * UNIT])


def weight_parts(de_own, de_far, rows, hidden, slope, second, de):
    half = de_own.shape[0]
    de[:half] = de_own[...]
    de[half:] = de_far[...]
    grad_second = jnp.dot(hidden[...], de[...], preferred_element_type=F32)
    dpre = (slope[...] * nt_dot(second[...], de[...])).astype(BF16)
    grad_first = jnp.dot(dpre, rows[...], preferred_element_type=F32)
    return (grad_first, grad_second)


def first_weights_kernel(de_own, de_far, rows, hidden, slope, second, out, de):
    grad_first, grad_second = weight_parts(de_own, de_far, rows, hidden, slope, second, de)
    out[:, : rows.shape[1]] = grad_first
    out[:, rows.shape[1] :] = grad_second


def last_weights_kernel(sums, de_own, de_far, rows, hidden, slope, second, out, de):
    grad_first, grad_second = weight_parts(de_own, de_far, rows, hidden, slope, second, de)
    grad_first += sums[:, : rows.shape[1]]
    grad_second += sums[:, rows.shape[1] :]
    many = out.shape[0]
    wide = sums.shape[1]
    out[:, : rows.shape[1]] = grad_first[:many].astype(BF16)
    out[:, rows.shape[1] : wide] = grad_second[:many].astype(BF16)
    rest = grad_first.shape[0] - many
    x = jnp.concatenate(
        [grad_first[many:], grad_second[many:], jnp.zeros((rest, 128), F32)], axis=1
    )
    near, far = x[:, :640], x[:, 640:]
    line = jnp.bitwise_and(lax.broadcasted_iota(jnp.int32, near.shape, 0), 7)
    even = jnp.where(line < 4, near, pltpu.roll(far, 4, 0)).astype(BF16)
    odd = jnp.where(line < 4, pltpu.roll(near, rest - 4, 0), far).astype(BF16)
    for b in range(rest // 8):
        out[b * 16 : b * 16 + 8, wide:] = even[b * 8 : (b + 1) * 8]
        out[b * 16 + 8 : b * 16 + 16, wide:] = odd[b * 8 : (b + 1) * 8]


VMEM = pl.BlockSpec(memory_space=pltpu.VMEM)
SMEM = pl.BlockSpec(memory_space=pltpu.SMEM)


def pack_overflow(counts, where, q, p, pos):
    width = q.shape[1]
    half = pl.BlockSpec((LOW, width), lambda i: (1, 0))
    return pl.pallas_call(
        pack_kernel,
        grid=(1,),
        in_specs=[SMEM, SMEM, half, half, pl.BlockSpec((2, LOW), lambda i: (0, 0))],
        out_specs=[pl.BlockSpec((16, UNIT, 2 * width + LOW), lambda i: (0, 0, 0)), SMEM],
        out_shape=[
            jax.ShapeDtypeStruct((16, UNIT, 2 * width + LOW), BF16),
            jax.ShapeDtypeStruct((1,), jnp.int32),
        ],
        name="pack_overflow",
    )(counts, where, q, p, pos)


def tail_rows(heavy_at, arrived, base_p, pos, w_first, w_second):
    emb_width = w_second.shape[1]
    return pl.pallas_call(
        tail_kernel,
        in_specs=[SMEM] + [VMEM] * 5,
        out_specs=[VMEM] * 2,
        out_shape=[
            jax.ShapeDtypeStruct((16, BLOCK, emb_width), BF16),
            jax.ShapeDtypeStruct((2 * UNIT, emb_width + w_first.shape[0]), BF16),
        ],
        name="tail_rows",
    )(heavy_at, arrived, base_p, pos, w_first, w_second)


def hidden_units(blocks, tails, first):
    rows = jax.ShapeDtypeStruct((8 * BLOCK, first.shape[1]), BF16)
    hidden = jax.ShapeDtypeStruct((first.shape[0], 8 * BLOCK), BF16)
    slope = jax.ShapeDtypeStruct((first.shape[0], 8 * BLOCK), F32)
    rows_q, rows_p, hidden_q, hidden_p, slope_q, slope_p = pl.pallas_call(
        units_kernel,
        in_specs=[VMEM] * 11,
        out_specs=[VMEM] * 6,
        out_shape=[rows, rows, hidden, hidden, slope, slope],
        name="hidden_units",
    )(*blocks, *tails, first)
    return ((rows_q, hidden_q, slope_q), (rows_p, hidden_p, slope_p))


def score_stats(sc, qs, ts, p, scale):
    width = p.shape[1]
    rows = 8 * BLOCK
    return pl.pallas_call(
        functools.partial(stats_kernel, scale=scale),
        in_specs=[SMEM] + [VMEM] * 5,
        out_specs=[VMEM] * 3,
        out_shape=[
            jax.ShapeDtypeStruct((rows, width), BF16),
            jax.ShapeDtypeStruct((1, rows), jnp.int32),
            jax.ShapeDtypeStruct((64, rows), F32),
        ],
        scratch_shapes=[pltpu.VMEM((8, LOW, width), BF16), pltpu.VMEM((8, 16, width), BF16)],
        name="score_stats",
    )(sc, *qs, *ts, p)


def score_grads(stats, q, p, place, scale):
    columns, width = p.shape
    rows = q.shape[0]
    return pl.pallas_call(
        functools.partial(grads_kernel, scale=scale),
        in_specs=[VMEM] * 4,
        out_specs=[VMEM] * 2,
        out_shape=[
            jax.ShapeDtypeStruct((columns // BLOCK * CHUNK, width), BF16),
            jax.ShapeDtypeStruct((columns, rows), BF16),
        ],
        name="score_grads",
    )(stats, q, p, place)


def query_grads(sc, p, g, scale):
    columns, width = p.shape
    return pl.pallas_call(
        functools.partial(query_kernel, scale=scale),
        in_specs=[SMEM] + [VMEM] * 2,
        out_specs=[VMEM] * 2,
        out_shape=[jax.ShapeDtypeStruct((4, BLOCK, width), F32)] * 2,
        scratch_shapes=[pltpu.VMEM((width, columns), BF16)],
        name="query_grads",
    )(sc, p, g)


def weight_grads(sums, des, rows, hidden, slope, second):
    scratch = [pltpu.VMEM((8 * BLOCK, second.shape[1]), BF16)]
    operands = (*des, rows, hidden, slope, second)
    if sums is None:
        shape = (second.shape[0], rows.shape[1] + second.shape[1])
        return pl.pallas_call(
            first_weights_kernel,
            in_specs=[VMEM] * 6,
            out_specs=VMEM,
            out_shape=jax.ShapeDtypeStruct(shape, F32),
            scratch_shapes=scratch,
            name="first_weights",
        )(*operands)
    return pl.pallas_call(
        last_weights_kernel,
        in_specs=[VMEM] * 7,
        out_specs=VMEM,
        out_shape=jax.ShapeDtypeStruct((128, 1792), BF16),
        scratch_shapes=scratch,
        name="last_weights",
    )(sums, *operands)


def body(query_features, passage_features, counts, positives, w_first, w_second):
    width = query_features.shape[1]
    hidden_width, emb_width = w_second.shape
    scale = 2.5 * emb_width ** (-0.5)
    group = lax.axis_index((LINE, CORE))
    pairs = BLOCK * lax.axis_size(DP)

    pos = positives.reshape(2, LOW)
    where = jnp.reshape(group, (1,)).astype(jnp.int32)
    over, heavy_at = pack_overflow(counts, where, query_features, passage_features, pos)
    over = over.reshape(16 * UNIT, -1)
    arrived = plane_exchange(over)

    def tower(x):
        pre = jnp.dot(x, w_first, preferred_element_type=F32)
        hidden = gelu_tanh(pre).astype(BF16)
        return jnp.dot(hidden, w_second, preferred_element_type=F32).astype(BF16)

    feats = jnp.concatenate([query_features[:LOW], passage_features[:LOW]], axis=0)
    base = tower(feats)
    qs = gathered(base[:LOW])

    feats = along_line(feats)
    feats = feats + [swap_core(x) for x in feats]

    p_send, q_tail = tail_rows(
        heavy_at, arrived.reshape(16, UNIT, -1), base[LOW:], pos, w_first, w_second
    )
    p_all = plane_exchange(p_send.reshape(16 * BLOCK, emb_width))
    ts = gathered(q_tail)

    late_counts, group, _ = lax.optimization_barrier((counts, group, q_tail))
    heavy = (late_counts > LOW).astype(jnp.int32)
    devices = jnp.arange(counts.shape[0], dtype=jnp.int32)
    mine = heavy * (devices % 8 == group)
    offsets = jnp.cumsum(late_counts) - late_counts
    over_start = jnp.sum(mine * offsets) + LOW
    group_start = lax.dynamic_slice_in_dim(offsets.reshape(16, 8), group, 1, 1)[:, 0]
    scalars = [heavy_at[0], over_start, lax.axis_index(LINE), lax.axis_index(CORE)]
    scalars = jnp.stack(scalars + [lax.axis_index(PLANE)])
    heavies = jnp.sum(heavy.reshape(16, 8) * jnp.arange(16, dtype=jnp.int32)[:, None], axis=0)
    sc = jnp.concatenate([group_start, scalars, heavies]).astype(jnp.int32)

    each = hidden_width // lax.axis_size(DP)
    unit = jnp.arange(16 * each, dtype=jnp.int32)
    rest = unit - LOW
    unit_of = jnp.where(
        unit < LOW, (unit // 8) * (8 * each) + unit % 8, (rest // 4) * (8 * each) + 8 + rest % 4
    )
    unit_of = unit_of + group * each
    pick = (unit_of[:, None] == jnp.arange(hidden_width, dtype=jnp.int32)[None, :]).astype(BF16)
    first_part = lax.dot_general(
        pick, w_first, (((1,), (1,)), ((), ())), preferred_element_type=F32
    ).astype(BF16)
    second_part = jnp.dot(pick, w_second, preferred_element_type=F32).astype(BF16)
    q_units, p_units = hidden_units(feats, ts, first_part)
    p_all, second_part = lax.optimization_barrier((p_all, second_part))

    q_all, place, stats = score_stats(sc, qs, ts, p_all, scale)
    stats = stats_exchange(stats)
    dp_part, g = score_grads(stats, q_all, p_all, place, scale)
    dp_all = plane_exchange(dp_part)
    dq_own, dq_far = query_grads(sc, p_all, g, scale)

    dq = dq_own + swap_core(dq_far)
    dq_sum = dq[0].astype(BF16).astype(F32)
    for k in (1, 2, 3):
        dq_sum = dq_sum + to_line(dq[k].astype(BF16), k).astype(F32)
    dqs = gathered(dq_sum.astype(BF16))

    dp_sum = jnp.sum(dp_all.reshape(16, CHUNK, emb_width).astype(F32), axis=0)
    mean_loss = (dp_sum[BLOCK, 0] + dp_sum[BLOCK + 1, 0] + dp_sum[BLOCK + 2, 0]) / pairs
    dps = gathered(dp_sum[:BLOCK].astype(BF16))
    sums = weight_grads(None, dqs, *q_units, second_part)
    grads = weight_grads(sums, dps, *p_units, second_part)
    out = jnp.sum(plane_exchange(grads).reshape(16, 8, -1).astype(F32), axis=0)
    wide = width + emb_width
    tail_out = jnp.concatenate([out[:4, wide:], out[4:, wide : 2 * wide - 640]], axis=1)
    out = jnp.concatenate([out[:, :wide], tail_out], axis=0)
    return (mean_loss, out[:, :width].T, out[:, width:])


def solution(mesh):
    finer = Mesh(mesh.devices.reshape(4, 4, 4, 2), DP)
    placed = (P(DP, None), P(DP, None), P(), P(DP), P(), P())
    return jax.shard_map(
        body,
        mesh=finer,
        in_specs=placed,
        out_specs=(P(), P(None, DP), P(DP, None)),
        check_vma=False,
    )
```

```python
import functools

import jax
import jax.numpy as jnp
from jax import lax
from jax.experimental import pallas as pl
from jax.experimental.pallas import tpu as pltpu
from jax.sharding import Mesh
from jax.sharding import PartitionSpec as P

DP = ("dp_0", "dp_1", "dp_2", "dp_3")
PLANE = ("dp_0", "dp_1")
LINE = "dp_2"
CORE = "dp_3"
F32 = jnp.float32
BF16 = jnp.bfloat16

LOW = 128
UNIT = 8
BLOCK = LOW + UNIT
CHUNK = 144
PAIR = 2 * BLOCK
TILE = 256
LOG2E = 1.4426950408889634


def gelu_tanh(values):
    return jax.nn.gelu(values, approximate=True)


def swap_core(x):
    return lax.ppermute(x, CORE, [(0, 1), (1, 0)])


def plane_exchange(x):
    return lax.all_to_all(x, PLANE, 0, 0, tiled=True)


def stats_exchange(x):
    return lax.all_to_all(x, (LINE, CORE), 0, 0, tiled=True)


def from_line(x, k):
    return lax.ppermute(x, LINE, [((i + k) % 4, i) for i in range(4)])


def to_line(x, k):
    return lax.ppermute(x, LINE, [(i, (i + k) % 4) for i in range(4)])


def along_line(x):
    return [x] + [from_line(x, k) for k in (1, 2, 3)]


def gathered(x):
    own = jnp.concatenate(along_line(x), axis=0)
    return (own, swap_core(own))


def place_of(pos, sc):
    over = pos - sc[17]
    slot = jnp.bitwise_and(lax.shift_right_logical(over, 3) + sc[16], 15)
    place = jnp.where(
        (over >= 0) & (over < LOW), slot * BLOCK + LOW + jnp.bitwise_and(over, 7), -1
    )
    for s in range(16):
        at = pos - sc[s]
        place = jnp.where((at >= 0) & (at < LOW), at + s * BLOCK, place)
    return place


def near_index(sc, j):
    return jnp.bitwise_and(j // 2 - sc[18], 3) + 4 * jnp.bitwise_xor(j % 2, sc[19])


def nt_dot(a, b):
    return lax.dot_general(a, b, (((1,), (1,)), ((), ())), preferred_element_type=F32)


def pack_kernel(counts, where, q, p, pos, out, heavy_out):
    heavy_at = jnp.int32(0)
    for s in range(16):
        heavy_at += jnp.where(counts[s * 8 + where[0]] > LOW, s, 0)
    heavy_out[0] = heavy_at
    width = q.shape[1]
    high = lax.shift_right_logical(pos[1:2], 7).astype(F32)
    low = jnp.bitwise_and(pos[1:2], 127).astype(F32)
    line = lax.broadcasted_iota(jnp.int32, (UNIT, LOW), 0)
    code = jnp.where(line == 2, high, jnp.where(line == 3, low, 0.0)).astype(BF16)
    for u in range(16):
        slot = jnp.bitwise_and(heavy_at + u, 15)
        out[slot, :, :width] = q[u * UNIT : (u + 1) * UNIT]
        out[slot, :, width : 2 * width] = p[u * UNIT : (u + 1) * UNIT]
        out[slot, :, 2 * width :] = code


def gelu_parts(v):
    square = v * v
    t = jnp.tanh(0.7978845608028654 * (v + 0.044715 * (square * v)))
    grown = 0.5 * (1.0 + t)
    slope = grown + (0.5 * v) * (1.0 - t * t) * (
        0.7978845608028654 * (1.0 + 3 * 0.044715 * square)
    )
    return (v * grown, slope)


def tail_kernel(heavy_at, arrived, base_p, pos, w_first, w_second, p_out, q_out):
    width, emb_width = w_first.shape[0], w_second.shape[1]
    tail = arrived[heavy_at[0]]
    feats = jnp.concatenate([tail[:, :width], tail[:, width : 2 * width]], axis=0)
    q_out[:, emb_width:] = feats
    pre = jnp.dot(feats, w_first[...], preferred_element_type=F32)
    hidden = gelu_parts(pre)[0].astype(BF16)
    emb = jnp.dot(hidden, w_second[...], preferred_element_type=F32).astype(BF16)
    for s in range(p_out.shape[0]):
        p_out[s, :LOW] = base_p[...]
        p_out[s, LOW:] = emb[UNIT:]
    high = lax.shift_right_logical(pos[0:1], 7).astype(F32)
    low = jnp.bitwise_and(pos[0:1], 127).astype(F32)
    line = lax.broadcasted_iota(jnp.int32, (UNIT, LOW), 0)
    code = tail[:, 2 * width :].astype(F32)
    code = jnp.where(line == 0, high, jnp.where(line == 1, low, code)).astype(BF16)
    q_out[:UNIT, :emb_width] = emb[:UNIT]
    q_out[UNIT:, LOW:emb_width] = jnp.zeros((UNIT, emb_width - LOW), BF16)
    q_out[UNIT:, :LOW] = code


def units_kernel(*refs):
    blocks, tails, (first, rows_q, rows_p, hidden_q, hidden_p, slope_q, slope_p) = (
        refs[:8],
        refs[8:10],
        refs[10:],
    )
    skip = tails[0].shape[1] - rows_q.shape[1]
    for k, block in enumerate(blocks):
        tail = tails[k // 4][(k % 4) * 2 * UNIT : (k % 4 + 1) * 2 * UNIT, skip:]
        at = k * BLOCK
        rows_q[at : at + LOW] = block[:LOW]
        rows_q[at + LOW : at + BLOCK] = tail[:UNIT]
        rows_p[at : at + LOW] = block[LOW:]
        rows_p[at + LOW : at + BLOCK] = tail[UNIT:]
    for rows, hidden, slope in ((rows_q, hidden_q, slope_q), (rows_p, hidden_p, slope_p)):
        value, gain = gelu_parts(nt_dot(first[...], rows[...]))
        hidden[...] = value.astype(BF16)
        slope[...] = gain


def stats_kernel(
    sc, q_own, q_far, t_own, t_far, p, q_out, place_out, stats_out, qs, ts, *, scale
):
    for k, (q, t) in enumerate(((q_own, t_own), (q_far, t_far))):
        for b in range(4):
            qs[4 * k + b] = q[b * LOW : (b + 1) * LOW]
            ts[4 * k + b] = t[b * 16 : (b + 1) * 16, : p.shape[1]]
    lane = lax.broadcasted_iota(jnp.int32, (1, LOW), 1) // UNIT
    codes = []
    spread = jnp.zeros((1, LOW), F32)
    for j in range(8):
        b = near_index(sc, j)
        q_out[j * LOW : (j + 1) * LOW] = qs[b]
        tail = ts[b]
        q_out[8 * LOW + j * UNIT : 8 * LOW + (j + 1) * UNIT] = tail[:UNIT]
        code = tail[UNIT:, :LOW].astype(F32)
        codes.append(code[0:1] * 128.0 + code[1:2])
        unit = jnp.bitwise_and(sc[20] - sc[21 + j], 15)
        part = pltpu.roll(code, jnp.bitwise_and(j - unit, 15) * UNIT, 1)
        spread = jnp.where(lane == j, part[2:3] * 128.0 + part[3:4], spread)
    codes.append(spread[:, : 8 * UNIT])
    place_out[...] = place_of(jnp.concatenate(codes, axis=1).astype(jnp.int32), sc)
    rows = q_out.shape[0]
    pull = scale * LOG2E
    top = jnp.full((1, rows), -1e30, F32)
    total = jnp.zeros((1, rows), F32)
    found = jnp.zeros((1, rows), F32)
    for at in range(0, p.shape[0], PAIR):
        tile = p[at : at + PAIR]
        s = nt_dot(tile, q_out[...])
        row = lax.broadcasted_iota(jnp.int32, s.shape, 0)
        found += jnp.sum(jnp.where(row == place_out[...] - at, s, 0.0), axis=0, keepdims=True)
        new_top = jnp.maximum(top, jnp.max(s, axis=0, keepdims=True))
        total = total * jnp.exp2((top - new_top) * pull) + jnp.sum(
            jnp.exp2(s * pull - new_top * pull), axis=0, keepdims=True
        )
        top = new_top
    line = lax.broadcasted_iota(jnp.int32, (8, rows), 0)
    stats = jnp.where(line == 0, top, jnp.where(line == 1, total, jnp.where(line == 2, found, 0.0)))
    for b in range(8):
        stats_out[b * 8 : (b + 1) * 8] = stats


def grads_kernel(stats, q, p, place, dp_out, g_out, dp_ref, g_ref, sems, *, scale):
    rows, width = q.shape
    pull = scale * LOG2E
    tops = [stats[b * 8 : b * 8 + 1] for b in range(8)]
    top = functools.reduce(jnp.maximum, tops)
    total = jnp.zeros((1, rows), F32)
    found = jnp.zeros((1, rows), F32)
    for b in range(8):
        total += stats[b * 8 + 1 : b * 8 + 2] * jnp.exp2((tops[b] - top) * pull)
        found += stats[b * 8 + 2 : b * 8 + 3]
    norm = top * scale + jnp.log(total)
    loss = jnp.sum(norm - found * scale, axis=1, keepdims=True)
    norm = norm * LOG2E
    loss_high = loss.astype(BF16).astype(F32)
    loss_mid = (loss - loss_high).astype(BF16).astype(F32)
    loss_low = loss - loss_high - loss_mid
    line = lax.broadcasted_iota(jnp.int32, (UNIT, width), 0)
    loss_tile = jnp.where(
        line == 0,
        loss_high,
        jnp.where(line == 1, loss_mid, jnp.where(line == 2, loss_low, 0.0)),
    ).astype(BF16)
    copies = []

    def send(src, dst, rows):
        copy = pltpu.make_async_copy(src.at[rows], dst.at[rows], sems.at[len(copies)])
        copy.start()
        copies.append(copy)

    for at in range(0, p.shape[0], PAIR):
        s = nt_dot(p[at : at + PAIR], q[...])
        row = lax.broadcasted_iota(jnp.int32, s.shape, 0)
        e = jnp.exp2(s * pull - norm)
        g_ref[at : at + PAIR] = jnp.where(row == place[...] - at, e - 1.0, e).astype(BF16)
        send(g_ref, g_out, pl.ds(at, PAIR))
    for k in range(p.shape[0] // PAIR):
        dp = scale * jnp.dot(g_ref[k * PAIR : (k + 1) * PAIR], q[...], preferred_element_type=F32)
        dp = dp.astype(BF16)
        for half in range(2):
            to = (2 * k + half) * CHUNK
            dp_ref[to : to + BLOCK] = dp[half * BLOCK : (half + 1) * BLOCK]
            dp_ref[to + BLOCK : to + CHUNK] = loss_tile
        send(dp_ref, dp_out, pl.ds(2 * k * CHUNK, 2 * CHUNK))
    for copy in copies:
        copy.wait()


def query_kernel(sc, p, g_in, own, far, turned, g, sems, *, scale):
    cut = p.shape[0] // 2 // TILE * TILE
    spans = (pl.ds(0, cut), pl.ds(cut, p.shape[0] - cut))
    copies = [
        pltpu.make_async_copy(g_in.at[span], g.at[span], sems.at[k]) for k, span in enumerate(spans)
    ]
    for copy in copies:
        copy.start()
    for at in range(0, p.shape[0], LOW):
        turned[:, at : at + LOW] = p[at : at + LOW].T

    def put(j, rows, part):
        b = near_index(sc, j)

        @pl.when(b < 4)
        def _():
            own[b, rows] = part

        @pl.when(b >= 4)
        def _():
            far[b - 4, rows] = part

    copies[0].wait()
    early = jnp.dot(turned[:, :cut], g[:cut], preferred_element_type=F32)
    copies[1].wait()
    dq = early + jnp.dot(turned[:, cut:], g[cut:], preferred_element_type=F32)
    dq = (scale * dq).T
    for j in range(8):
        put(j, slice(0, LOW), dq[j * LOW : (j + 1) * LOW])
    dq = dq[8 * LOW :]
    for j in range(8):
        put(j, slice(LOW, BLOCK), dq[j * UNIT : (j + 1) * UNIT])


def weight_parts(de_own, de_far, rows, hidden, slope, second, de):
    half = de_own.shape[0]
    de[:half] = de_own[...]
    de[half:] = de_far[...]
    grad_second = jnp.dot(hidden[...], de[...], preferred_element_type=F32)
    dpre = (slope[...] * nt_dot(second[...], de[...])).astype(BF16)
    grad_first = jnp.dot(dpre, rows[...], preferred_element_type=F32)
    return (grad_first, grad_second)


def first_weights_kernel(de_own, de_far, rows, hidden, slope, second, out, de):
    grad_first, grad_second = weight_parts(de_own, de_far, rows, hidden, slope, second, de)
    out[:, : rows.shape[1]] = grad_first
    out[:, rows.shape[1] :] = grad_second


def last_weights_kernel(sums, de_own, de_far, rows, hidden, slope, second, out, de):
    grad_first, grad_second = weight_parts(de_own, de_far, rows, hidden, slope, second, de)
    grad_first += sums[:, : rows.shape[1]]
    grad_second += sums[:, rows.shape[1] :]
    many = out.shape[0]
    wide = sums.shape[1]
    out[:, : rows.shape[1]] = grad_first[:many].astype(BF16)
    out[:, rows.shape[1] : wide] = grad_second[:many].astype(BF16)
    rest = grad_first.shape[0] - many
    x = jnp.concatenate(
        [grad_first[many:], grad_second[many:], jnp.zeros((rest, 128), F32)], axis=1
    )
    near, far = x[:, :640], x[:, 640:]
    line = jnp.bitwise_and(lax.broadcasted_iota(jnp.int32, near.shape, 0), 7)
    even = jnp.where(line < 4, near, pltpu.roll(far, 4, 0)).astype(BF16)
    odd = jnp.where(line < 4, pltpu.roll(near, rest - 4, 0), far).astype(BF16)
    for b in range(rest // 8):
        out[b * 16 : b * 16 + 8, wide:] = even[b * 8 : (b + 1) * 8]
        out[b * 16 + 8 : b * 16 + 16, wide:] = odd[b * 8 : (b + 1) * 8]


VMEM = pl.BlockSpec(memory_space=pltpu.VMEM)
SMEM = pl.BlockSpec(memory_space=pltpu.SMEM)
HBM = pl.BlockSpec(memory_space=pltpu.HBM)


def pack_overflow(counts, where, q, p, pos):
    width = q.shape[1]
    half = pl.BlockSpec((LOW, width), lambda i: (1, 0))
    return pl.pallas_call(
        pack_kernel,
        grid=(1,),
        in_specs=[SMEM, SMEM, half, half, pl.BlockSpec((2, LOW), lambda i: (0, 0))],
        out_specs=[pl.BlockSpec((16, UNIT, 2 * width + LOW), lambda i: (0, 0, 0)), SMEM],
        out_shape=[
            jax.ShapeDtypeStruct((16, UNIT, 2 * width + LOW), BF16),
            jax.ShapeDtypeStruct((1,), jnp.int32),
        ],
        name="pack_overflow",
    )(counts, where, q, p, pos)


def tail_rows(heavy_at, arrived, base_p, pos, w_first, w_second):
    emb_width = w_second.shape[1]
    return pl.pallas_call(
        tail_kernel,
        in_specs=[SMEM] + [VMEM] * 5,
        out_specs=[VMEM] * 2,
        out_shape=[
            jax.ShapeDtypeStruct((16, BLOCK, emb_width), BF16),
            jax.ShapeDtypeStruct((2 * UNIT, emb_width + w_first.shape[0]), BF16),
        ],
        name="tail_rows",
    )(heavy_at, arrived, base_p, pos, w_first, w_second)


def hidden_units(blocks, tails, first):
    rows = jax.ShapeDtypeStruct((8 * BLOCK, first.shape[1]), BF16)
    hidden = jax.ShapeDtypeStruct((first.shape[0], 8 * BLOCK), BF16)
    slope = jax.ShapeDtypeStruct((first.shape[0], 8 * BLOCK), F32)
    rows_q, rows_p, hidden_q, hidden_p, slope_q, slope_p = pl.pallas_call(
        units_kernel,
        in_specs=[VMEM] * 11,
        out_specs=[VMEM] * 6,
        out_shape=[rows, rows, hidden, hidden, slope, slope],
        name="hidden_units",
    )(*blocks, *tails, first)
    return ((rows_q, hidden_q, slope_q), (rows_p, hidden_p, slope_p))


def score_stats(sc, qs, ts, p, scale):
    width = p.shape[1]
    rows = 8 * BLOCK
    return pl.pallas_call(
        functools.partial(stats_kernel, scale=scale),
        in_specs=[SMEM] + [VMEM] * 5,
        out_specs=[VMEM] * 3,
        out_shape=[
            jax.ShapeDtypeStruct((rows, width), BF16),
            jax.ShapeDtypeStruct((1, rows), jnp.int32),
            jax.ShapeDtypeStruct((64, rows), F32),
        ],
        scratch_shapes=[pltpu.VMEM((8, LOW, width), BF16), pltpu.VMEM((8, 16, width), BF16)],
        name="score_stats",
    )(sc, *qs, *ts, p)


def score_grads(stats, q, p, place, scale):
    columns, width = p.shape
    rows = q.shape[0]
    steps = columns // PAIR
    return pl.pallas_call(
        functools.partial(grads_kernel, scale=scale),
        in_specs=[VMEM] * 4,
        out_specs=[HBM] * 2,
        out_shape=[
            jax.ShapeDtypeStruct((2 * steps * CHUNK, width), BF16),
            jax.ShapeDtypeStruct((columns, rows), BF16),
        ],
        scratch_shapes=[
            pltpu.VMEM((2 * steps * CHUNK, width), BF16),
            pltpu.VMEM((columns, rows), BF16),
            pltpu.SemaphoreType.DMA((2 * steps,)),
        ],
        name="score_grads",
    )(stats, q, p, place)


def query_grads(sc, p, g, scale):
    columns, width = p.shape
    return pl.pallas_call(
        functools.partial(query_kernel, scale=scale),
        in_specs=[SMEM, VMEM, HBM],
        out_specs=[VMEM] * 2,
        out_shape=[jax.ShapeDtypeStruct((4, BLOCK, width), F32)] * 2,
        scratch_shapes=[
            pltpu.VMEM((width, columns), BF16),
            pltpu.VMEM(g.shape, BF16),
            pltpu.SemaphoreType.DMA((2,)),
        ],
        name="query_grads",
    )(sc, p, g)


def weight_grads(sums, des, rows, hidden, slope, second):
    scratch = [pltpu.VMEM((8 * BLOCK, second.shape[1]), BF16)]
    operands = (*des, rows, hidden, slope, second)
    if sums is None:
        shape = (second.shape[0], rows.shape[1] + second.shape[1])
        return pl.pallas_call(
            first_weights_kernel,
            in_specs=[VMEM] * 6,
            out_specs=VMEM,
            out_shape=jax.ShapeDtypeStruct(shape, F32),
            scratch_shapes=scratch,
            name="first_weights",
        )(*operands)
    return pl.pallas_call(
        last_weights_kernel,
        in_specs=[VMEM] * 7,
        out_specs=VMEM,
        out_shape=jax.ShapeDtypeStruct((128, 1792), BF16),
        scratch_shapes=scratch,
        name="last_weights",
    )(sums, *operands)


def body(query_features, passage_features, counts, positives, w_first, w_second):
    width = query_features.shape[1]
    hidden_width, emb_width = w_second.shape
    scale = 2.5 * emb_width ** (-0.5)
    group = lax.axis_index((LINE, CORE))
    pairs = BLOCK * lax.axis_size(DP)

    pos = positives.reshape(2, LOW)
    where = jnp.reshape(group, (1,)).astype(jnp.int32)
    over, heavy_at = pack_overflow(counts, where, query_features, passage_features, pos)
    over = over.reshape(16 * UNIT, -1)
    arrived = plane_exchange(over)

    def tower(x):
        pre = jnp.dot(x, w_first, preferred_element_type=F32)
        hidden = gelu_tanh(pre).astype(BF16)
        return jnp.dot(hidden, w_second, preferred_element_type=F32).astype(BF16)

    feats = jnp.concatenate([query_features[:LOW], passage_features[:LOW]], axis=0)
    base = tower(feats)
    qs = gathered(base[:LOW])

    feats = along_line(feats)
    feats = feats + [swap_core(x) for x in feats]

    p_send, q_tail = tail_rows(
        heavy_at, arrived.reshape(16, UNIT, -1), base[LOW:], pos, w_first, w_second
    )
    p_all = plane_exchange(p_send.reshape(16 * BLOCK, emb_width))
    ts = gathered(q_tail)

    late_counts, group, _ = lax.optimization_barrier((counts, group, q_tail))
    heavy = (late_counts > LOW).astype(jnp.int32)
    devices = jnp.arange(counts.shape[0], dtype=jnp.int32)
    mine = heavy * (devices % 8 == group)
    offsets = jnp.cumsum(late_counts) - late_counts
    over_start = jnp.sum(mine * offsets) + LOW
    group_start = lax.dynamic_slice_in_dim(offsets.reshape(16, 8), group, 1, 1)[:, 0]
    scalars = [heavy_at[0], over_start, lax.axis_index(LINE), lax.axis_index(CORE)]
    scalars = jnp.stack(scalars + [lax.axis_index(PLANE)])
    heavies = jnp.sum(heavy.reshape(16, 8) * jnp.arange(16, dtype=jnp.int32)[:, None], axis=0)
    sc = jnp.concatenate([group_start, scalars, heavies]).astype(jnp.int32)

    each = hidden_width // lax.axis_size(DP)
    unit = jnp.arange(16 * each, dtype=jnp.int32)
    rest = unit - LOW
    unit_of = jnp.where(
        unit < LOW, (unit // 8) * (8 * each) + unit % 8, (rest // 4) * (8 * each) + 8 + rest % 4
    )
    unit_of = unit_of + group * each
    pick = (unit_of[:, None] == jnp.arange(hidden_width, dtype=jnp.int32)[None, :]).astype(BF16)
    first_part = lax.dot_general(
        pick, w_first, (((1,), (1,)), ((), ())), preferred_element_type=F32
    ).astype(BF16)
    second_part = jnp.dot(pick, w_second, preferred_element_type=F32).astype(BF16)
    p_all, first_part = lax.optimization_barrier((p_all, first_part))

    q_all, place, stats = score_stats(sc, qs, ts, p_all, scale)
    stats = stats_exchange(stats)
    q_units, p_units = hidden_units(feats, ts, first_part)
    dp_part, g = score_grads(stats, q_all, p_all, place, scale)
    dp_all = plane_exchange(dp_part)
    dq_own, dq_far = query_grads(sc, p_all, g, scale)

    dq = dq_own + swap_core(dq_far)
    dq_sum = dq[0].astype(BF16).astype(F32)
    for k in (1, 2, 3):
        dq_sum = dq_sum + to_line(dq[k].astype(BF16), k).astype(F32)
    dqs = gathered(dq_sum.astype(BF16))

    dp_sum = jnp.sum(dp_all.reshape(16, CHUNK, emb_width).astype(F32), axis=0)
    mean_loss = (dp_sum[BLOCK, 0] + dp_sum[BLOCK + 1, 0] + dp_sum[BLOCK + 2, 0]) / pairs
    dps = gathered(dp_sum[:BLOCK].astype(BF16))
    sums = weight_grads(None, dqs, *q_units, second_part)
    grads = weight_grads(sums, dps, *p_units, second_part)
    out = jnp.sum(plane_exchange(grads).reshape(16, 8, -1).astype(F32), axis=0)
    wide = width + emb_width
    tail_out = jnp.concatenate([out[:4, wide:], out[4:, wide : 2 * wide - 640]], axis=1)
    out = jnp.concatenate([out[:, :wide], tail_out], axis=0)
    return (mean_loss, out[:, :width].T, out[:, width:])


def solution(mesh):
    finer = Mesh(mesh.devices.reshape(4, 4, 4, 2), DP)
    placed = (P(DP, None), P(DP, None), P(), P(DP), P(), P())
    return jax.shard_map(
        body,
        mesh=finer,
        in_specs=placed,
        out_specs=(P(), P(None, DP), P(DP, None)),
        check_vma=False,
    )
```

```python
import functools

import jax
import jax.numpy as jnp
from jax import lax
from jax.experimental import pallas as pl
from jax.experimental.pallas import tpu as pltpu
from jax.sharding import Mesh
from jax.sharding import PartitionSpec as P


DP = ("dp_0", "dp_1", "dp_2", "dp_3")
PLANE = ("dp_0", "dp_1")
LINE = "dp_2"
CORE = "dp_3"
F32 = jnp.float32
BF16 = jnp.bfloat16

LOW = 128
UNIT = 8
BLOCK = LOW + UNIT
CHUNK = 144
PAIR = 2 * BLOCK
TILE = 256
LOG2E = 1.4426950408889634


def gelu_tanh(values):
    return jax.nn.gelu(values, approximate=True)


def swap_core(x):
    return lax.ppermute(x, CORE, [(0, 1), (1, 0)])


def plane_exchange(x):
    return lax.all_to_all(x, PLANE, 0, 0, tiled=True)


def stats_exchange(x):
    return lax.all_to_all(x, (LINE, CORE), 0, 0, tiled=True)


def from_line(x, k):
    return lax.ppermute(x, LINE, [((i + k) % 4, i) for i in range(4)])


def along_line(x):
    return [x] + [from_line(x, k) for k in (1, 2, 3)]


def gathered(x):
    own = jnp.concatenate(along_line(x), axis=0)
    return (own, swap_core(own))


def place_of(pos, sc):
    over = pos - sc[17]
    slot = jnp.bitwise_and(lax.shift_right_logical(over, 3) + sc[16], 15)
    place = jnp.where(
        (over >= 0) & (over < LOW), slot * BLOCK + LOW + jnp.bitwise_and(over, 7), -1
    )
    for s in range(16):
        at = pos - sc[s]
        place = jnp.where((at >= 0) & (at < LOW), at + s * BLOCK, place)
    return place


def near_index(sc, j):
    return jnp.bitwise_and(j // 2 - sc[18], 3) + 4 * jnp.bitwise_xor(j % 2, sc[19])


def nt_dot(a, b):
    return lax.dot_general(a, b, (((1,), (1,)), ((), ())), preferred_element_type=F32)


def pack_kernel(counts, where, q, p, pos, out, heavy_out):
    heavy_at = jnp.int32(0)
    for s in range(16):
        heavy_at += jnp.where(counts[s * 8 + where[0]] > LOW, s, 0)
    heavy_out[0] = heavy_at
    width = q.shape[1]
    high = lax.shift_right_logical(pos[1:2], 7).astype(F32)
    low = jnp.bitwise_and(pos[1:2], 127).astype(F32)
    line = lax.broadcasted_iota(jnp.int32, (UNIT, LOW), 0)
    code = jnp.where(line == 2, high, jnp.where(line == 3, low, 0.0)).astype(BF16)
    for u in range(16):
        slot = jnp.bitwise_and(heavy_at + u, 15)
        out[slot, :, :width] = q[u * UNIT : (u + 1) * UNIT]
        out[slot, :, width : 2 * width] = p[u * UNIT : (u + 1) * UNIT]
        out[slot, :, 2 * width :] = code


def gelu_parts(v):
    square = v * v
    t = jnp.tanh(0.7978845608028654 * (v + 0.044715 * (square * v)))
    grown = 0.5 * (1.0 + t)
    slope = grown + (0.5 * v) * (1.0 - t * t) * (
        0.7978845608028654 * (1.0 + 3 * 0.044715 * square)
    )
    return (v * grown, slope)


def tail_kernel(heavy_at, arrived, base_p, pos, w_first, w_second, p_out, q_out):
    width, emb_width = w_first.shape[0], w_second.shape[1]
    tail = arrived[heavy_at[0]]
    feats = jnp.concatenate([tail[:, :width], tail[:, width : 2 * width]], axis=0)
    q_out[:, emb_width:] = feats
    pre = jnp.dot(feats, w_first[...], preferred_element_type=F32)
    hidden = gelu_parts(pre)[0].astype(BF16)
    emb = jnp.dot(hidden, w_second[...], preferred_element_type=F32).astype(BF16)
    for s in range(p_out.shape[0]):
        p_out[s, :LOW] = base_p[...]
        p_out[s, LOW:] = emb[UNIT:]
    high = lax.shift_right_logical(pos[0:1], 7).astype(F32)
    low = jnp.bitwise_and(pos[0:1], 127).astype(F32)
    line = lax.broadcasted_iota(jnp.int32, (UNIT, LOW), 0)
    code = tail[:, 2 * width :].astype(F32)
    code = jnp.where(line == 0, high, jnp.where(line == 1, low, code)).astype(BF16)
    q_out[:UNIT, :emb_width] = emb[:UNIT]
    q_out[UNIT:, LOW:emb_width] = jnp.zeros((UNIT, emb_width - LOW), BF16)
    q_out[UNIT:, :LOW] = code


def units_kernel(*refs):
    blocks, tails, (first, rows_q, rows_p, hidden_q, hidden_p, slope_q, slope_p) = (
        refs[:8],
        refs[8:10],
        refs[10:],
    )
    skip = tails[0].shape[1] - rows_q.shape[1]
    for k, block in enumerate(blocks):
        tail = tails[k // 4][(k % 4) * 2 * UNIT : (k % 4 + 1) * 2 * UNIT, skip:]
        at = k * BLOCK
        rows_q[at : at + LOW] = block[:LOW]
        rows_q[at + LOW : at + BLOCK] = tail[:UNIT]
        rows_p[at : at + LOW] = block[LOW:]
        rows_p[at + LOW : at + BLOCK] = tail[UNIT:]
    for rows, hidden, slope in ((rows_q, hidden_q, slope_q), (rows_p, hidden_p, slope_p)):
        value, gain = gelu_parts(nt_dot(first[...], rows[...]))
        hidden[...] = value.astype(BF16)
        slope[...] = gain


def stats_kernel(
    sc, q_own, q_far, t_own, t_far, p, q_out, place_out, stats_out, qs, ts, *, scale
):
    for k, (q, t) in enumerate(((q_own, t_own), (q_far, t_far))):
        for b in range(4):
            qs[4 * k + b] = q[b * LOW : (b + 1) * LOW]
            ts[4 * k + b] = t[b * 16 : (b + 1) * 16, : p.shape[1]]
    lane = lax.broadcasted_iota(jnp.int32, (1, LOW), 1) // UNIT
    codes = []
    spread = jnp.zeros((1, LOW), F32)
    for j in range(8):
        b = near_index(sc, j)
        q_out[j * LOW : (j + 1) * LOW] = qs[b]
        tail = ts[b]
        q_out[8 * LOW + j * UNIT : 8 * LOW + (j + 1) * UNIT] = tail[:UNIT]
        code = tail[UNIT:, :LOW].astype(F32)
        codes.append(code[0:1] * 128.0 + code[1:2])
        unit = jnp.bitwise_and(sc[20] - sc[21 + j], 15)
        part = pltpu.roll(code, jnp.bitwise_and(j - unit, 15) * UNIT, 1)
        spread = jnp.where(lane == j, part[2:3] * 128.0 + part[3:4], spread)
    codes.append(spread[:, : 8 * UNIT])
    place_out[...] = place_of(jnp.concatenate(codes, axis=1).astype(jnp.int32), sc)
    rows = q_out.shape[0]
    pull = scale * LOG2E
    top = jnp.full((1, rows), -1e30, F32)
    total = jnp.zeros((1, rows), F32)
    found = jnp.zeros((1, rows), F32)
    for at in range(0, p.shape[0], PAIR):
        tile = p[at : at + PAIR]
        s = nt_dot(tile, q_out[...])
        row = lax.broadcasted_iota(jnp.int32, s.shape, 0)
        found += jnp.sum(jnp.where(row == place_out[...] - at, s, 0.0), axis=0, keepdims=True)
        new_top = jnp.maximum(top, jnp.max(s, axis=0, keepdims=True))
        total = total * jnp.exp2((top - new_top) * pull) + jnp.sum(
            jnp.exp2(s * pull - new_top * pull), axis=0, keepdims=True
        )
        top = new_top
    line = lax.broadcasted_iota(jnp.int32, (8, rows), 0)
    stats = jnp.where(line == 0, top, jnp.where(line == 1, total, jnp.where(line == 2, found, 0.0)))
    for b in range(8):
        stats_out[b * 8 : (b + 1) * 8] = stats


def grads_kernel(stats, q, p, place, dp_out, g_out, dp_ref, g_ref, sems, *, scale):
    rows, width = q.shape
    pull = scale * LOG2E
    tops = [stats[b * 8 : b * 8 + 1] for b in range(8)]
    top = functools.reduce(jnp.maximum, tops)
    total = jnp.zeros((1, rows), F32)
    found = jnp.zeros((1, rows), F32)
    for b in range(8):
        total += stats[b * 8 + 1 : b * 8 + 2] * jnp.exp2((tops[b] - top) * pull)
        found += stats[b * 8 + 2 : b * 8 + 3]
    norm = top * scale + jnp.log(total)
    loss = jnp.sum(norm - found * scale, axis=1, keepdims=True)
    norm = norm * LOG2E
    loss_high = loss.astype(BF16).astype(F32)
    loss_mid = (loss - loss_high).astype(BF16).astype(F32)
    loss_low = loss - loss_high - loss_mid
    line = lax.broadcasted_iota(jnp.int32, (UNIT, width), 0)
    loss_tile = jnp.where(
        line == 0,
        loss_high,
        jnp.where(line == 1, loss_mid, jnp.where(line == 2, loss_low, 0.0)),
    ).astype(BF16)
    copies = []

    def send(src, dst, rows):
        copy = pltpu.make_async_copy(src.at[rows], dst.at[rows], sems.at[len(copies)])
        copy.start()
        copies.append(copy)

    for at in range(0, p.shape[0], PAIR):
        s = nt_dot(p[at : at + PAIR], q[...])
        row = lax.broadcasted_iota(jnp.int32, s.shape, 0)
        e = jnp.exp2(s * pull - norm)
        g_ref[at : at + PAIR] = jnp.where(row == place[...] - at, e - 1.0, e).astype(BF16)
        send(g_ref, g_out, pl.ds(at, PAIR))
    for k in range(p.shape[0] // PAIR):
        dp = scale * jnp.dot(g_ref[k * PAIR : (k + 1) * PAIR], q[...], preferred_element_type=F32)
        dp = dp.astype(BF16)
        for half in range(2):
            to = (2 * k + half) * CHUNK
            dp_ref[to : to + BLOCK] = dp[half * BLOCK : (half + 1) * BLOCK]
            dp_ref[to + BLOCK : to + CHUNK] = loss_tile
        send(dp_ref, dp_out, pl.ds(2 * k * CHUNK, 2 * CHUNK))
    for copy in copies:
        copy.wait()


def query_kernel(sc, p, g_in, own, far, turned, g, sems, *, scale):
    cut = p.shape[0] // 2 // TILE * TILE
    spans = (pl.ds(0, cut), pl.ds(cut, p.shape[0] - cut))
    copies = [
        pltpu.make_async_copy(g_in.at[span], g.at[span], sems.at[k]) for k, span in enumerate(spans)
    ]
    for copy in copies:
        copy.start()
    for at in range(0, p.shape[0], LOW):
        turned[:, at : at + LOW] = p[at : at + LOW].T

    def put(j, rows, part):
        b = near_index(sc, j)

        @pl.when(b < 4)
        def _():
            own[b, rows] = part

        @pl.when(b >= 4)
        def _():
            far[b - 4, rows] = part

    copies[0].wait()
    early = jnp.dot(turned[:, :cut], g[:cut], preferred_element_type=F32)
    copies[1].wait()
    dq = early + jnp.dot(turned[:, cut:], g[cut:], preferred_element_type=F32)
    dq = (scale * dq).T
    for j in range(8):
        put(j, slice(0, LOW), dq[j * LOW : (j + 1) * LOW])
    dq = dq[8 * LOW :]
    for j in range(8):
        put(j, slice(LOW, BLOCK), dq[j * UNIT : (j + 1) * UNIT])


def total_kernel(*refs):
    parts, out = refs[:4], refs[4]
    for b in range(4):
        blocks = [part[(b - k) % 4].astype(F32) for k, part in enumerate(parts)]
        total = (blocks[0] + blocks[1]) + (blocks[2] + blocks[3])
        out[b * BLOCK : (b + 1) * BLOCK] = total.astype(BF16)


def weight_parts(de_own, de_far, rows, hidden, slope, second, de):
    half = de_own.shape[0]
    de[:half] = de_own[...]
    de[half:] = de_far[...]
    grad_second = jnp.dot(hidden[...], de[...], preferred_element_type=F32)
    dpre = (slope[...] * nt_dot(second[...], de[...])).astype(BF16)
    grad_first = jnp.dot(dpre, rows[...], preferred_element_type=F32)
    return (grad_first, grad_second)


def first_weights_kernel(de_own, de_far, rows, hidden, slope, second, out, de):
    grad_first, grad_second = weight_parts(de_own, de_far, rows, hidden, slope, second, de)
    out[:, : rows.shape[1]] = grad_first
    out[:, rows.shape[1] :] = grad_second


def last_weights_kernel(sums, de_own, de_far, rows, hidden, slope, second, out, de):
    grad_first, grad_second = weight_parts(de_own, de_far, rows, hidden, slope, second, de)
    grad_first += sums[:, : rows.shape[1]]
    grad_second += sums[:, rows.shape[1] :]
    many = out.shape[0]
    wide = sums.shape[1]
    out[:, : rows.shape[1]] = grad_first[:many].astype(BF16)
    out[:, rows.shape[1] : wide] = grad_second[:many].astype(BF16)
    rest = grad_first.shape[0] - many
    x = jnp.concatenate(
        [grad_first[many:], grad_second[many:], jnp.zeros((rest, 128), F32)], axis=1
    )
    near, far = x[:, :640], x[:, 640:]
    line = jnp.bitwise_and(lax.broadcasted_iota(jnp.int32, near.shape, 0), 7)
    even = jnp.where(line < 4, near, pltpu.roll(far, 4, 0)).astype(BF16)
    odd = jnp.where(line < 4, pltpu.roll(near, rest - 4, 0), far).astype(BF16)
    for b in range(rest // 8):
        out[b * 16 : b * 16 + 8, wide:] = even[b * 8 : (b + 1) * 8]
        out[b * 16 + 8 : b * 16 + 16, wide:] = odd[b * 8 : (b + 1) * 8]


VMEM = pl.BlockSpec(memory_space=pltpu.VMEM)
SMEM = pl.BlockSpec(memory_space=pltpu.SMEM)
HBM = pl.BlockSpec(memory_space=pltpu.HBM)


def pack_overflow(counts, where, q, p, pos):
    width = q.shape[1]
    half = pl.BlockSpec((LOW, width), lambda i: (1, 0))
    return pl.pallas_call(
        pack_kernel,
        grid=(1,),
        in_specs=[SMEM, SMEM, half, half, pl.BlockSpec((2, LOW), lambda i: (0, 0))],
        out_specs=[pl.BlockSpec((16, UNIT, 2 * width + LOW), lambda i: (0, 0, 0)), SMEM],
        out_shape=[
            jax.ShapeDtypeStruct((16, UNIT, 2 * width + LOW), BF16),
            jax.ShapeDtypeStruct((1,), jnp.int32),
        ],
        name="pack_overflow",
    )(counts, where, q, p, pos)


def tail_rows(heavy_at, arrived, base_p, pos, w_first, w_second):
    emb_width = w_second.shape[1]
    return pl.pallas_call(
        tail_kernel,
        in_specs=[SMEM] + [VMEM] * 5,
        out_specs=[VMEM] * 2,
        out_shape=[
            jax.ShapeDtypeStruct((16, BLOCK, emb_width), BF16),
            jax.ShapeDtypeStruct((2 * UNIT, emb_width + w_first.shape[0]), BF16),
        ],
        name="tail_rows",
    )(heavy_at, arrived, base_p, pos, w_first, w_second)


def hidden_units(blocks, tails, first):
    rows = jax.ShapeDtypeStruct((8 * BLOCK, first.shape[1]), BF16)
    hidden = jax.ShapeDtypeStruct((first.shape[0], 8 * BLOCK), BF16)
    slope = jax.ShapeDtypeStruct((first.shape[0], 8 * BLOCK), F32)
    rows_q, rows_p, hidden_q, hidden_p, slope_q, slope_p = pl.pallas_call(
        units_kernel,
        in_specs=[VMEM] * 11,
        out_specs=[VMEM] * 6,
        out_shape=[rows, rows, hidden, hidden, slope, slope],
        name="hidden_units",
    )(*blocks, *tails, first)
    return ((rows_q, hidden_q, slope_q), (rows_p, hidden_p, slope_p))


def score_stats(sc, qs, ts, p, scale):
    width = p.shape[1]
    rows = 8 * BLOCK
    return pl.pallas_call(
        functools.partial(stats_kernel, scale=scale),
        in_specs=[SMEM] + [VMEM] * 5,
        out_specs=[VMEM] * 3,
        out_shape=[
            jax.ShapeDtypeStruct((rows, width), BF16),
            jax.ShapeDtypeStruct((1, rows), jnp.int32),
            jax.ShapeDtypeStruct((64, rows), F32),
        ],
        scratch_shapes=[pltpu.VMEM((8, LOW, width), BF16), pltpu.VMEM((8, 16, width), BF16)],
        name="score_stats",
    )(sc, *qs, *ts, p)


def score_grads(stats, q, p, place, scale):
    columns, width = p.shape
    rows = q.shape[0]
    steps = columns // PAIR
    return pl.pallas_call(
        functools.partial(grads_kernel, scale=scale),
        in_specs=[VMEM] * 4,
        out_specs=[HBM] * 2,
        out_shape=[
            jax.ShapeDtypeStruct((2 * steps * CHUNK, width), BF16),
            jax.ShapeDtypeStruct((columns, rows), BF16),
        ],
        scratch_shapes=[
            pltpu.VMEM((2 * steps * CHUNK, width), BF16),
            pltpu.VMEM((columns, rows), BF16),
            pltpu.SemaphoreType.DMA((2 * steps,)),
        ],
        name="score_grads",
    )(stats, q, p, place)


def query_grads(sc, p, g, scale):
    columns, width = p.shape
    return pl.pallas_call(
        functools.partial(query_kernel, scale=scale),
        in_specs=[SMEM, VMEM, HBM],
        out_specs=[VMEM] * 2,
        out_shape=[jax.ShapeDtypeStruct((4, BLOCK, width), F32)] * 2,
        scratch_shapes=[
            pltpu.VMEM((width, columns), BF16),
            pltpu.VMEM(g.shape, BF16),
            pltpu.SemaphoreType.DMA((2,)),
        ],
        name="query_grads",
    )(sc, p, g)


def line_total(parts):
    blocks, rows, width = parts[0].shape
    return pl.pallas_call(
        total_kernel,
        in_specs=[VMEM] * 4,
        out_specs=VMEM,
        out_shape=jax.ShapeDtypeStruct((blocks * rows, width), BF16),
        name="line_total",
    )(*parts)


def weight_grads(sums, des, rows, hidden, slope, second):
    scratch = [pltpu.VMEM((8 * BLOCK, second.shape[1]), BF16)]
    operands = (*des, rows, hidden, slope, second)
    if sums is None:
        shape = (second.shape[0], rows.shape[1] + second.shape[1])
        return pl.pallas_call(
            first_weights_kernel,
            in_specs=[VMEM] * 6,
            out_specs=VMEM,
            out_shape=jax.ShapeDtypeStruct(shape, F32),
            scratch_shapes=scratch,
            name="first_weights",
        )(*operands)
    return pl.pallas_call(
        last_weights_kernel,
        in_specs=[VMEM] * 7,
        out_specs=VMEM,
        out_shape=jax.ShapeDtypeStruct((128, 1792), BF16),
        scratch_shapes=scratch,
        name="last_weights",
    )(sums, *operands)


def body(query_features, passage_features, counts, positives, w_first, w_second):
    width = query_features.shape[1]
    hidden_width, emb_width = w_second.shape
    scale = 2.5 * emb_width ** (-0.5)
    group = lax.axis_index((LINE, CORE))
    pairs = BLOCK * lax.axis_size(DP)

    pos = positives.reshape(2, LOW)
    where = jnp.reshape(group, (1,)).astype(jnp.int32)
    over, heavy_at = pack_overflow(counts, where, query_features, passage_features, pos)
    over = over.reshape(16 * UNIT, -1)
    arrived = plane_exchange(over)

    def tower(x):
        pre = jnp.dot(x, w_first, preferred_element_type=F32)
        hidden = gelu_tanh(pre).astype(BF16)
        return jnp.dot(hidden, w_second, preferred_element_type=F32).astype(BF16)

    feats = jnp.concatenate([query_features[:LOW], passage_features[:LOW]], axis=0)
    base = tower(feats)
    qs = gathered(base[:LOW])

    feats = along_line(feats)
    feats = feats + [swap_core(x) for x in feats]

    p_send, q_tail = tail_rows(
        heavy_at, arrived.reshape(16, UNIT, -1), base[LOW:], pos, w_first, w_second
    )
    p_all = plane_exchange(p_send.reshape(16 * BLOCK, emb_width))
    ts = gathered(q_tail)

    late_counts, group, _ = lax.optimization_barrier((counts, group, q_tail))
    heavy = (late_counts > LOW).astype(jnp.int32)
    devices = jnp.arange(counts.shape[0], dtype=jnp.int32)
    mine = heavy * (devices % 8 == group)
    offsets = jnp.cumsum(late_counts) - late_counts
    over_start = jnp.sum(mine * offsets) + LOW
    group_start = lax.dynamic_slice_in_dim(offsets.reshape(16, 8), group, 1, 1)[:, 0]
    scalars = [heavy_at[0], over_start, lax.axis_index(LINE), lax.axis_index(CORE)]
    scalars = jnp.stack(scalars + [lax.axis_index(PLANE)])
    heavies = jnp.sum(heavy.reshape(16, 8) * jnp.arange(16, dtype=jnp.int32)[:, None], axis=0)
    sc = jnp.concatenate([group_start, scalars, heavies]).astype(jnp.int32)

    each = hidden_width // lax.axis_size(DP)
    unit = jnp.arange(16 * each, dtype=jnp.int32)
    rest = unit - LOW
    unit_of = jnp.where(
        unit < LOW, (unit // 8) * (8 * each) + unit % 8, (rest // 4) * (8 * each) + 8 + rest % 4
    )
    unit_of = unit_of + group * each
    pick = (unit_of[:, None] == jnp.arange(hidden_width, dtype=jnp.int32)[None, :]).astype(BF16)
    first_part = lax.dot_general(
        pick, w_first, (((1,), (1,)), ((), ())), preferred_element_type=F32
    ).astype(BF16)
    second_part = jnp.dot(pick, w_second, preferred_element_type=F32).astype(BF16)
    p_all, first_part = lax.optimization_barrier((p_all, first_part))

    q_all, place, stats = score_stats(sc, qs, ts, p_all, scale)
    stats = stats_exchange(stats)
    q_units, p_units = hidden_units(feats, ts, first_part)
    dp_part, g = score_grads(stats, q_all, p_all, place, scale)
    dp_all = plane_exchange(dp_part)
    dq_own, dq_far = query_grads(sc, p_all, g, scale)

    dq = dq_own + swap_core(dq_far)
    parts = along_line(dq.astype(BF16))
    dq_sum = line_total(parts)
    dqs = (dq_sum, swap_core(dq_sum))

    dp_sum = jnp.sum(dp_all.reshape(16, CHUNK, emb_width).astype(F32), axis=0)
    mean_loss = (dp_sum[BLOCK, 0] + dp_sum[BLOCK + 1, 0] + dp_sum[BLOCK + 2, 0]) / pairs
    dps = gathered(dp_sum[:BLOCK].astype(BF16))
    sums = weight_grads(None, dqs, *q_units, second_part)
    grads = weight_grads(sums, dps, *p_units, second_part)
    out = jnp.sum(plane_exchange(grads).reshape(16, 8, -1).astype(F32), axis=0)
    wide = width + emb_width
    tail_out = jnp.concatenate([out[:4, wide:], out[4:, wide : 2 * wide - 640]], axis=1)
    out = jnp.concatenate([out[:, :wide], tail_out], axis=0)
    return (mean_loss, out[:, :width].T, out[:, width:])


def solution(mesh):
    finer = Mesh(mesh.devices.reshape(4, 4, 4, 2), DP)
    placed = (P(DP, None), P(DP, None), P(), P(DP), P(), P())
    return jax.shard_map(
        body,
        mesh=finer,
        in_specs=placed,
        out_specs=(P(), P(None, DP), P(DP, None)),
        check_vma=False,
    )
```

```python
import functools

import jax
import jax.numpy as jnp
from jax import lax
from jax.experimental import pallas as pl
from jax.experimental.pallas import tpu as pltpu
from jax.sharding import Mesh
from jax.sharding import PartitionSpec as P


DP = ("dp_0", "dp_1", "dp_2", "dp_3")
PLANE = ("dp_0", "dp_1")
LINE = "dp_2"
CORE = "dp_3"
F32 = jnp.float32
BF16 = jnp.bfloat16

LOW = 128
UNIT = 8
BLOCK = LOW + UNIT
CHUNK = 144
PAIR = 2 * BLOCK
LOG2E = 1.4426950408889634


def gelu_tanh(values):
    return jax.nn.gelu(values, approximate=True)


def swap_core(x):
    return lax.ppermute(x, CORE, [(0, 1), (1, 0)])


def plane_exchange(x):
    return lax.all_to_all(x, PLANE, 0, 0, tiled=True)


def stats_exchange(x):
    return lax.all_to_all(x, (LINE, CORE), 0, 0, tiled=True)


def from_line(x, k):
    return lax.ppermute(x, LINE, [((i + k) % 4, i) for i in range(4)])


def to_line(x, k):
    return lax.ppermute(x, LINE, [(i, (i + k) % 4) for i in range(4)])


def along_line(x):
    return [x] + [from_line(x, k) for k in (1, 2, 3)]


def gathered(x):
    own = jnp.concatenate(along_line(x), axis=0)
    return (own, swap_core(own))


def place_of(pos, sc):
    over = pos - sc[17]
    slot = jnp.bitwise_and(lax.shift_right_logical(over, 3) + sc[16], 15)
    place = jnp.where(
        (over >= 0) & (over < LOW), slot * BLOCK + LOW + jnp.bitwise_and(over, 7), -1
    )
    for s in range(16):
        at = pos - sc[s]
        place = jnp.where((at >= 0) & (at < LOW), at + s * BLOCK, place)
    return place


def near_index(sc, j):
    return jnp.bitwise_and(j // 2 - sc[18], 3) + 4 * jnp.bitwise_xor(j % 2, sc[19])


def nt_dot(a, b):
    return lax.dot_general(a, b, (((1,), (1,)), ((), ())), preferred_element_type=F32)


def pack_kernel(counts, where, q, p, pos, out, heavy_out):
    heavy_at = jnp.int32(0)
    for s in range(16):
        heavy_at += jnp.where(counts[s * 8 + where[0]] > LOW, s, 0)
    heavy_out[0] = heavy_at
    width = q.shape[1]
    high = lax.shift_right_logical(pos[1:2], 7).astype(F32)
    low = jnp.bitwise_and(pos[1:2], 127).astype(F32)
    line = lax.broadcasted_iota(jnp.int32, (UNIT, LOW), 0)
    code = jnp.where(line == 2, high, jnp.where(line == 3, low, 0.0)).astype(BF16)
    for u in range(16):
        slot = jnp.bitwise_and(heavy_at + u, 15)
        out[slot, :, :width] = q[u * UNIT : (u + 1) * UNIT]
        out[slot, :, width : 2 * width] = p[u * UNIT : (u + 1) * UNIT]
        out[slot, :, 2 * width :] = code


def gelu_parts(v):
    square = v * v
    t = jnp.tanh(0.7978845608028654 * (v + 0.044715 * (square * v)))
    grown = 0.5 * (1.0 + t)
    slope = grown + (0.5 * v) * (1.0 - t * t) * (
        0.7978845608028654 * (1.0 + 3 * 0.044715 * square)
    )
    return (v * grown, slope)


def tail_kernel(heavy_at, arrived, base_p, pos, w_first, w_second, p_out, q_out):
    width, emb_width = w_first.shape[0], w_second.shape[1]
    tail = arrived[heavy_at[0]]
    feats = jnp.concatenate([tail[:, :width], tail[:, width : 2 * width]], axis=0)
    q_out[:, emb_width:] = feats
    pre = jnp.dot(feats, w_first[...], preferred_element_type=F32)
    hidden = gelu_parts(pre)[0].astype(BF16)
    emb = jnp.dot(hidden, w_second[...], preferred_element_type=F32).astype(BF16)
    for s in range(p_out.shape[0]):
        p_out[s, :LOW] = base_p[...]
        p_out[s, LOW:] = emb[UNIT:]
    high = lax.shift_right_logical(pos[0:1], 7).astype(F32)
    low = jnp.bitwise_and(pos[0:1], 127).astype(F32)
    line = lax.broadcasted_iota(jnp.int32, (UNIT, LOW), 0)
    code = tail[:, 2 * width :].astype(F32)
    code = jnp.where(line == 0, high, jnp.where(line == 1, low, code)).astype(BF16)
    q_out[:UNIT, :emb_width] = emb[:UNIT]
    q_out[UNIT:, LOW:emb_width] = jnp.zeros((UNIT, emb_width - LOW), BF16)
    q_out[UNIT:, :LOW] = code


def units_kernel(*refs):
    blocks, tails, (first, rows_q, rows_p, hidden_q, hidden_p, slope_q, slope_p) = (
        refs[:8],
        refs[8:10],
        refs[10:],
    )
    skip = tails[0].shape[1] - rows_q.shape[1]
    for k, block in enumerate(blocks):
        tail = tails[k // 4][(k % 4) * 2 * UNIT : (k % 4 + 1) * 2 * UNIT, skip:]
        at = k * BLOCK
        rows_q[at : at + LOW] = block[:LOW]
        rows_q[at + LOW : at + BLOCK] = tail[:UNIT]
        rows_p[at : at + LOW] = block[LOW:]
        rows_p[at + LOW : at + BLOCK] = tail[UNIT:]
    for rows, hidden, slope in ((rows_q, hidden_q, slope_q), (rows_p, hidden_p, slope_p)):
        value, gain = gelu_parts(nt_dot(first[...], rows[...]))
        hidden[...] = value.astype(BF16)
        slope[...] = gain


def stats_kernel(
    sc, q_own, q_far, t_own, t_far, p, q_out, place_out, stats_out, qs, ts, *, scale
):
    for k, (q, t) in enumerate(((q_own, t_own), (q_far, t_far))):
        for b in range(4):
            qs[4 * k + b] = q[b * LOW : (b + 1) * LOW]
            ts[4 * k + b] = t[b * 16 : (b + 1) * 16, : p.shape[1]]
    lane = lax.broadcasted_iota(jnp.int32, (1, LOW), 1) // UNIT
    codes = []
    spread = jnp.zeros((1, LOW), F32)
    for j in range(8):
        b = near_index(sc, j)
        q_out[j * LOW : (j + 1) * LOW] = qs[b]
        tail = ts[b]
        q_out[8 * LOW + j * UNIT : 8 * LOW + (j + 1) * UNIT] = tail[:UNIT]
        code = tail[UNIT:, :LOW].astype(F32)
        codes.append(code[0:1] * 128.0 + code[1:2])
        unit = jnp.bitwise_and(sc[20] - sc[21 + j], 15)
        part = pltpu.roll(code, jnp.bitwise_and(j - unit, 15) * UNIT, 1)
        spread = jnp.where(lane == j, part[2:3] * 128.0 + part[3:4], spread)
    codes.append(spread[:, : 8 * UNIT])
    place_out[...] = place_of(jnp.concatenate(codes, axis=1).astype(jnp.int32), sc)
    rows = q_out.shape[0]
    pull = scale * LOG2E
    top = jnp.full((1, rows), -1e30, F32)
    total = jnp.zeros((1, rows), F32)
    found = jnp.zeros((1, rows), F32)
    for at in range(0, p.shape[0], PAIR):
        tile = p[at : at + PAIR]
        s = nt_dot(tile, q_out[...])
        row = lax.broadcasted_iota(jnp.int32, s.shape, 0)
        found += jnp.sum(jnp.where(row == place_out[...] - at, s, 0.0), axis=0, keepdims=True)
        new_top = jnp.maximum(top, jnp.max(s, axis=0, keepdims=True))
        total = total * jnp.exp2((top - new_top) * pull) + jnp.sum(
            jnp.exp2(s * pull - new_top * pull), axis=0, keepdims=True
        )
        top = new_top
    line = lax.broadcasted_iota(jnp.int32, (8, rows), 0)
    stats = jnp.where(line == 0, top, jnp.where(line == 1, total, jnp.where(line == 2, found, 0.0)))
    for b in range(8):
        stats_out[b * 8 : (b + 1) * 8] = stats


def grads_kernel(stats, q, p, place, dp_out, g_out, dp_ref, g_ref, sems, *, scale):
    rows, width = q.shape
    pull = scale * LOG2E
    tops = [stats[b * 8 : b * 8 + 1] for b in range(8)]
    top = functools.reduce(jnp.maximum, tops)
    total = jnp.zeros((1, rows), F32)
    found = jnp.zeros((1, rows), F32)
    for b in range(8):
        total += stats[b * 8 + 1 : b * 8 + 2] * jnp.exp2((tops[b] - top) * pull)
        found += stats[b * 8 + 2 : b * 8 + 3]
    norm = top * scale + jnp.log(total)
    loss = jnp.sum(norm - found * scale, axis=1, keepdims=True)
    norm = norm * LOG2E
    loss_high = loss.astype(BF16).astype(F32)
    loss_mid = (loss - loss_high).astype(BF16).astype(F32)
    loss_low = loss - loss_high - loss_mid
    line = lax.broadcasted_iota(jnp.int32, (UNIT, width), 0)
    loss_tile = jnp.where(
        line == 0,
        loss_high,
        jnp.where(line == 1, loss_mid, jnp.where(line == 2, loss_low, 0.0)),
    ).astype(BF16)
    copies = []

    def send(src, dst, rows):
        copy = pltpu.make_async_copy(src.at[rows], dst.at[rows], sems.at[len(copies)])
        copy.start()
        copies.append(copy)

    for at in range(0, p.shape[0], PAIR):
        s = nt_dot(p[at : at + PAIR], q[...])
        row = lax.broadcasted_iota(jnp.int32, s.shape, 0)
        e = jnp.exp2(s * pull - norm)
        g_ref[at : at + PAIR] = jnp.where(row == place[...] - at, e - 1.0, e).astype(BF16)
        send(g_ref, g_out, pl.ds(at, PAIR))
    for k in range(p.shape[0] // PAIR):
        dp = scale * jnp.dot(g_ref[k * PAIR : (k + 1) * PAIR], q[...], preferred_element_type=F32)
        dp = dp.astype(BF16)
        for half in range(2):
            to = (2 * k + half) * CHUNK
            dp_ref[to : to + BLOCK] = dp[half * BLOCK : (half + 1) * BLOCK]
            dp_ref[to + BLOCK : to + CHUNK] = loss_tile
        send(dp_ref, dp_out, pl.ds(2 * k * CHUNK, 2 * CHUNK))
    for copy in copies:
        copy.wait()


def query_kernel(sc, p, g, own, far, *, scale):
    def put(j, rows, part):
        b = near_index(sc, j)

        @pl.when(b < 4)
        def _():
            own[b, rows] = part

        @pl.when(b >= 4)
        def _():
            far[b - 4, rows] = part

    def part(first, size):
        dq = lax.dot_general(
            g[:, first : first + size], p[...], (((0,), (0,)), ((), ())), preferred_element_type=F32
        )
        return scale * dq

    for k in range(2):
        dq = part(4 * k * LOW, 4 * LOW)
        for j in range(4):
            put(4 * k + j, slice(0, LOW), dq[j * LOW : (j + 1) * LOW])
    dq = part(8 * LOW, 8 * UNIT)
    for j in range(8):
        put(j, slice(LOW, BLOCK), dq[j * UNIT : (j + 1) * UNIT])


def weight_parts(de_own, de_far, rows, hidden, slope, second, de):
    half = de_own.shape[0]
    de[:half] = de_own[...]
    de[half:] = de_far[...]
    grad_second = jnp.dot(hidden[...], de[...], preferred_element_type=F32)
    dpre = (slope[...] * nt_dot(second[...], de[...])).astype(BF16)
    grad_first = jnp.dot(dpre, rows[...], preferred_element_type=F32)
    return (grad_first, grad_second)


def weights_kernel(*refs):
    second, out, de = refs[10:]
    first_q, second_q = weight_parts(*refs[:5], second, de)
    grad_first, grad_second = weight_parts(*refs[5:10], second, de)
    grad_first += first_q
    grad_second += second_q
    many = out.shape[0]
    width = grad_first.shape[1]
    wide = width + grad_second.shape[1]
    out[:, :width] = grad_first[:many].astype(BF16)
    out[:, width:wide] = grad_second[:many].astype(BF16)
    rest = grad_first.shape[0] - many
    x = jnp.concatenate(
        [grad_first[many:], grad_second[many:], jnp.zeros((rest, 128), F32)], axis=1
    )
    near, far = x[:, :640], x[:, 640:]
    line = jnp.bitwise_and(lax.broadcasted_iota(jnp.int32, near.shape, 0), 7)
    even = jnp.where(line < 4, near, pltpu.roll(far, 4, 0)).astype(BF16)
    odd = jnp.where(line < 4, pltpu.roll(near, rest - 4, 0), far).astype(BF16)
    for b in range(rest // 8):
        out[b * 16 : b * 16 + 8, wide:] = even[b * 8 : (b + 1) * 8]
        out[b * 16 + 8 : b * 16 + 16, wide:] = odd[b * 8 : (b + 1) * 8]


VMEM = pl.BlockSpec(memory_space=pltpu.VMEM)
SMEM = pl.BlockSpec(memory_space=pltpu.SMEM)
HBM = pl.BlockSpec(memory_space=pltpu.HBM)


def pack_overflow(counts, where, q, p, pos):
    width = q.shape[1]
    half = pl.BlockSpec((LOW, width), lambda i: (1, 0))
    return pl.pallas_call(
        pack_kernel,
        grid=(1,),
        in_specs=[SMEM, SMEM, half, half, pl.BlockSpec((2, LOW), lambda i: (0, 0))],
        out_specs=[pl.BlockSpec((16, UNIT, 2 * width + LOW), lambda i: (0, 0, 0)), SMEM],
        out_shape=[
            jax.ShapeDtypeStruct((16, UNIT, 2 * width + LOW), BF16),
            jax.ShapeDtypeStruct((1,), jnp.int32),
        ],
        name="pack_overflow",
    )(counts, where, q, p, pos)


def tail_rows(heavy_at, arrived, base_p, pos, w_first, w_second):
    emb_width = w_second.shape[1]
    return pl.pallas_call(
        tail_kernel,
        in_specs=[SMEM] + [VMEM] * 5,
        out_specs=[VMEM] * 2,
        out_shape=[
            jax.ShapeDtypeStruct((16, BLOCK, emb_width), BF16),
            jax.ShapeDtypeStruct((2 * UNIT, emb_width + w_first.shape[0]), BF16),
        ],
        name="tail_rows",
    )(heavy_at, arrived, base_p, pos, w_first, w_second)


def hidden_units(blocks, tails, first):
    rows = jax.ShapeDtypeStruct((8 * BLOCK, first.shape[1]), BF16)
    hidden = jax.ShapeDtypeStruct((first.shape[0], 8 * BLOCK), BF16)
    slope = jax.ShapeDtypeStruct((first.shape[0], 8 * BLOCK), F32)
    rows_q, rows_p, hidden_q, hidden_p, slope_q, slope_p = pl.pallas_call(
        units_kernel,
        in_specs=[VMEM] * 11,
        out_specs=[VMEM] * 6,
        out_shape=[rows, rows, hidden, hidden, slope, slope],
        name="hidden_units",
    )(*blocks, *tails, first)
    return ((rows_q, hidden_q, slope_q), (rows_p, hidden_p, slope_p))


def score_stats(sc, qs, ts, p, scale):
    width = p.shape[1]
    rows = 8 * BLOCK
    return pl.pallas_call(
        functools.partial(stats_kernel, scale=scale),
        in_specs=[SMEM] + [VMEM] * 5,
        out_specs=[VMEM] * 3,
        out_shape=[
            jax.ShapeDtypeStruct((rows, width), BF16),
            jax.ShapeDtypeStruct((1, rows), jnp.int32),
            jax.ShapeDtypeStruct((64, rows), F32),
        ],
        scratch_shapes=[pltpu.VMEM((8, LOW, width), BF16), pltpu.VMEM((8, 16, width), BF16)],
        name="score_stats",
    )(sc, *qs, *ts, p)


def score_grads(stats, q, p, place, scale):
    columns, width = p.shape
    rows = q.shape[0]
    steps = columns // PAIR
    return pl.pallas_call(
        functools.partial(grads_kernel, scale=scale),
        in_specs=[VMEM] * 4,
        out_specs=[HBM] * 2,
        out_shape=[
            jax.ShapeDtypeStruct((2 * steps * CHUNK, width), BF16),
            jax.ShapeDtypeStruct((columns, rows), BF16),
        ],
        scratch_shapes=[
            pltpu.VMEM((2 * steps * CHUNK, width), BF16),
            pltpu.VMEM((columns, rows), BF16),
            pltpu.SemaphoreType.DMA((2 * steps,)),
        ],
        name="score_grads",
    )(stats, q, p, place)


def query_grads(sc, p, g, scale):
    width = p.shape[1]
    return pl.pallas_call(
        functools.partial(query_kernel, scale=scale),
        in_specs=[SMEM, VMEM, VMEM],
        out_specs=[VMEM] * 2,
        out_shape=[jax.ShapeDtypeStruct((4, BLOCK, width), F32)] * 2,
        name="query_grads",
    )(sc, p, g)


def weight_grads(dqs, q_units, dps, p_units, second):
    return pl.pallas_call(
        weights_kernel,
        in_specs=[VMEM] * 11,
        out_specs=VMEM,
        out_shape=jax.ShapeDtypeStruct((128, 1792), BF16),
        scratch_shapes=[pltpu.VMEM((8 * BLOCK, second.shape[1]), BF16)],
        name="weight_grads",
    )(*dqs, *q_units, *dps, *p_units, second)


def body(query_features, passage_features, counts, positives, w_first, w_second):
    width = query_features.shape[1]
    hidden_width, emb_width = w_second.shape
    scale = 2.5 * emb_width ** (-0.5)
    group = lax.axis_index((LINE, CORE))
    pairs = BLOCK * lax.axis_size(DP)

    pos = positives.reshape(2, LOW)
    where = jnp.reshape(group, (1,)).astype(jnp.int32)
    over, heavy_at = pack_overflow(counts, where, query_features, passage_features, pos)
    over = over.reshape(16 * UNIT, -1)
    arrived = plane_exchange(over)

    def tower(x):
        pre = jnp.dot(x, w_first, preferred_element_type=F32)
        hidden = gelu_tanh(pre).astype(BF16)
        return jnp.dot(hidden, w_second, preferred_element_type=F32).astype(BF16)

    feats = jnp.concatenate([query_features[:LOW], passage_features[:LOW]], axis=0)
    base = tower(feats)
    qs = gathered(base[:LOW])

    feats = along_line(feats)
    feats = feats + [swap_core(x) for x in feats]

    p_send, q_tail = tail_rows(
        heavy_at, arrived.reshape(16, UNIT, -1), base[LOW:], pos, w_first, w_second
    )
    p_all = plane_exchange(p_send.reshape(16 * BLOCK, emb_width))
    ts = gathered(q_tail)

    late_counts, group, _ = lax.optimization_barrier((counts, group, q_tail))
    heavy = (late_counts > LOW).astype(jnp.int32)
    devices = jnp.arange(counts.shape[0], dtype=jnp.int32)
    mine = heavy * (devices % 8 == group)
    offsets = jnp.cumsum(late_counts) - late_counts
    over_start = jnp.sum(mine * offsets) + LOW
    group_start = lax.dynamic_slice_in_dim(offsets.reshape(16, 8), group, 1, 1)[:, 0]
    scalars = [heavy_at[0], over_start, lax.axis_index(LINE), lax.axis_index(CORE)]
    scalars = jnp.stack(scalars + [lax.axis_index(PLANE)])
    heavies = jnp.sum(heavy.reshape(16, 8) * jnp.arange(16, dtype=jnp.int32)[:, None], axis=0)
    sc = jnp.concatenate([group_start, scalars, heavies]).astype(jnp.int32)

    each = hidden_width // lax.axis_size(DP)
    unit = jnp.arange(16 * each, dtype=jnp.int32)
    rest = unit - LOW
    unit_of = jnp.where(
        unit < LOW, (unit // 8) * (8 * each) + unit % 8, (rest // 4) * (8 * each) + 8 + rest % 4
    )
    unit_of = unit_of + group * each
    pick = (unit_of[:, None] == jnp.arange(hidden_width, dtype=jnp.int32)[None, :]).astype(BF16)
    first_part = lax.dot_general(
        pick, w_first, (((1,), (1,)), ((), ())), preferred_element_type=F32
    ).astype(BF16)
    second_part = jnp.dot(pick, w_second, preferred_element_type=F32).astype(BF16)
    p_all, first_part = lax.optimization_barrier((p_all, first_part))

    q_all, place, stats = score_stats(sc, qs, ts, p_all, scale)
    stats = stats_exchange(stats)
    q_units, p_units = hidden_units(feats, ts, first_part)
    dp_part, g = score_grads(stats, q_all, p_all, place, scale)
    dp_all = plane_exchange(dp_part)
    dq_own, dq_far = query_grads(sc, p_all, g, scale)

    dq = dq_own + swap_core(dq_far)
    dq_sum = dq[0].astype(BF16).astype(F32)
    for k in (1, 2, 3):
        dq_sum = dq_sum + to_line(dq[k].astype(BF16), k).astype(F32)
    dqs = gathered(dq_sum.astype(BF16))

    dp_sum = jnp.sum(dp_all.reshape(16, CHUNK, emb_width).astype(F32), axis=0)
    mean_loss = (dp_sum[BLOCK, 0] + dp_sum[BLOCK + 1, 0] + dp_sum[BLOCK + 2, 0]) / pairs
    dps = gathered(dp_sum[:BLOCK].astype(BF16))
    grads = weight_grads(dqs, q_units, dps, p_units, second_part)
    out = jnp.sum(plane_exchange(grads).reshape(16, 8, -1).astype(F32), axis=0)
    wide = width + emb_width
    tail_out = jnp.concatenate([out[:4, wide:], out[4:, wide : 2 * wide - 640]], axis=1)
    out = jnp.concatenate([out[:, :wide], tail_out], axis=0)
    return (mean_loss, out[:, :width].T, out[:, width:])


def solution(mesh):
    finer = Mesh(mesh.devices.reshape(4, 4, 4, 2), DP)
    placed = (P(DP, None), P(DP, None), P(), P(DP), P(), P())
    return jax.shard_map(
        body,
        mesh=finer,
        in_specs=placed,
        out_specs=(P(), P(None, DP), P(DP, None)),
        check_vma=False,
    )
```

```python
import functools

import jax
import jax.numpy as jnp
from jax import lax
from jax.experimental import pallas as pl
from jax.experimental.pallas import tpu as pltpu
from jax.sharding import Mesh
from jax.sharding import PartitionSpec as P


DP = ("dp_0", "dp_1", "dp_2", "dp_3")
PLANE = ("dp_0", "dp_1")
LINE = "dp_2"
CORE = "dp_3"
F32 = jnp.float32
BF16 = jnp.bfloat16

LOW = 128
UNIT = 8
BLOCK = LOW + UNIT
CHUNK = 144
PAIR = 2 * BLOCK
LOG2E = 1.4426950408889634


def gelu_tanh(values):
    return jax.nn.gelu(values, approximate=True)


def swap_core(x):
    return lax.ppermute(x, CORE, [(0, 1), (1, 0)])


def plane_exchange(x):
    return lax.all_to_all(x, PLANE, 0, 0, tiled=True)


def stats_exchange(x):
    return lax.all_to_all(x, (LINE, CORE), 0, 0, tiled=True)


def from_line(x, k):
    return lax.ppermute(x, LINE, [((i + k) % 4, i) for i in range(4)])


def to_line(x, k):
    return lax.ppermute(x, LINE, [(i, (i + k) % 4) for i in range(4)])


def along_line(x):
    return [x] + [from_line(x, k) for k in (1, 2, 3)]


def gathered(x):
    own = jnp.concatenate(along_line(x), axis=0)
    return (own, swap_core(own))


def place_of(pos, sc):
    over = pos - sc[17]
    slot = jnp.bitwise_and(lax.shift_right_logical(over, 3) + sc[16], 15)
    place = jnp.where(
        (over >= 0) & (over < LOW), slot * BLOCK + LOW + jnp.bitwise_and(over, 7), -1
    )
    for s in range(16):
        at = pos - sc[s]
        place = jnp.where((at >= 0) & (at < LOW), at + s * BLOCK, place)
    return place


def near_index(sc, j):
    return jnp.bitwise_and(j // 2 - sc[18], 3) + 4 * jnp.bitwise_xor(j % 2, sc[19])


def nt_dot(a, b):
    return lax.dot_general(a, b, (((1,), (1,)), ((), ())), preferred_element_type=F32)


def pack_kernel(counts, where, q, p, pos, out, heavy_out):
    heavy_at = jnp.int32(0)
    for s in range(16):
        heavy_at += jnp.where(counts[s * 8 + where[0]] > LOW, s, 0)
    heavy_out[0] = heavy_at
    width = q.shape[1]
    high = lax.shift_right_logical(pos[1:2], 7).astype(F32)
    low = jnp.bitwise_and(pos[1:2], 127).astype(F32)
    line = lax.broadcasted_iota(jnp.int32, (UNIT, LOW), 0)
    code = jnp.where(line == 2, high, jnp.where(line == 3, low, 0.0)).astype(BF16)
    for u in range(16):
        slot = jnp.bitwise_and(heavy_at + u, 15)
        out[slot, :, :width] = q[u * UNIT : (u + 1) * UNIT]
        out[slot, :, width : 2 * width] = p[u * UNIT : (u + 1) * UNIT]
        out[slot, :, 2 * width :] = code


def gelu_parts(v):
    square = v * v
    t = jnp.tanh(0.7978845608028654 * (v + 0.044715 * (square * v)))
    grown = 0.5 * (1.0 + t)
    slope = grown + (0.5 * v) * (1.0 - t * t) * (
        0.7978845608028654 * (1.0 + 3 * 0.044715 * square)
    )
    return (v * grown, slope)


def tail_kernel(heavy_at, arrived, base_p, pos, w_first, w_second, p_out, q_out):
    width, emb_width = w_first.shape[0], w_second.shape[1]
    tail = arrived[heavy_at[0]]
    feats = jnp.concatenate([tail[:, :width], tail[:, width : 2 * width]], axis=0)
    q_out[:, emb_width:] = feats
    pre = jnp.dot(feats, w_first[...], preferred_element_type=F32)
    hidden = gelu_parts(pre)[0].astype(BF16)
    emb = jnp.dot(hidden, w_second[...], preferred_element_type=F32).astype(BF16)
    for s in range(p_out.shape[0]):
        p_out[s, :LOW] = base_p[...]
        p_out[s, LOW:] = emb[UNIT:]
    high = lax.shift_right_logical(pos[0:1], 7).astype(F32)
    low = jnp.bitwise_and(pos[0:1], 127).astype(F32)
    line = lax.broadcasted_iota(jnp.int32, (UNIT, LOW), 0)
    code = tail[:, 2 * width :].astype(F32)
    code = jnp.where(line == 0, high, jnp.where(line == 1, low, code)).astype(BF16)
    q_out[:UNIT, :emb_width] = emb[:UNIT]
    q_out[UNIT:, LOW:emb_width] = jnp.zeros((UNIT, emb_width - LOW), BF16)
    q_out[UNIT:, :LOW] = code


def units_kernel(*refs):
    blocks, tails, (first, rows_q, rows_p, hidden_q, hidden_p, slope_q, slope_p) = (
        refs[:8],
        refs[8:10],
        refs[10:],
    )
    skip = tails[0].shape[1] - rows_q.shape[1]
    for k, block in enumerate(blocks):
        tail = tails[k // 4][(k % 4) * 2 * UNIT : (k % 4 + 1) * 2 * UNIT, skip:]
        at = k * BLOCK
        rows_q[at : at + LOW] = block[:LOW]
        rows_q[at + LOW : at + BLOCK] = tail[:UNIT]
        rows_p[at : at + LOW] = block[LOW:]
        rows_p[at + LOW : at + BLOCK] = tail[UNIT:]
    for rows, hidden, slope in ((rows_q, hidden_q, slope_q), (rows_p, hidden_p, slope_p)):
        value, gain = gelu_parts(nt_dot(first[...], rows[...]))
        hidden[...] = value.astype(BF16)
        slope[...] = gain


def stats_kernel(
    sc, q_own, q_far, t_own, t_far, p, q_out, place_out, stats_out, qs, ts, *, scale
):
    for k, (q, t) in enumerate(((q_own, t_own), (q_far, t_far))):
        for b in range(4):
            qs[4 * k + b] = q[b * LOW : (b + 1) * LOW]
            ts[4 * k + b] = t[b * 16 : (b + 1) * 16, : p.shape[1]]
    lane = lax.broadcasted_iota(jnp.int32, (1, LOW), 1) // UNIT
    codes = []
    spread = jnp.zeros((1, LOW), F32)
    for j in range(8):
        b = near_index(sc, j)
        q_out[j * LOW : (j + 1) * LOW] = qs[b]
        tail = ts[b]
        q_out[8 * LOW + j * UNIT : 8 * LOW + (j + 1) * UNIT] = tail[:UNIT]
        code = tail[UNIT:, :LOW].astype(F32)
        codes.append(code[0:1] * 128.0 + code[1:2])
        unit = jnp.bitwise_and(sc[20] - sc[21 + j], 15)
        part = pltpu.roll(code, jnp.bitwise_and(j - unit, 15) * UNIT, 1)
        spread = jnp.where(lane == j, part[2:3] * 128.0 + part[3:4], spread)
    codes.append(spread[:, : 8 * UNIT])
    place_out[...] = place_of(jnp.concatenate(codes, axis=1).astype(jnp.int32), sc)
    rows = q_out.shape[0]
    pull = scale * LOG2E
    top = jnp.full((1, rows), -1e30, F32)
    total = jnp.zeros((1, rows), F32)
    found = jnp.zeros((1, rows), F32)
    for at in range(0, p.shape[0], PAIR):
        tile = p[at : at + PAIR]
        s = nt_dot(tile, q_out[...])
        row = lax.broadcasted_iota(jnp.int32, s.shape, 0)
        found += jnp.sum(jnp.where(row == place_out[...] - at, s, 0.0), axis=0, keepdims=True)
        new_top = jnp.maximum(top, jnp.max(s, axis=0, keepdims=True))
        total = total * jnp.exp2((top - new_top) * pull) + jnp.sum(
            jnp.exp2(s * pull - new_top * pull), axis=0, keepdims=True
        )
        top = new_top
    line = lax.broadcasted_iota(jnp.int32, (8, rows), 0)
    stats = jnp.where(line == 0, top, jnp.where(line == 1, total, jnp.where(line == 2, found, 0.0)))
    for b in range(8):
        stats_out[b * 8 : (b + 1) * 8] = stats


def grads_kernel(stats, q, p, place, dp_out, g_out, dp_ref, g_ref, sems, *, scale):
    rows, width = q.shape
    pull = scale * LOG2E
    tops = [stats[b * 8 : b * 8 + 1] for b in range(8)]
    top = functools.reduce(jnp.maximum, tops)
    total = jnp.zeros((1, rows), F32)
    found = jnp.zeros((1, rows), F32)
    for b in range(8):
        total += stats[b * 8 + 1 : b * 8 + 2] * jnp.exp2((tops[b] - top) * pull)
        found += stats[b * 8 + 2 : b * 8 + 3]
    norm = top * scale + jnp.log(total)
    loss = jnp.sum(norm - found * scale, axis=1, keepdims=True)
    norm = norm * LOG2E
    loss_high = loss.astype(BF16).astype(F32)
    loss_mid = (loss - loss_high).astype(BF16).astype(F32)
    loss_low = loss - loss_high - loss_mid
    line = lax.broadcasted_iota(jnp.int32, (UNIT, width), 0)
    loss_tile = jnp.where(
        line == 0,
        loss_high,
        jnp.where(line == 1, loss_mid, jnp.where(line == 2, loss_low, 0.0)),
    ).astype(BF16)
    copies = []

    def send(src, dst, rows):
        copy = pltpu.make_async_copy(src.at[rows], dst.at[rows], sems.at[len(copies)])
        copy.start()
        copies.append(copy)

    for at in range(0, p.shape[0], PAIR):
        s = nt_dot(p[at : at + PAIR], q[...])
        row = lax.broadcasted_iota(jnp.int32, s.shape, 0)
        e = jnp.exp2(s * pull - norm)
        g_ref[at : at + PAIR] = jnp.where(row == place[...] - at, e - 1.0, e).astype(BF16)
        send(g_ref, g_out, pl.ds(at, PAIR))
    for k in range(p.shape[0] // PAIR):
        dp = scale * jnp.dot(g_ref[k * PAIR : (k + 1) * PAIR], q[...], preferred_element_type=F32)
        dp = dp.astype(BF16)
        for half in range(2):
            to = (2 * k + half) * CHUNK
            dp_ref[to : to + BLOCK] = dp[half * BLOCK : (half + 1) * BLOCK]
            dp_ref[to + BLOCK : to + CHUNK] = loss_tile
        send(dp_ref, dp_out, pl.ds(2 * k * CHUNK, 2 * CHUNK))
    for copy in copies:
        copy.wait()


def query_kernel(sc, p, g, own, far, *, scale):
    def put(j, rows, part):
        b = near_index(sc, j)

        @pl.when(b < 4)
        def _():
            own[b, rows] = part

        @pl.when(b >= 4)
        def _():
            far[b - 4, rows] = part

    def part(first, size):
        dq = lax.dot_general(
            g[:, first : first + size], p[...], (((0,), (0,)), ((), ())), preferred_element_type=F32
        )
        return scale * dq

    for k in range(2):
        dq = part(4 * k * LOW, 4 * LOW)
        for j in range(4):
            put(4 * k + j, slice(0, LOW), dq[j * LOW : (j + 1) * LOW])
    dq = part(8 * LOW, 8 * UNIT)
    for j in range(8):
        put(j, slice(LOW, BLOCK), dq[j * UNIT : (j + 1) * UNIT])


def weight_parts(de_own, de_far, rows, hidden, slope, second, de):
    half = de_own.shape[0]
    de[:half] = de_own[...]
    de[half:] = de_far[...]
    grad_second = jnp.dot(hidden[...], de[...], preferred_element_type=F32)
    dpre = (slope[...] * nt_dot(second[...], de[...])).astype(BF16)
    grad_first = jnp.dot(dpre, rows[...], preferred_element_type=F32)
    return (grad_first, grad_second)


def weights_kernel(*refs):
    second, out, de = refs[10:]
    first_q, second_q = weight_parts(*refs[:5], second, de)
    grad_first, grad_second = weight_parts(*refs[5:10], second, de)
    grad_first += first_q
    grad_second += second_q
    many = out.shape[0]
    width = grad_first.shape[1]
    wide = width + grad_second.shape[1]
    out[:, :width] = grad_first[:many].astype(BF16)
    out[:, width:wide] = grad_second[:many].astype(BF16)
    rest = grad_first.shape[0] - many
    x = jnp.concatenate(
        [grad_first[many:], grad_second[many:], jnp.zeros((rest, 128), F32)], axis=1
    )
    near, far = x[:, :640], x[:, 640:]
    line = jnp.bitwise_and(lax.broadcasted_iota(jnp.int32, near.shape, 0), 7)
    even = jnp.where(line < 4, near, pltpu.roll(far, 4, 0)).astype(BF16)
    odd = jnp.where(line < 4, pltpu.roll(near, rest - 4, 0), far).astype(BF16)
    for b in range(rest // 8):
        out[b * 16 : b * 16 + 8, wide:] = even[b * 8 : (b + 1) * 8]
        out[b * 16 + 8 : b * 16 + 16, wide:] = odd[b * 8 : (b + 1) * 8]


VMEM = pl.BlockSpec(memory_space=pltpu.VMEM)
SMEM = pl.BlockSpec(memory_space=pltpu.SMEM)
HBM = pl.BlockSpec(memory_space=pltpu.HBM)


def pack_overflow(counts, where, q, p, pos):
    width = q.shape[1]
    half = pl.BlockSpec((LOW, width), lambda i: (1, 0))
    return pl.pallas_call(
        pack_kernel,
        grid=(1,),
        in_specs=[SMEM, SMEM, half, half, pl.BlockSpec((2, LOW), lambda i: (0, 0))],
        out_specs=[pl.BlockSpec((16, UNIT, 2 * width + LOW), lambda i: (0, 0, 0)), SMEM],
        out_shape=[
            jax.ShapeDtypeStruct((16, UNIT, 2 * width + LOW), BF16),
            jax.ShapeDtypeStruct((1,), jnp.int32),
        ],
        name="pack_overflow",
    )(counts, where, q, p, pos)


def tail_rows(heavy_at, arrived, base_p, pos, w_first, w_second):
    emb_width = w_second.shape[1]
    return pl.pallas_call(
        tail_kernel,
        in_specs=[SMEM] + [VMEM] * 5,
        out_specs=[VMEM] * 2,
        out_shape=[
            jax.ShapeDtypeStruct((16, BLOCK, emb_width), BF16),
            jax.ShapeDtypeStruct((2 * UNIT, emb_width + w_first.shape[0]), BF16),
        ],
        name="tail_rows",
    )(heavy_at, arrived, base_p, pos, w_first, w_second)


def hidden_units(blocks, tails, first):
    rows = jax.ShapeDtypeStruct((8 * BLOCK, first.shape[1]), BF16)
    hidden = jax.ShapeDtypeStruct((first.shape[0], 8 * BLOCK), BF16)
    slope = jax.ShapeDtypeStruct((first.shape[0], 8 * BLOCK), F32)
    rows_q, rows_p, hidden_q, hidden_p, slope_q, slope_p = pl.pallas_call(
        units_kernel,
        in_specs=[VMEM] * 11,
        out_specs=[VMEM] * 6,
        out_shape=[rows, rows, hidden, hidden, slope, slope],
        name="hidden_units",
    )(*blocks, *tails, first)
    return ((rows_q, hidden_q, slope_q), (rows_p, hidden_p, slope_p))


def score_stats(sc, qs, ts, p, scale):
    width = p.shape[1]
    rows = 8 * BLOCK
    return pl.pallas_call(
        functools.partial(stats_kernel, scale=scale),
        in_specs=[SMEM] + [VMEM] * 5,
        out_specs=[VMEM] * 3,
        out_shape=[
            jax.ShapeDtypeStruct((rows, width), BF16),
            jax.ShapeDtypeStruct((1, rows), jnp.int32),
            jax.ShapeDtypeStruct((64, rows), F32),
        ],
        scratch_shapes=[pltpu.VMEM((8, LOW, width), BF16), pltpu.VMEM((8, 16, width), BF16)],
        name="score_stats",
    )(sc, *qs, *ts, p)


def score_grads(stats, q, p, place, scale):
    columns, width = p.shape
    rows = q.shape[0]
    steps = columns // PAIR
    return pl.pallas_call(
        functools.partial(grads_kernel, scale=scale),
        in_specs=[VMEM] * 4,
        out_specs=[HBM] * 2,
        out_shape=[
            jax.ShapeDtypeStruct((2 * steps * CHUNK, width), BF16),
            jax.ShapeDtypeStruct((columns, rows), BF16),
        ],
        scratch_shapes=[
            pltpu.VMEM((2 * steps * CHUNK, width), BF16),
            pltpu.VMEM((columns, rows), BF16),
            pltpu.SemaphoreType.DMA((2 * steps,)),
        ],
        name="score_grads",
    )(stats, q, p, place)


def query_grads(sc, p, g, scale):
    width = p.shape[1]
    return pl.pallas_call(
        functools.partial(query_kernel, scale=scale),
        in_specs=[SMEM, VMEM, VMEM],
        out_specs=[VMEM] * 2,
        out_shape=[jax.ShapeDtypeStruct((4, BLOCK, width), F32)] * 2,
        name="query_grads",
    )(sc, p, g)


def weight_grads(dqs, q_units, dps, p_units, second):
    return pl.pallas_call(
        weights_kernel,
        in_specs=[VMEM] * 11,
        out_specs=VMEM,
        out_shape=jax.ShapeDtypeStruct((128, 1792), BF16),
        scratch_shapes=[pltpu.VMEM((8 * BLOCK, second.shape[1]), BF16)],
        name="weight_grads",
    )(*dqs, *q_units, *dps, *p_units, second)


def body(query_features, passage_features, counts, positives, w_first, w_second):
    width = query_features.shape[1]
    hidden_width, emb_width = w_second.shape
    scale = 2.5 * emb_width ** (-0.5)
    group = lax.axis_index((LINE, CORE))
    pairs = BLOCK * lax.axis_size(DP)

    pos = positives.reshape(2, LOW)
    where = jnp.reshape(group, (1,)).astype(jnp.int32)
    over, heavy_at = pack_overflow(counts, where, query_features, passage_features, pos)
    over = over.reshape(16 * UNIT, -1)
    arrived = plane_exchange(over)

    def tower(x):
        pre = jnp.dot(x, w_first, preferred_element_type=F32)
        hidden = gelu_tanh(pre).astype(BF16)
        return jnp.dot(hidden, w_second, preferred_element_type=F32).astype(BF16)

    feats = jnp.concatenate([query_features[:LOW], passage_features[:LOW]], axis=0)
    base = tower(feats)
    qs = gathered(base[:LOW])

    feats = along_line(feats)
    feats = feats + [swap_core(x) for x in feats]

    p_send, q_tail = tail_rows(
        heavy_at, arrived.reshape(16, UNIT, -1), base[LOW:], pos, w_first, w_second
    )
    p_all = plane_exchange(p_send.reshape(16 * BLOCK, emb_width))
    ts = gathered(q_tail)

    late_counts, group, _ = lax.optimization_barrier((counts, group, q_tail))
    heavy = (late_counts > LOW).astype(jnp.int32)
    devices = jnp.arange(counts.shape[0], dtype=jnp.int32)
    mine = heavy * (devices % 8 == group)
    offsets = jnp.cumsum(late_counts) - late_counts
    over_start = jnp.sum(mine * offsets) + LOW
    group_start = lax.dynamic_slice_in_dim(offsets.reshape(16, 8), group, 1, 1)[:, 0]
    scalars = [heavy_at[0], over_start, lax.axis_index(LINE), lax.axis_index(CORE)]
    scalars = jnp.stack(scalars + [lax.axis_index(PLANE)])
    heavies = jnp.sum(heavy.reshape(16, 8) * jnp.arange(16, dtype=jnp.int32)[:, None], axis=0)
    sc = jnp.concatenate([group_start, scalars, heavies]).astype(jnp.int32)

    each = hidden_width // lax.axis_size(DP)
    unit = jnp.arange(16 * each, dtype=jnp.int32)
    rest = unit - LOW
    unit_of = jnp.where(
        unit < LOW, (unit // 8) * (8 * each) + unit % 8, (rest // 4) * (8 * each) + 8 + rest % 4
    )
    unit_of = unit_of + group * each
    pick = (unit_of[:, None] == jnp.arange(hidden_width, dtype=jnp.int32)[None, :]).astype(BF16)
    first_part = lax.dot_general(
        pick, w_first, (((1,), (1,)), ((), ())), preferred_element_type=F32
    ).astype(BF16)
    second_part = jnp.dot(pick, w_second, preferred_element_type=F32).astype(BF16)
    p_all, first_part = lax.optimization_barrier((p_all, first_part))

    q_all, place, stats = score_stats(sc, qs, ts, p_all, scale)
    stats = stats_exchange(stats)
    q_units, p_units = hidden_units(feats, ts, first_part)
    dp_part, g = score_grads(stats, q_all, p_all, place, scale)
    dp_all = plane_exchange(dp_part)
    dq_own, dq_far = query_grads(sc, p_all, g, scale)

    dq = dq_own + swap_core(dq_far)
    dq_sum = dq[0].astype(BF16).astype(F32)
    arrived = [to_line(dq[k].astype(BF16), k) for k in (1, 2, 3)]
    for part in arrived:
        dq_sum = dq_sum + part.astype(F32)
    dqs = gathered(dq_sum.astype(BF16))

    dp_sum = jnp.sum(dp_all.reshape(16, CHUNK, emb_width).astype(F32), axis=0)
    mean_loss = (dp_sum[BLOCK, 0] + dp_sum[BLOCK + 1, 0] + dp_sum[BLOCK + 2, 0]) / pairs
    dps = gathered(dp_sum[:BLOCK].astype(BF16))
    grads = weight_grads(dqs, q_units, dps, p_units, second_part)
    out = jnp.sum(plane_exchange(grads).reshape(16, 8, -1).astype(F32), axis=0)
    wide = width + emb_width
    tail_out = jnp.concatenate([out[:4, wide:], out[4:, wide : 2 * wide - 640]], axis=1)
    out = jnp.concatenate([out[:, :wide], tail_out], axis=0)
    return (mean_loss, out[:, :width].T, out[:, width:])


def solution(mesh):
    finer = Mesh(mesh.devices.reshape(4, 4, 4, 2), DP)
    placed = (P(DP, None), P(DP, None), P(), P(DP), P(), P())
    return jax.shard_map(
        body,
        mesh=finer,
        in_specs=placed,
        out_specs=(P(), P(None, DP), P(DP, None)),
        check_vma=False,
    )
```

```python
import functools

import jax
import jax.numpy as jnp
from jax import lax
from jax.experimental import pallas as pl
from jax.experimental.pallas import tpu as pltpu
from jax.sharding import Mesh
from jax.sharding import PartitionSpec as P


DP = ("dp_0", "dp_1", "dp_2", "dp_3")
PLANE = ("dp_0", "dp_1")
LINE = "dp_2"
CORE = "dp_3"
F32 = jnp.float32
BF16 = jnp.bfloat16

LOW = 128
UNIT = 8
BLOCK = LOW + UNIT
PAIR = 2 * BLOCK
LOG2E = 1.4426950408889634


def swap_core(x):
    return lax.ppermute(x, CORE, [(0, 1), (1, 0)])


def plane_exchange(x):
    return lax.all_to_all(x, PLANE, 0, 0, tiled=True)


def stats_exchange(x):
    return lax.all_to_all(x, (LINE, CORE), 0, 0, tiled=True)


def from_line(x, k):
    return lax.ppermute(x, LINE, [((i + k) % 4, i) for i in range(4)])


def to_line(x, k):
    return lax.ppermute(x, LINE, [(i, (i + k) % 4) for i in range(4)])


def along_line(x):
    return [x] + [from_line(x, k) for k in (1, 2, 3)]


def gathered(x):
    own = jnp.concatenate(along_line(x), axis=0)
    return (own, swap_core(own))


def place_of(pos, sc):
    over = pos - sc[17]
    slot = jnp.bitwise_and(lax.shift_right_logical(over, 3) + sc[16], 15)
    place = jnp.where(
        (over >= 0) & (over < LOW), slot * BLOCK + LOW + jnp.bitwise_and(over, 7), -1
    )
    for s in range(16):
        at = pos - sc[s]
        place = jnp.where((at >= 0) & (at < LOW), at + s * BLOCK, place)
    return place


def near_index(sc, j):
    return jnp.bitwise_and(j // 2 - sc[18], 3) + 4 * jnp.bitwise_xor(j % 2, sc[19])


def nt_dot(a, b):
    return lax.dot_general(a, b, (((1,), (1,)), ((), ())), preferred_element_type=F32)


def pack_kernel(counts, where, q, p, pos, out, heavy_out):
    heavy_at = jnp.int32(0)
    for s in range(16):
        heavy_at += jnp.where(counts[s * 8 + where[0]] > LOW, s, 0)
    heavy_out[0] = heavy_at
    width = q.shape[1]
    high = lax.shift_right_logical(pos[1:2], 7).astype(F32)
    low = jnp.bitwise_and(pos[1:2], 127).astype(F32)
    line = lax.broadcasted_iota(jnp.int32, (UNIT, LOW), 0)
    code = jnp.where(line == 2, high, jnp.where(line == 3, low, 0.0)).astype(BF16)
    for u in range(16):
        slot = jnp.bitwise_and(heavy_at + u, 15)
        out[slot, :, :width] = q[u * UNIT : (u + 1) * UNIT]
        out[slot, :, width : 2 * width] = p[u * UNIT : (u + 1) * UNIT]
        out[slot, :, 2 * width :] = code


def gelu_parts(v):
    square = v * v
    t = jnp.tanh(0.7978845608028654 * (v + 0.044715 * (square * v)))
    grown = 0.5 * (1.0 + t)
    slope = grown + (0.5 * v) * (1.0 - t * t) * (
        0.7978845608028654 * (1.0 + 3 * 0.044715 * square)
    )
    return (v * grown, slope)


def base_kernel(q, p, w_first, w_second, q_out, p_out, feats):
    feats[:LOW] = q[...]
    feats[LOW:] = p[...]
    pre = jnp.dot(feats[...], w_first[...], preferred_element_type=F32)
    hidden = gelu_parts(pre)[0].astype(BF16)
    emb = jnp.dot(hidden, w_second[...], preferred_element_type=F32).astype(BF16)
    q_out[...] = emb[:LOW]
    p_out[...] = emb[LOW:]


def tail_kernel(heavy_at, arrived, base_p, pos, w_first, w_second, p_out, q_out):
    width, emb_width = w_first.shape[0], w_second.shape[1]
    tail = arrived[heavy_at[0]]
    feats = jnp.concatenate([tail[:, :width], tail[:, width : 2 * width]], axis=0)
    q_out[:, emb_width:] = feats
    pre = jnp.dot(feats, w_first[...], preferred_element_type=F32)
    hidden = gelu_parts(pre)[0].astype(BF16)
    emb = jnp.dot(hidden, w_second[...], preferred_element_type=F32).astype(BF16)
    for s in range(p_out.shape[0]):
        p_out[s, :LOW] = base_p[...]
        p_out[s, LOW:] = emb[UNIT:]
    high = lax.shift_right_logical(pos[0:1], 7).astype(F32)
    low = jnp.bitwise_and(pos[0:1], 127).astype(F32)
    line = lax.broadcasted_iota(jnp.int32, (UNIT, LOW), 0)
    code = tail[:, 2 * width :].astype(F32)
    code = jnp.where(line == 0, high, jnp.where(line == 1, low, code)).astype(BF16)
    q_out[:UNIT, :emb_width] = emb[:UNIT]
    q_out[UNIT:, LOW:emb_width] = jnp.zeros((UNIT, emb_width - LOW), BF16)
    q_out[UNIT:, :LOW] = code


def units_kernel(*refs):
    blocks, tails, (first, rows_q, rows_p, hidden_q, hidden_p, slope_q, slope_p) = (
        refs[:8],
        refs[8:10],
        refs[10:],
    )
    skip = tails[0].shape[1] - rows_q.shape[1]
    for k, block in enumerate(blocks):
        tail = tails[k // 4][(k % 4) * 2 * UNIT : (k % 4 + 1) * 2 * UNIT, skip:]
        at = k * BLOCK
        rows_q[at : at + LOW] = block[:LOW]
        rows_q[at + LOW : at + BLOCK] = tail[:UNIT]
        rows_p[at : at + LOW] = block[LOW:]
        rows_p[at + LOW : at + BLOCK] = tail[UNIT:]
    for rows, hidden, slope in ((rows_q, hidden_q, slope_q), (rows_p, hidden_p, slope_p)):
        value, gain = gelu_parts(nt_dot(first[...], rows[...]))
        hidden[...] = value.astype(BF16)
        slope[...] = gain


def stats_kernel(
    sc, q_own, q_far, t_own, t_far, p, q_out, place_out, stats_out, qs, ts, *, scale
):
    for k, (q, t) in enumerate(((q_own, t_own), (q_far, t_far))):
        for b in range(4):
            qs[4 * k + b] = q[b * LOW : (b + 1) * LOW]
            ts[4 * k + b] = t[b * 16 : (b + 1) * 16, : p.shape[1]]
    lane = lax.broadcasted_iota(jnp.int32, (1, LOW), 1) // UNIT
    codes = []
    spread = jnp.zeros((1, LOW), F32)
    for j in range(8):
        b = near_index(sc, j)
        q_out[j * LOW : (j + 1) * LOW] = qs[b]
        tail = ts[b]
        q_out[8 * LOW + j * UNIT : 8 * LOW + (j + 1) * UNIT] = tail[:UNIT]
        code = tail[UNIT:, :LOW].astype(F32)
        codes.append(code[0:1] * 128.0 + code[1:2])
        unit = jnp.bitwise_and(sc[20] - sc[21 + j], 15)
        part = pltpu.roll(code, jnp.bitwise_and(j - unit, 15) * UNIT, 1)
        spread = jnp.where(lane == j, part[2:3] * 128.0 + part[3:4], spread)
    codes.append(spread[:, : 8 * UNIT])
    place_out[...] = place_of(jnp.concatenate(codes, axis=1).astype(jnp.int32), sc)
    rows = q_out.shape[0]
    pull = scale * LOG2E
    top = jnp.full((1, rows), -1e30, F32)
    total = jnp.zeros((1, rows), F32)
    found = jnp.zeros((1, rows), F32)
    for at in range(0, p.shape[0], PAIR):
        tile = p[at : at + PAIR]
        s = nt_dot(tile, q_out[...])
        row = lax.broadcasted_iota(jnp.int32, s.shape, 0)
        found += jnp.sum(jnp.where(row == place_out[...] - at, s, 0.0), axis=0, keepdims=True)
        new_top = jnp.maximum(top, jnp.max(s, axis=0, keepdims=True))
        total = total * jnp.exp2((top - new_top) * pull) + jnp.sum(
            jnp.exp2(s * pull - new_top * pull), axis=0, keepdims=True
        )
        top = new_top
    line = lax.broadcasted_iota(jnp.int32, (8, rows), 0)
    stats = jnp.where(line == 0, top, jnp.where(line == 1, total, jnp.where(line == 2, found, 0.0)))
    for b in range(8):
        stats_out[b * 8 : (b + 1) * 8] = stats


def grads_kernel(stats, q, p, place, dp_out, g_out, loss_out, dp_ref, g_ref, sems, *, scale):
    rows = q.shape[0]
    pull = scale * LOG2E
    tops = [stats[b * 8 : b * 8 + 1] for b in range(8)]
    top = functools.reduce(jnp.maximum, tops)
    total = jnp.zeros((1, rows), F32)
    found = jnp.zeros((1, rows), F32)
    for b in range(8):
        total += stats[b * 8 + 1 : b * 8 + 2] * jnp.exp2((tops[b] - top) * pull)
        found += stats[b * 8 + 2 : b * 8 + 3]
    norm = top * scale + jnp.log(total)
    loss = jnp.sum(norm - found * scale, axis=1, keepdims=True)
    norm = norm * LOG2E
    loss_high = loss.astype(BF16).astype(F32)
    loss_mid = (loss - loss_high).astype(BF16).astype(F32)
    loss_low = loss - loss_high - loss_mid
    line = jnp.bitwise_and(lax.broadcasted_iota(jnp.int32, loss_out.shape, 0), 3)
    loss_out[...] = jnp.where(
        line == 0,
        loss_high,
        jnp.where(line == 1, loss_mid, jnp.where(line == 2, loss_low, 0.0)),
    )
    copies = []

    def send(src, dst, rows):
        copy = pltpu.make_async_copy(src.at[rows], dst.at[rows], sems.at[len(copies)])
        copy.start()
        copies.append(copy)

    for at in range(0, p.shape[0], PAIR):
        s = nt_dot(p[at : at + PAIR], q[...])
        row = lax.broadcasted_iota(jnp.int32, s.shape, 0)
        e = jnp.exp2(s * pull - norm)
        g_ref[at : at + PAIR] = jnp.where(row == place[...] - at, e - 1.0, e).astype(BF16)
        send(g_ref, g_out, pl.ds(at, PAIR))
    for k in range(p.shape[0] // PAIR):
        dp = scale * jnp.dot(g_ref[k * PAIR : (k + 1) * PAIR], q[...], preferred_element_type=F32)
        dp_ref[k * PAIR : (k + 1) * PAIR] = dp.astype(BF16)
        send(dp_ref, dp_out, pl.ds(k * PAIR, PAIR))
    for copy in copies:
        copy.wait()


def query_kernel(sc, p, g, own, far, *, scale):
    def put(j, rows, part):
        b = near_index(sc, j)

        @pl.when(b < 4)
        def _():
            own[b, rows] = part

        @pl.when(b >= 4)
        def _():
            far[b - 4, rows] = part

    def part(first, size):
        dq = lax.dot_general(
            g[:, first : first + size], p[...], (((0,), (0,)), ((), ())), preferred_element_type=F32
        )
        return scale * dq

    for k in range(2):
        dq = part(4 * k * LOW, 4 * LOW)
        for j in range(4):
            put(4 * k + j, slice(0, LOW), dq[j * LOW : (j + 1) * LOW])
    dq = part(8 * LOW, 8 * UNIT)
    for j in range(8):
        put(j, slice(LOW, BLOCK), dq[j * UNIT : (j + 1) * UNIT])


def total_kernel(parts, out):
    total = parts[:BLOCK].astype(F32)
    for k in range(1, 16):
        total += parts[k * BLOCK : (k + 1) * BLOCK].astype(F32)
    out[...] = total.astype(BF16)


def weight_parts(de_own, de_far, hidden, slope, rows, second, de, copies):
    half = de_own.shape[0]
    de[:half] = de_own[...]
    de[half:] = de_far[...]
    back = nt_dot(second[...], de[...])
    copies[0].wait()
    grad_second = jnp.dot(hidden[...], de[...], preferred_element_type=F32)
    copies[1].wait()
    dpre = (slope[...] * back).astype(BF16)
    copies[2].wait()
    grad_first = jnp.dot(dpre, rows[...], preferred_element_type=F32)
    return (grad_first, grad_second)


def weights_kernel(*refs):
    des, (second, loss), units, (out, de), held, sems = (
        refs[:4],
        refs[4:6],
        refs[6:12],
        refs[12:14],
        refs[14:20],
        refs[20],
    )
    copies = [
        pltpu.make_async_copy(unit, hold, sems.at[k])
        for k, (unit, hold) in enumerate(zip(units, held))
    ]
    for copy in copies:
        copy.start()
    first_q, second_q = weight_parts(*des[:2], *held[:3], second, de, copies[:3])
    grad_first, grad_second = weight_parts(*des[2:], *held[3:], second, de, copies[3:])
    grad_first += first_q
    grad_second += second_q
    many = out.shape[0]
    width = grad_first.shape[1]
    wide = width + grad_second.shape[1]
    out[:, :width] = grad_first[:many].astype(BF16)
    out[:, width:wide] = grad_second[:many].astype(BF16)
    rest = grad_first.shape[0] - many
    x = jnp.concatenate(
        [grad_first[many:], grad_second[many:], jnp.concatenate([loss[...]] * (rest // UNIT))],
        axis=1,
    )
    near, far = x[:, :640], x[:, 640:]
    line = jnp.bitwise_and(lax.broadcasted_iota(jnp.int32, near.shape, 0), 7)
    even = jnp.where(line < 4, near, pltpu.roll(far, 4, 0)).astype(BF16)
    odd = jnp.where(line < 4, pltpu.roll(near, rest - 4, 0), far).astype(BF16)
    for b in range(rest // 8):
        out[b * 16 : b * 16 + 8, wide:] = even[b * 8 : (b + 1) * 8]
        out[b * 16 + 8 : b * 16 + 16, wide:] = odd[b * 8 : (b + 1) * 8]


VMEM = pl.BlockSpec(memory_space=pltpu.VMEM)
SMEM = pl.BlockSpec(memory_space=pltpu.SMEM)
HBM = pl.BlockSpec(memory_space=pltpu.HBM)


def pack_overflow(counts, where, q, p, pos):
    width = q.shape[1]
    half = pl.BlockSpec((LOW, width), lambda i: (1, 0))
    return pl.pallas_call(
        pack_kernel,
        grid=(1,),
        in_specs=[SMEM, SMEM, half, half, pl.BlockSpec((2, LOW), lambda i: (0, 0))],
        out_specs=[pl.BlockSpec((16, UNIT, 2 * width + LOW), lambda i: (0, 0, 0)), SMEM],
        out_shape=[
            jax.ShapeDtypeStruct((16, UNIT, 2 * width + LOW), BF16),
            jax.ShapeDtypeStruct((1,), jnp.int32),
        ],
        name="pack_overflow",
    )(counts, where, q, p, pos)


def base_rows(q, p, w_first, w_second):
    width, emb_width = w_first.shape[0], w_second.shape[1]
    rows = pl.BlockSpec((LOW, width), lambda i: (0, 0))

    def whole(shape):
        return pl.BlockSpec(shape, lambda i: (0, 0))

    shapes = [(LOW, emb_width), (LOW, emb_width), (2 * LOW, width)]
    return pl.pallas_call(
        base_kernel,
        grid=(1,),
        in_specs=[rows, rows, whole(w_first.shape), whole(w_second.shape)],
        out_specs=[whole(shape) for shape in shapes],
        out_shape=[jax.ShapeDtypeStruct(shape, BF16) for shape in shapes],
        name="base_rows",
    )(q, p, w_first, w_second)


def tail_rows(heavy_at, arrived, base_p, pos, w_first, w_second):
    emb_width = w_second.shape[1]
    return pl.pallas_call(
        tail_kernel,
        in_specs=[SMEM] + [VMEM] * 5,
        out_specs=[VMEM] * 2,
        out_shape=[
            jax.ShapeDtypeStruct((16, BLOCK, emb_width), BF16),
            jax.ShapeDtypeStruct((2 * UNIT, emb_width + w_first.shape[0]), BF16),
        ],
        name="tail_rows",
    )(heavy_at, arrived, base_p, pos, w_first, w_second)


def hidden_units(blocks, tails, first):
    rows = jax.ShapeDtypeStruct((8 * BLOCK, first.shape[1]), BF16)
    hidden = jax.ShapeDtypeStruct((first.shape[0], 8 * BLOCK), BF16)
    slope = jax.ShapeDtypeStruct((first.shape[0], 8 * BLOCK), F32)
    rows_q, rows_p, hidden_q, hidden_p, slope_q, slope_p = pl.pallas_call(
        units_kernel,
        in_specs=[VMEM] * 11,
        out_specs=[VMEM] * 6,
        out_shape=[rows, rows, hidden, hidden, slope, slope],
        name="hidden_units",
    )(*blocks, *tails, first)
    return ((hidden_q, slope_q, rows_q), (hidden_p, slope_p, rows_p))


def score_stats(sc, qs, ts, p, scale):
    width = p.shape[1]
    rows = 8 * BLOCK
    return pl.pallas_call(
        functools.partial(stats_kernel, scale=scale),
        in_specs=[SMEM] + [VMEM] * 5,
        out_specs=[VMEM] * 3,
        out_shape=[
            jax.ShapeDtypeStruct((rows, width), BF16),
            jax.ShapeDtypeStruct((1, rows), jnp.int32),
            jax.ShapeDtypeStruct((64, rows), F32),
        ],
        scratch_shapes=[pltpu.VMEM((8, LOW, width), BF16), pltpu.VMEM((8, 16, width), BF16)],
        name="score_stats",
    )(sc, *qs, *ts, p)


def score_grads(stats, q, p, place, scale):
    columns, width = p.shape
    rows = q.shape[0]
    steps = columns // PAIR
    return pl.pallas_call(
        functools.partial(grads_kernel, scale=scale),
        in_specs=[VMEM] * 4,
        out_specs=[HBM, HBM, VMEM],
        out_shape=[
            jax.ShapeDtypeStruct((columns, width), BF16),
            jax.ShapeDtypeStruct((columns, rows), BF16),
            jax.ShapeDtypeStruct((UNIT, LOW), F32),
        ],
        scratch_shapes=[
            pltpu.VMEM((columns, width), BF16),
            pltpu.VMEM((columns, rows), BF16),
            pltpu.SemaphoreType.DMA((2 * steps,)),
        ],
        name="score_grads",
    )(stats, q, p, place)


def query_grads(sc, p, g, scale):
    width = p.shape[1]
    return pl.pallas_call(
        functools.partial(query_kernel, scale=scale),
        in_specs=[SMEM, VMEM, VMEM],
        out_specs=[VMEM] * 2,
        out_shape=[jax.ShapeDtypeStruct((4, BLOCK, width), F32)] * 2,
        name="query_grads",
    )(sc, p, g)


def plane_total(parts):
    return pl.pallas_call(
        total_kernel,
        in_specs=[VMEM],
        out_specs=VMEM,
        out_shape=jax.ShapeDtypeStruct((BLOCK, parts.shape[1]), BF16),
        name="plane_total",
    )(parts)


def weight_grads(dqs, q_units, dps, p_units, second, loss):
    held = [pltpu.VMEM(x.shape, x.dtype) for x in (*q_units, *p_units)]
    return pl.pallas_call(
        weights_kernel,
        in_specs=[VMEM] * 6 + [HBM] * 6,
        out_specs=VMEM,
        out_shape=jax.ShapeDtypeStruct((LOW, 1792), BF16),
        scratch_shapes=[pltpu.VMEM((8 * BLOCK, second.shape[1]), BF16)]
        + held
        + [pltpu.SemaphoreType.DMA((6,))],
        name="weight_grads",
    )(*dqs, *dps, second, loss, *q_units, *p_units)


def body(query_features, passage_features, counts, positives, w_first, w_second):
    width = query_features.shape[1]
    hidden_width, emb_width = w_second.shape
    scale = 2.5 * emb_width ** (-0.5)
    group = lax.axis_index((LINE, CORE))
    pairs = BLOCK * lax.axis_size(DP)

    pos = positives.reshape(2, LOW)
    where = jnp.reshape(group, (1,)).astype(jnp.int32)
    over, heavy_at = pack_overflow(counts, where, query_features, passage_features, pos)
    over = over.reshape(16 * UNIT, -1)
    arrived = plane_exchange(over)

    q_base, p_base, feats = base_rows(query_features, passage_features, w_first, w_second)
    qs = gathered(q_base)

    feats = along_line(feats)
    feats = feats + [swap_core(x) for x in feats]

    p_send, q_tail = tail_rows(
        heavy_at, arrived.reshape(16, UNIT, -1), p_base, pos, w_first, w_second
    )
    p_all = plane_exchange(p_send.reshape(16 * BLOCK, emb_width))
    ts = gathered(q_tail)

    late_counts, group, _ = lax.optimization_barrier((counts, group, q_tail))
    heavy = (late_counts > LOW).astype(jnp.int32)
    devices = jnp.arange(counts.shape[0], dtype=jnp.int32)
    mine = heavy * (devices % 8 == group)
    offsets = jnp.cumsum(late_counts) - late_counts
    over_start = jnp.sum(mine * offsets) + LOW
    group_start = lax.dynamic_slice_in_dim(offsets.reshape(16, 8), group, 1, 1)[:, 0]
    scalars = [heavy_at[0], over_start, lax.axis_index(LINE), lax.axis_index(CORE)]
    scalars = jnp.stack(scalars + [lax.axis_index(PLANE)])
    heavies = jnp.sum(heavy.reshape(16, 8) * jnp.arange(16, dtype=jnp.int32)[:, None], axis=0)
    sc = jnp.concatenate([group_start, scalars, heavies]).astype(jnp.int32)

    each = hidden_width // lax.axis_size(DP)
    unit = jnp.arange(16 * each, dtype=jnp.int32)
    rest = unit - LOW
    unit_of = jnp.where(
        unit < LOW, (unit // 8) * (8 * each) + unit % 8, (rest // 4) * (8 * each) + 8 + rest % 4
    )
    unit_of = unit_of + group * each
    pick = (unit_of[:, None] == jnp.arange(hidden_width, dtype=jnp.int32)[None, :]).astype(BF16)
    first_part = lax.dot_general(
        pick, w_first, (((1,), (1,)), ((), ())), preferred_element_type=F32
    ).astype(BF16)
    second_part = jnp.dot(pick, w_second, preferred_element_type=F32).astype(BF16)
    p_all, first_part = lax.optimization_barrier((p_all, first_part))

    q_all, place, stats = score_stats(sc, qs, ts, p_all, scale)
    stats = stats_exchange(stats)
    q_units, p_units = hidden_units(feats, ts, first_part)
    dp_part, g, loss = score_grads(stats, q_all, p_all, place, scale)
    dp_all = plane_exchange(dp_part)
    dq_own, dq_far = query_grads(sc, p_all, g, scale)

    dq = dq_own + swap_core(dq_far)
    dq_sum = dq[0].astype(BF16).astype(F32)
    arrived = [to_line(dq[k].astype(BF16), k) for k in (1, 2, 3)]
    for part in arrived:
        dq_sum = dq_sum + part.astype(F32)
    dqs = gathered(dq_sum.astype(BF16))

    dp_sum = plane_total(dp_all)
    dps = gathered(dp_sum)
    grads = weight_grads(dqs, q_units, dps, p_units, second_part, loss)
    out = jnp.sum(plane_exchange(grads).reshape(16, 8, -1).astype(F32), axis=0)
    wide = width + emb_width
    mean_loss = (out[4, -1] + out[5, -1] + out[6, -1]) / pairs
    tail_out = jnp.concatenate([out[:4, wide:], out[4:, wide : 2 * wide - 640]], axis=1)
    out = jnp.concatenate([out[:, :wide], tail_out], axis=0)
    return (mean_loss, out[:, :width].T, out[:, width:])


def solution(mesh):
    finer = Mesh(mesh.devices.reshape(4, 4, 4, 2), DP)
    placed = (P(DP, None), P(DP, None), P(), P(DP), P(), P())
    return jax.shard_map(
        body,
        mesh=finer,
        in_specs=placed,
        out_specs=(P(), P(None, DP), P(DP, None)),
        check_vma=False,
    )
```

```python
import functools

import jax
import jax.numpy as jnp
from jax import lax
from jax.experimental import pallas as pl
from jax.experimental.pallas import tpu as pltpu
from jax.sharding import Mesh
from jax.sharding import PartitionSpec as P


DP = ("dp_0", "dp_1", "dp_2", "dp_3")
PLANE = ("dp_0", "dp_1")
LINE = "dp_2"
CORE = "dp_3"
F32 = jnp.float32
BF16 = jnp.bfloat16

LOW = 128
UNIT = 8
BLOCK = LOW + UNIT
CHUNK = 144
PAIR = 2 * BLOCK
LOG2E = 1.4426950408889634


def swap_core(x):
    return lax.ppermute(x, CORE, [(0, 1), (1, 0)])


def plane_exchange(x):
    return lax.all_to_all(x, PLANE, 0, 0, tiled=True)


def stats_exchange(x):
    return lax.all_to_all(x, (LINE, CORE), 0, 0, tiled=True)


def from_line(x, k):
    return lax.ppermute(x, LINE, [((i + k) % 4, i) for i in range(4)])


def to_line(x, k):
    return lax.ppermute(x, LINE, [(i, (i + k) % 4) for i in range(4)])


def along_line(x):
    return [x] + [from_line(x, k) for k in (1, 2, 3)]


def gathered(x):
    own = jnp.concatenate(along_line(x), axis=0)
    return (own, swap_core(own))


def place_of(pos, sc):
    over = pos - sc[17]
    slot = jnp.bitwise_and(lax.shift_right_logical(over, 3) + sc[16], 15)
    place = jnp.where(
        (over >= 0) & (over < LOW), slot * BLOCK + LOW + jnp.bitwise_and(over, 7), -1
    )
    for s in range(16):
        at = pos - sc[s]
        place = jnp.where((at >= 0) & (at < LOW), at + s * BLOCK, place)
    return place


def near_index(sc, j):
    return jnp.bitwise_and(j // 2 - sc[18], 3) + 4 * jnp.bitwise_xor(j % 2, sc[19])


def nt_dot(a, b):
    return lax.dot_general(a, b, (((1,), (1,)), ((), ())), preferred_element_type=F32)


def pack_kernel(counts, where, q, p, pos, out, heavy_out):
    heavy_at = jnp.int32(0)
    for s in range(16):
        heavy_at += jnp.where(counts[s * 8 + where[0]] > LOW, s, 0)
    heavy_out[0] = heavy_at
    width = q.shape[1]
    high = lax.shift_right_logical(pos[1:2], 7).astype(F32)
    low = jnp.bitwise_and(pos[1:2], 127).astype(F32)
    line = lax.broadcasted_iota(jnp.int32, (UNIT, LOW), 0)
    code = jnp.where(line == 2, high, jnp.where(line == 3, low, 0.0)).astype(BF16)
    for u in range(16):
        slot = jnp.bitwise_and(heavy_at + u, 15)
        out[slot, :, :width] = q[u * UNIT : (u + 1) * UNIT]
        out[slot, :, width : 2 * width] = p[u * UNIT : (u + 1) * UNIT]
        out[slot, :, 2 * width :] = code


def gelu_parts(v):
    square = v * v
    t = jnp.tanh(0.7978845608028654 * (v + 0.044715 * (square * v)))
    grown = 0.5 * (1.0 + t)
    slope = grown + (0.5 * v) * (1.0 - t * t) * (
        0.7978845608028654 * (1.0 + 3 * 0.044715 * square)
    )
    return (v * grown, slope)


def base_kernel(q, p, w_first, w_second, emb, feats):
    feats[:LOW] = q[...]
    feats[LOW:] = p[...]
    pre = jnp.dot(feats[...], w_first[...], preferred_element_type=F32)
    hidden = gelu_parts(pre)[0].astype(BF16)
    emb[...] = jnp.dot(hidden, w_second[...], preferred_element_type=F32).astype(BF16)


def tail_kernel(heavy_at, arrived, base_p, pos, w_first, w_second, p_out, q_out):
    width, emb_width = w_first.shape[0], w_second.shape[1]
    tail = arrived[heavy_at[0]]
    feats = jnp.concatenate([tail[:, :width], tail[:, width : 2 * width]], axis=0)
    q_out[:, emb_width:] = feats
    pre = jnp.dot(feats, w_first[...], preferred_element_type=F32)
    hidden = gelu_parts(pre)[0].astype(BF16)
    emb = jnp.dot(hidden, w_second[...], preferred_element_type=F32).astype(BF16)
    for s in range(p_out.shape[0]):
        p_out[s, :LOW] = base_p[...]
        p_out[s, LOW:] = emb[UNIT:]
    high = lax.shift_right_logical(pos[0:1], 7).astype(F32)
    low = jnp.bitwise_and(pos[0:1], 127).astype(F32)
    line = lax.broadcasted_iota(jnp.int32, (UNIT, LOW), 0)
    code = tail[:, 2 * width :].astype(F32)
    code = jnp.where(line == 0, high, jnp.where(line == 1, low, code)).astype(BF16)
    q_out[:UNIT, :emb_width] = emb[:UNIT]
    q_out[UNIT:, LOW:emb_width] = jnp.zeros((UNIT, emb_width - LOW), BF16)
    q_out[UNIT:, :LOW] = code


def units_kernel(*refs):
    blocks, tails, (first, rows_q, rows_p, hidden_q, hidden_p, slope_q, slope_p) = (
        refs[:8],
        refs[8:10],
        refs[10:],
    )
    skip = tails[0].shape[1] - rows_q.shape[1]
    for k, block in enumerate(blocks):
        tail = tails[k // 4][(k % 4) * 2 * UNIT : (k % 4 + 1) * 2 * UNIT, skip:]
        at = k * BLOCK
        rows_q[at : at + LOW] = block[:LOW]
        rows_q[at + LOW : at + BLOCK] = tail[:UNIT]
        rows_p[at : at + LOW] = block[LOW:]
        rows_p[at + LOW : at + BLOCK] = tail[UNIT:]
    for rows, hidden, slope in ((rows_q, hidden_q, slope_q), (rows_p, hidden_p, slope_p)):
        value, gain = gelu_parts(nt_dot(first[...], rows[...]))
        hidden[...] = value.astype(BF16)
        slope[...] = gain


def stats_kernel(
    sc, q_own, q_far, t_own, t_far, p, q_out, place_out, stats_out, qs, ts, *, scale
):
    for k, (q, t) in enumerate(((q_own, t_own), (q_far, t_far))):
        for b in range(4):
            qs[4 * k + b] = q[b * LOW : (b + 1) * LOW]
            ts[4 * k + b] = t[b * 16 : (b + 1) * 16, : p.shape[1]]
    lane = lax.broadcasted_iota(jnp.int32, (1, LOW), 1) // UNIT
    codes = []
    spread = jnp.zeros((1, LOW), F32)
    for j in range(8):
        b = near_index(sc, j)
        q_out[j * LOW : (j + 1) * LOW] = qs[b]
        tail = ts[b]
        q_out[8 * LOW + j * UNIT : 8 * LOW + (j + 1) * UNIT] = tail[:UNIT]
        code = tail[UNIT:, :LOW].astype(F32)
        codes.append(code[0:1] * 128.0 + code[1:2])
        unit = jnp.bitwise_and(sc[20] - sc[21 + j], 15)
        part = pltpu.roll(code, jnp.bitwise_and(j - unit, 15) * UNIT, 1)
        spread = jnp.where(lane == j, part[2:3] * 128.0 + part[3:4], spread)
    codes.append(spread[:, : 8 * UNIT])
    place_out[...] = place_of(jnp.concatenate(codes, axis=1).astype(jnp.int32), sc)
    rows = q_out.shape[0]
    pull = scale * LOG2E
    top = jnp.full((1, rows), -1e30, F32)
    total = jnp.zeros((1, rows), F32)
    found = jnp.zeros((1, rows), F32)
    for at in range(0, p.shape[0], PAIR):
        tile = p[at : at + PAIR]
        s = nt_dot(tile, q_out[...])
        row = lax.broadcasted_iota(jnp.int32, s.shape, 0)
        found += jnp.sum(jnp.where(row == place_out[...] - at, s, 0.0), axis=0, keepdims=True)
        new_top = jnp.maximum(top, jnp.max(s, axis=0, keepdims=True))
        total = total * jnp.exp2((top - new_top) * pull) + jnp.sum(
            jnp.exp2(s * pull - new_top * pull), axis=0, keepdims=True
        )
        top = new_top
    line = lax.broadcasted_iota(jnp.int32, (8, rows), 0)
    stats = jnp.where(line == 0, top, jnp.where(line == 1, total, jnp.where(line == 2, found, 0.0)))
    for b in range(8):
        stats_out[b * 8 : (b + 1) * 8] = stats


def grads_kernel(stats, q, p, place, dp_out, g_out, dp_ref, g_ref, sems, *, scale):
    rows, width = q.shape
    pull = scale * LOG2E
    tops = [stats[b * 8 : b * 8 + 1] for b in range(8)]
    top = functools.reduce(jnp.maximum, tops)
    total = jnp.zeros((1, rows), F32)
    found = jnp.zeros((1, rows), F32)
    for b in range(8):
        total += stats[b * 8 + 1 : b * 8 + 2] * jnp.exp2((tops[b] - top) * pull)
        found += stats[b * 8 + 2 : b * 8 + 3]
    norm = top * scale + jnp.log(total)
    loss = jnp.sum(norm - found * scale, axis=1, keepdims=True)
    norm = norm * LOG2E
    loss_high = loss.astype(BF16).astype(F32)
    loss_mid = (loss - loss_high).astype(BF16).astype(F32)
    loss_low = loss - loss_high - loss_mid
    line = lax.broadcasted_iota(jnp.int32, (UNIT, width), 0)
    loss_tile = jnp.where(
        line == 0,
        loss_high,
        jnp.where(line == 1, loss_mid, jnp.where(line == 2, loss_low, 0.0)),
    ).astype(BF16)
    copies = []

    def send(src, dst, rows):
        copy = pltpu.make_async_copy(src.at[rows], dst.at[rows], sems.at[len(copies)])
        copy.start()
        copies.append(copy)

    for at in range(0, p.shape[0], PAIR):
        s = nt_dot(p[at : at + PAIR], q[...])
        row = lax.broadcasted_iota(jnp.int32, s.shape, 0)
        e = jnp.exp2(s * pull - norm)
        g_ref[at : at + PAIR] = jnp.where(row == place[...] - at, e - 1.0, e).astype(BF16)
        send(g_ref, g_out, pl.ds(at, PAIR))
    for k in range(p.shape[0] // PAIR):
        dp = scale * jnp.dot(g_ref[k * PAIR : (k + 1) * PAIR], q[...], preferred_element_type=F32)
        dp = dp.astype(BF16)
        for half in range(2):
            to = (2 * k + half) * CHUNK
            dp_ref[to : to + BLOCK] = dp[half * BLOCK : (half + 1) * BLOCK]
            dp_ref[to + BLOCK : to + CHUNK] = loss_tile
        send(dp_ref, dp_out, pl.ds(2 * k * CHUNK, 2 * CHUNK))
    for copy in copies:
        copy.wait()


def query_kernel(sc, p, g, own, far, *, scale):
    def put(j, rows, part):
        b = near_index(sc, j)

        @pl.when(b < 4)
        def _():
            own[b, rows] = part

        @pl.when(b >= 4)
        def _():
            far[b - 4, rows] = part

    def part(first, size):
        dq = lax.dot_general(
            g[:, first : first + size], p[...], (((0,), (0,)), ((), ())), preferred_element_type=F32
        )
        return scale * dq

    for k in range(2):
        dq = part(4 * k * LOW, 4 * LOW)
        for j in range(4):
            put(4 * k + j, slice(0, LOW), dq[j * LOW : (j + 1) * LOW])
    dq = part(8 * LOW, 8 * UNIT)
    for j in range(8):
        put(j, slice(LOW, BLOCK), dq[j * UNIT : (j + 1) * UNIT])


def weight_parts(de_own, de_far, hidden, slope, rows, second, de, copies):
    half = de_own.shape[0]
    de[:half] = de_own[...]
    de[half:] = de_far[...]
    back = nt_dot(second[...], de[...])
    copies[0].wait()
    grad_second = jnp.dot(hidden[...], de[...], preferred_element_type=F32)
    copies[1].wait()
    dpre = (slope[...] * back).astype(BF16)
    copies[2].wait()
    grad_first = jnp.dot(dpre, rows[...], preferred_element_type=F32)
    return (grad_first, grad_second)


def weights_kernel(*refs):
    des, second, units, (out, de), held, sems = (
        refs[:4],
        refs[4],
        refs[5:11],
        refs[11:13],
        refs[13:19],
        refs[19],
    )
    copies = [
        pltpu.make_async_copy(unit, hold, sems.at[k])
        for k, (unit, hold) in enumerate(zip(units, held))
    ]
    for copy in copies:
        copy.start()
    first_q, second_q = weight_parts(*des[:2], *held[:3], second, de, copies[:3])
    grad_first, grad_second = weight_parts(*des[2:], *held[3:], second, de, copies[3:])
    grad_first += first_q
    grad_second += second_q
    many = out.shape[0]
    width = grad_first.shape[1]
    wide = width + grad_second.shape[1]
    out[:, :width] = grad_first[:many].astype(BF16)
    out[:, width:wide] = grad_second[:many].astype(BF16)
    rest = grad_first.shape[0] - many
    x = jnp.concatenate(
        [grad_first[many:], grad_second[many:], jnp.zeros((rest, 128), F32)], axis=1
    )
    near, far = x[:, :640], x[:, 640:]
    line = jnp.bitwise_and(lax.broadcasted_iota(jnp.int32, near.shape, 0), 7)
    even = jnp.where(line < 4, near, pltpu.roll(far, 4, 0)).astype(BF16)
    odd = jnp.where(line < 4, pltpu.roll(near, rest - 4, 0), far).astype(BF16)
    for b in range(rest // 8):
        out[b * 16 : b * 16 + 8, wide:] = even[b * 8 : (b + 1) * 8]
        out[b * 16 + 8 : b * 16 + 16, wide:] = odd[b * 8 : (b + 1) * 8]


VMEM = pl.BlockSpec(memory_space=pltpu.VMEM)
SMEM = pl.BlockSpec(memory_space=pltpu.SMEM)
HBM = pl.BlockSpec(memory_space=pltpu.HBM)


def pack_overflow(counts, where, q, p, pos):
    width = q.shape[1]
    half = pl.BlockSpec((LOW, width), lambda i: (1, 0))
    return pl.pallas_call(
        pack_kernel,
        grid=(1,),
        in_specs=[SMEM, SMEM, half, half, pl.BlockSpec((2, LOW), lambda i: (0, 0))],
        out_specs=[pl.BlockSpec((16, UNIT, 2 * width + LOW), lambda i: (0, 0, 0)), SMEM],
        out_shape=[
            jax.ShapeDtypeStruct((16, UNIT, 2 * width + LOW), BF16),
            jax.ShapeDtypeStruct((1,), jnp.int32),
        ],
        name="pack_overflow",
    )(counts, where, q, p, pos)


def base_rows(q, p, w_first, w_second):
    width, emb_width = w_first.shape[0], w_second.shape[1]
    rows = pl.BlockSpec((LOW, width), lambda i: (0, 0))

    def whole(shape):
        return pl.BlockSpec(shape, lambda i: (0, 0))

    shapes = [(2 * LOW, emb_width), (2 * LOW, width)]
    return pl.pallas_call(
        base_kernel,
        grid=(1,),
        in_specs=[rows, rows, whole(w_first.shape), whole(w_second.shape)],
        out_specs=[whole(shape) for shape in shapes],
        out_shape=[jax.ShapeDtypeStruct(shape, BF16) for shape in shapes],
        name="base_rows",
    )(q, p, w_first, w_second)


def tail_rows(heavy_at, arrived, base_p, pos, w_first, w_second):
    emb_width = w_second.shape[1]
    return pl.pallas_call(
        tail_kernel,
        in_specs=[SMEM] + [VMEM] * 5,
        out_specs=[VMEM] * 2,
        out_shape=[
            jax.ShapeDtypeStruct((16, BLOCK, emb_width), BF16),
            jax.ShapeDtypeStruct((2 * UNIT, emb_width + w_first.shape[0]), BF16),
        ],
        name="tail_rows",
    )(heavy_at, arrived, base_p, pos, w_first, w_second)


def hidden_units(blocks, tails, first):
    rows = jax.ShapeDtypeStruct((8 * BLOCK, first.shape[1]), BF16)
    hidden = jax.ShapeDtypeStruct((first.shape[0], 8 * BLOCK), BF16)
    slope = jax.ShapeDtypeStruct((first.shape[0], 8 * BLOCK), F32)
    rows_q, rows_p, hidden_q, hidden_p, slope_q, slope_p = pl.pallas_call(
        units_kernel,
        in_specs=[VMEM] * 11,
        out_specs=[VMEM] * 6,
        out_shape=[rows, rows, hidden, hidden, slope, slope],
        name="hidden_units",
    )(*blocks, *tails, first)
    return ((hidden_q, slope_q, rows_q), (hidden_p, slope_p, rows_p))


def score_stats(sc, qs, ts, p, scale):
    width = p.shape[1]
    rows = 8 * BLOCK
    return pl.pallas_call(
        functools.partial(stats_kernel, scale=scale),
        in_specs=[SMEM] + [VMEM] * 5,
        out_specs=[VMEM] * 3,
        out_shape=[
            jax.ShapeDtypeStruct((rows, width), BF16),
            jax.ShapeDtypeStruct((1, rows), jnp.int32),
            jax.ShapeDtypeStruct((64, rows), F32),
        ],
        scratch_shapes=[pltpu.VMEM((8, LOW, width), BF16), pltpu.VMEM((8, 16, width), BF16)],
        name="score_stats",
    )(sc, *qs, *ts, p)


def score_grads(stats, q, p, place, scale):
    columns, width = p.shape
    rows = q.shape[0]
    steps = columns // PAIR
    return pl.pallas_call(
        functools.partial(grads_kernel, scale=scale),
        in_specs=[VMEM] * 4,
        out_specs=[HBM] * 2,
        out_shape=[
            jax.ShapeDtypeStruct((2 * steps * CHUNK, width), BF16),
            jax.ShapeDtypeStruct((columns, rows), BF16),
        ],
        scratch_shapes=[
            pltpu.VMEM((2 * steps * CHUNK, width), BF16),
            pltpu.VMEM((columns, rows), BF16),
            pltpu.SemaphoreType.DMA((2 * steps,)),
        ],
        name="score_grads",
    )(stats, q, p, place)


def query_grads(sc, p, g, scale):
    width = p.shape[1]
    return pl.pallas_call(
        functools.partial(query_kernel, scale=scale),
        in_specs=[SMEM, VMEM, VMEM],
        out_specs=[VMEM] * 2,
        out_shape=[jax.ShapeDtypeStruct((4, BLOCK, width), F32)] * 2,
        name="query_grads",
    )(sc, p, g)


def weight_grads(dqs, q_units, dps, p_units, second):
    held = [pltpu.VMEM(x.shape, x.dtype) for x in (*q_units, *p_units)]
    return pl.pallas_call(
        weights_kernel,
        in_specs=[VMEM] * 5 + [HBM] * 6,
        out_specs=VMEM,
        out_shape=jax.ShapeDtypeStruct((LOW, 1792), BF16),
        scratch_shapes=[pltpu.VMEM((8 * BLOCK, second.shape[1]), BF16)]
        + held
        + [pltpu.SemaphoreType.DMA((6,))],
        name="weight_grads",
    )(*dqs, *dps, second, *q_units, *p_units)


def body(query_features, passage_features, counts, positives, w_first, w_second):
    width = query_features.shape[1]
    hidden_width, emb_width = w_second.shape
    scale = 2.5 * emb_width ** (-0.5)
    group = lax.axis_index((LINE, CORE))
    pairs = BLOCK * lax.axis_size(DP)

    pos = positives.reshape(2, LOW)
    where = jnp.reshape(group, (1,)).astype(jnp.int32)
    over, heavy_at = pack_overflow(counts, where, query_features, passage_features, pos)
    over = over.reshape(16 * UNIT, -1)
    arrived = plane_exchange(over)

    base, feats = base_rows(query_features, passage_features, w_first, w_second)
    qs = gathered(base[:LOW])

    feats = along_line(feats)
    feats = feats + [swap_core(x) for x in feats]

    p_send, q_tail = tail_rows(
        heavy_at, arrived.reshape(16, UNIT, -1), base[LOW:], pos, w_first, w_second
    )
    p_all = plane_exchange(p_send.reshape(16 * BLOCK, emb_width))
    ts = gathered(q_tail)

    late_counts, group, _ = lax.optimization_barrier((counts, group, q_tail))
    heavy = (late_counts > LOW).astype(jnp.int32)
    devices = jnp.arange(counts.shape[0], dtype=jnp.int32)
    mine = heavy * (devices % 8 == group)
    offsets = jnp.cumsum(late_counts) - late_counts
    over_start = jnp.sum(mine * offsets) + LOW
    group_start = lax.dynamic_slice_in_dim(offsets.reshape(16, 8), group, 1, 1)[:, 0]
    scalars = [heavy_at[0], over_start, lax.axis_index(LINE), lax.axis_index(CORE)]
    scalars = jnp.stack(scalars + [lax.axis_index(PLANE)])
    heavies = jnp.sum(heavy.reshape(16, 8) * jnp.arange(16, dtype=jnp.int32)[:, None], axis=0)
    sc = jnp.concatenate([group_start, scalars, heavies]).astype(jnp.int32)

    each = hidden_width // lax.axis_size(DP)
    unit = jnp.arange(16 * each, dtype=jnp.int32)
    rest = unit - LOW
    unit_of = jnp.where(
        unit < LOW, (unit // 8) * (8 * each) + unit % 8, (rest // 4) * (8 * each) + 8 + rest % 4
    )
    unit_of = unit_of + group * each
    pick = (unit_of[:, None] == jnp.arange(hidden_width, dtype=jnp.int32)[None, :]).astype(BF16)
    first_part = lax.dot_general(
        pick, w_first, (((1,), (1,)), ((), ())), preferred_element_type=F32
    ).astype(BF16)
    second_part = jnp.dot(pick, w_second, preferred_element_type=F32).astype(BF16)
    p_all, first_part = lax.optimization_barrier((p_all, first_part))

    q_all, place, stats = score_stats(sc, qs, ts, p_all, scale)
    stats = stats_exchange(stats)
    q_units, p_units = hidden_units(feats, ts, first_part)
    dp_part, g = score_grads(stats, q_all, p_all, place, scale)
    dp_all = plane_exchange(dp_part)
    dq_own, dq_far = query_grads(sc, p_all, g, scale)

    dq = dq_own + swap_core(dq_far)
    dq_sum = dq[0].astype(BF16).astype(F32)
    arrived = [to_line(dq[k].astype(BF16), k) for k in (1, 2, 3)]
    for part in arrived:
        dq_sum = dq_sum + part.astype(F32)
    dqs = gathered(dq_sum.astype(BF16))

    dp_sum = jnp.sum(dp_all.reshape(16, CHUNK, emb_width).astype(F32), axis=0)
    mean_loss = (dp_sum[BLOCK, 0] + dp_sum[BLOCK + 1, 0] + dp_sum[BLOCK + 2, 0]) / pairs
    dps = gathered(dp_sum[:BLOCK].astype(BF16))
    grads = weight_grads(dqs, q_units, dps, p_units, second_part)
    out = jnp.sum(plane_exchange(grads).reshape(16, 8, -1).astype(F32), axis=0)
    wide = width + emb_width
    tail_out = jnp.concatenate([out[:4, wide:], out[4:, wide : 2 * wide - 640]], axis=1)
    out = jnp.concatenate([out[:, :wide], tail_out], axis=0)
    return (mean_loss, out[:, :width].T, out[:, width:])


def solution(mesh):
    finer = Mesh(mesh.devices.reshape(4, 4, 4, 2), DP)
    placed = (P(DP, None), P(DP, None), P(), P(DP), P(), P())
    return jax.shard_map(
        body,
        mesh=finer,
        in_specs=placed,
        out_specs=(P(), P(None, DP), P(DP, None)),
        check_vma=False,
    )
```

```python
import functools

import jax
import jax.numpy as jnp
from jax import lax
from jax.experimental import pallas as pl
from jax.experimental.pallas import tpu as pltpu
from jax.sharding import Mesh
from jax.sharding import PartitionSpec as P


DP = ("dp_0", "dp_1", "dp_2", "dp_3")
PLANE = ("dp_0", "dp_1")
LINE = "dp_2"
CORE = "dp_3"
F32 = jnp.float32
BF16 = jnp.bfloat16

LOW = 128
UNIT = 8
BLOCK = LOW + UNIT
CHUNK = 144
PAIR = 2 * BLOCK
LOG2E = 1.4426950408889634


def swap_core(x):
    return lax.ppermute(x, CORE, [(0, 1), (1, 0)])


def plane_exchange(x):
    return lax.all_to_all(x, PLANE, 0, 0, tiled=True)


def stats_exchange(x):
    return lax.all_to_all(x, (LINE, CORE), 0, 0, tiled=True)


def from_line(x, k):
    return lax.ppermute(x, LINE, [((i + k) % 4, i) for i in range(4)])


def to_line(x, k):
    return lax.ppermute(x, LINE, [(i, (i + k) % 4) for i in range(4)])


def along_line(x):
    return [x] + [from_line(x, k) for k in (1, 2, 3)]


def gathered(x):
    own = jnp.concatenate(along_line(x), axis=0)
    return (own, swap_core(own))


def place_of(pos, sc):
    over = pos - sc[17]
    slot = jnp.bitwise_and(lax.shift_right_logical(over, 3) + sc[16], 15)
    place = jnp.where(
        (over >= 0) & (over < LOW), slot * BLOCK + LOW + jnp.bitwise_and(over, 7), -1
    )
    for s in range(16):
        at = pos - sc[s]
        place = jnp.where((at >= 0) & (at < LOW), at + s * BLOCK, place)
    return place


def near_index(sc, j):
    return jnp.bitwise_and(j // 2 - sc[18], 3) + 4 * jnp.bitwise_xor(j % 2, sc[19])


def nt_dot(a, b):
    return lax.dot_general(a, b, (((1,), (1,)), ((), ())), preferred_element_type=F32)


def pack_kernel(counts, where, q, p, pos, out, heavy_out):
    heavy_at = jnp.int32(0)
    for s in range(16):
        heavy_at += jnp.where(counts[s * 8 + where[0]] > LOW, s, 0)
    heavy_out[0] = heavy_at
    width = q.shape[1]
    high = lax.shift_right_logical(pos[1:2], 7).astype(F32)
    low = jnp.bitwise_and(pos[1:2], 127).astype(F32)
    line = lax.broadcasted_iota(jnp.int32, (UNIT, LOW), 0)
    code = jnp.where(line == 2, high, jnp.where(line == 3, low, 0.0)).astype(BF16)
    for u in range(16):
        slot = jnp.bitwise_and(heavy_at + u, 15)
        out[slot, :, :width] = q[u * UNIT : (u + 1) * UNIT]
        out[slot, :, width : 2 * width] = p[u * UNIT : (u + 1) * UNIT]
        out[slot, :, 2 * width :] = code


def gelu_parts(v):
    square = v * v
    t = jnp.tanh(0.7978845608028654 * (v + 0.044715 * (square * v)))
    grown = 0.5 * (1.0 + t)
    slope = grown + (0.5 * v) * (1.0 - t * t) * (
        0.7978845608028654 * (1.0 + 3 * 0.044715 * square)
    )
    return (v * grown, slope)


def base_kernel(q, p, w_first, w_second, q_out, p_out, feats):
    feats[:LOW] = q[...]
    feats[LOW:] = p[...]
    pre = jnp.dot(feats[...], w_first[...], preferred_element_type=F32)
    hidden = gelu_parts(pre)[0].astype(BF16)
    emb = jnp.dot(hidden, w_second[...], preferred_element_type=F32).astype(BF16)
    q_out[...] = emb[:LOW]
    p_out[...] = emb[LOW:]


def tail_kernel(heavy_at, arrived, base_p, pos, w_first, w_second, p_out, q_out):
    width, emb_width = w_first.shape[0], w_second.shape[1]
    tail = arrived[heavy_at[0]]
    feats = jnp.concatenate([tail[:, :width], tail[:, width : 2 * width]], axis=0)
    q_out[:, emb_width:] = feats
    pre = jnp.dot(feats, w_first[...], preferred_element_type=F32)
    hidden = gelu_parts(pre)[0].astype(BF16)
    emb = jnp.dot(hidden, w_second[...], preferred_element_type=F32).astype(BF16)
    for s in range(p_out.shape[0]):
        p_out[s, :LOW] = base_p[...]
        p_out[s, LOW:] = emb[UNIT:]
    high = lax.shift_right_logical(pos[0:1], 7).astype(F32)
    low = jnp.bitwise_and(pos[0:1], 127).astype(F32)
    line = lax.broadcasted_iota(jnp.int32, (UNIT, LOW), 0)
    code = tail[:, 2 * width :].astype(F32)
    code = jnp.where(line == 0, high, jnp.where(line == 1, low, code)).astype(BF16)
    q_out[:UNIT, :emb_width] = emb[:UNIT]
    q_out[UNIT:, LOW:emb_width] = jnp.zeros((UNIT, emb_width - LOW), BF16)
    q_out[UNIT:, :LOW] = code


def units_kernel(*refs):
    blocks, tails, (first, rows_q, rows_p, hidden_q, hidden_p, slope_q, slope_p) = (
        refs[:8],
        refs[8:10],
        refs[10:],
    )
    skip = tails[0].shape[1] - rows_q.shape[1]
    for k, block in enumerate(blocks):
        tail = tails[k // 4][(k % 4) * 2 * UNIT : (k % 4 + 1) * 2 * UNIT, skip:]
        at = k * BLOCK
        rows_q[at : at + LOW] = block[:LOW]
        rows_q[at + LOW : at + BLOCK] = tail[:UNIT]
        rows_p[at : at + LOW] = block[LOW:]
        rows_p[at + LOW : at + BLOCK] = tail[UNIT:]
    for rows, hidden, slope in ((rows_q, hidden_q, slope_q), (rows_p, hidden_p, slope_p)):
        value, gain = gelu_parts(nt_dot(first[...], rows[...]))
        hidden[...] = value.astype(BF16)
        slope[...] = gain


def stats_kernel(
    sc, q_own, q_far, t_own, t_far, p, q_out, place_out, stats_out, qs, ts, *, scale
):
    for k, (q, t) in enumerate(((q_own, t_own), (q_far, t_far))):
        for b in range(4):
            qs[4 * k + b] = q[b * LOW : (b + 1) * LOW]
            ts[4 * k + b] = t[b * 16 : (b + 1) * 16, : p.shape[1]]
    lane = lax.broadcasted_iota(jnp.int32, (1, LOW), 1) // UNIT
    codes = []
    spread = jnp.zeros((1, LOW), F32)
    for j in range(8):
        b = near_index(sc, j)
        q_out[j * LOW : (j + 1) * LOW] = qs[b]
        tail = ts[b]
        q_out[8 * LOW + j * UNIT : 8 * LOW + (j + 1) * UNIT] = tail[:UNIT]
        code = tail[UNIT:, :LOW].astype(F32)
        codes.append(code[0:1] * 128.0 + code[1:2])
        unit = jnp.bitwise_and(sc[20] - sc[21 + j], 15)
        part = pltpu.roll(code, jnp.bitwise_and(j - unit, 15) * UNIT, 1)
        spread = jnp.where(lane == j, part[2:3] * 128.0 + part[3:4], spread)
    codes.append(spread[:, : 8 * UNIT])
    place_out[...] = place_of(jnp.concatenate(codes, axis=1).astype(jnp.int32), sc)
    rows = q_out.shape[0]
    pull = scale * LOG2E
    top = jnp.full((1, rows), -1e30, F32)
    total = jnp.zeros((1, rows), F32)
    found = jnp.zeros((1, rows), F32)
    for at in range(0, p.shape[0], PAIR):
        tile = p[at : at + PAIR]
        s = nt_dot(tile, q_out[...])
        row = lax.broadcasted_iota(jnp.int32, s.shape, 0)
        found += jnp.sum(jnp.where(row == place_out[...] - at, s, 0.0), axis=0, keepdims=True)
        new_top = jnp.maximum(top, jnp.max(s, axis=0, keepdims=True))
        total = total * jnp.exp2((top - new_top) * pull) + jnp.sum(
            jnp.exp2(s * pull - new_top * pull), axis=0, keepdims=True
        )
        top = new_top
    line = lax.broadcasted_iota(jnp.int32, (8, rows), 0)
    stats = jnp.where(line == 0, top, jnp.where(line == 1, total, jnp.where(line == 2, found, 0.0)))
    for b in range(8):
        stats_out[b * 8 : (b + 1) * 8] = stats


def grads_kernel(stats, q, p, place, dp_out, g_out, dp_ref, g_ref, sems, *, scale):
    rows, width = q.shape
    pull = scale * LOG2E
    tops = [stats[b * 8 : b * 8 + 1] for b in range(8)]
    top = functools.reduce(jnp.maximum, tops)
    total = jnp.zeros((1, rows), F32)
    found = jnp.zeros((1, rows), F32)
    for b in range(8):
        total += stats[b * 8 + 1 : b * 8 + 2] * jnp.exp2((tops[b] - top) * pull)
        found += stats[b * 8 + 2 : b * 8 + 3]
    norm = top * scale + jnp.log(total)
    loss = jnp.sum(norm - found * scale, axis=1, keepdims=True)
    norm = norm * LOG2E
    loss_high = loss.astype(BF16).astype(F32)
    loss_mid = (loss - loss_high).astype(BF16).astype(F32)
    loss_low = loss - loss_high - loss_mid
    line = lax.broadcasted_iota(jnp.int32, (UNIT, width), 0)
    loss_tile = jnp.where(
        line == 0,
        loss_high,
        jnp.where(line == 1, loss_mid, jnp.where(line == 2, loss_low, 0.0)),
    ).astype(BF16)
    copies = []

    def send(src, dst, rows):
        copy = pltpu.make_async_copy(src.at[rows], dst.at[rows], sems.at[len(copies)])
        copy.start()
        copies.append(copy)

    for at in range(0, p.shape[0], PAIR):
        s = nt_dot(p[at : at + PAIR], q[...])
        row = lax.broadcasted_iota(jnp.int32, s.shape, 0)
        e = jnp.exp2(s * pull - norm)
        g_ref[at : at + PAIR] = jnp.where(row == place[...] - at, e - 1.0, e).astype(BF16)
        send(g_ref, g_out, pl.ds(at, PAIR))
    for k in range(p.shape[0] // PAIR):
        dp = scale * jnp.dot(g_ref[k * PAIR : (k + 1) * PAIR], q[...], preferred_element_type=F32)
        dp = dp.astype(BF16)
        for half in range(2):
            to = (2 * k + half) * CHUNK
            dp_ref[to : to + BLOCK] = dp[half * BLOCK : (half + 1) * BLOCK]
            dp_ref[to + BLOCK : to + CHUNK] = loss_tile
        send(dp_ref, dp_out, pl.ds(2 * k * CHUNK, 2 * CHUNK))
    for copy in copies:
        copy.wait()


def query_kernel(sc, p, g, own, far, *, scale):
    def put(j, rows, part):
        b = near_index(sc, j)

        @pl.when(b < 4)
        def _():
            own[b, rows] = part

        @pl.when(b >= 4)
        def _():
            far[b - 4, rows] = part

    def part(first, size):
        dq = lax.dot_general(
            g[:, first : first + size], p[...], (((0,), (0,)), ((), ())), preferred_element_type=F32
        )
        return scale * dq

    for k in range(2):
        dq = part(4 * k * LOW, 4 * LOW)
        for j in range(4):
            put(4 * k + j, slice(0, LOW), dq[j * LOW : (j + 1) * LOW])
    dq = part(8 * LOW, 8 * UNIT)
    for j in range(8):
        put(j, slice(LOW, BLOCK), dq[j * UNIT : (j + 1) * UNIT])


def weight_parts(de_own, de_far, hidden, slope, rows, second, de, copies):
    half = de_own.shape[0]
    de[:half] = de_own[...]
    de[half:] = de_far[...]
    back = nt_dot(second[...], de[...])
    copies[0].wait()
    grad_second = jnp.dot(hidden[...], de[...], preferred_element_type=F32)
    copies[1].wait()
    dpre = (slope[...] * back).astype(BF16)
    copies[2].wait()
    grad_first = jnp.dot(dpre, rows[...], preferred_element_type=F32)
    return (grad_first, grad_second)


def weights_kernel(*refs):
    des, second, units, (out, de), held, sems = (
        refs[:4],
        refs[4],
        refs[5:11],
        refs[11:13],
        refs[13:19],
        refs[19],
    )
    copies = [
        pltpu.make_async_copy(unit, hold, sems.at[k])
        for k, (unit, hold) in enumerate(zip(units, held))
    ]
    for copy in copies:
        copy.start()
    first_q, second_q = weight_parts(*des[:2], *held[:3], second, de, copies[:3])
    grad_first, grad_second = weight_parts(*des[2:], *held[3:], second, de, copies[3:])
    grad_first += first_q
    grad_second += second_q
    many = out.shape[0]
    width = grad_first.shape[1]
    wide = width + grad_second.shape[1]
    out[:, :width] = grad_first[:many].astype(BF16)
    out[:, width:wide] = grad_second[:many].astype(BF16)
    rest = grad_first.shape[0] - many
    x = jnp.concatenate(
        [grad_first[many:], grad_second[many:], jnp.zeros((rest, 128), F32)], axis=1
    )
    near, far = x[:, :640], x[:, 640:]
    line = jnp.bitwise_and(lax.broadcasted_iota(jnp.int32, near.shape, 0), 7)
    even = jnp.where(line < 4, near, pltpu.roll(far, 4, 0)).astype(BF16)
    odd = jnp.where(line < 4, pltpu.roll(near, rest - 4, 0), far).astype(BF16)
    for b in range(rest // 8):
        out[b * 16 : b * 16 + 8, wide:] = even[b * 8 : (b + 1) * 8]
        out[b * 16 + 8 : b * 16 + 16, wide:] = odd[b * 8 : (b + 1) * 8]


VMEM = pl.BlockSpec(memory_space=pltpu.VMEM)
SMEM = pl.BlockSpec(memory_space=pltpu.SMEM)
HBM = pl.BlockSpec(memory_space=pltpu.HBM)


def pack_overflow(counts, where, q, p, pos):
    width = q.shape[1]
    half = pl.BlockSpec((LOW, width), lambda i: (1, 0))
    return pl.pallas_call(
        pack_kernel,
        grid=(1,),
        in_specs=[SMEM, SMEM, half, half, pl.BlockSpec((2, LOW), lambda i: (0, 0))],
        out_specs=[pl.BlockSpec((16, UNIT, 2 * width + LOW), lambda i: (0, 0, 0)), SMEM],
        out_shape=[
            jax.ShapeDtypeStruct((16, UNIT, 2 * width + LOW), BF16),
            jax.ShapeDtypeStruct((1,), jnp.int32),
        ],
        name="pack_overflow",
    )(counts, where, q, p, pos)


def base_rows(q, p, w_first, w_second):
    width, emb_width = w_first.shape[0], w_second.shape[1]
    rows = pl.BlockSpec((LOW, width), lambda i: (0, 0))

    def whole(shape):
        return pl.BlockSpec(shape, lambda i: (0, 0))

    shapes = [(LOW, emb_width), (LOW, emb_width), (2 * LOW, width)]
    return pl.pallas_call(
        base_kernel,
        grid=(1,),
        in_specs=[rows, rows, whole(w_first.shape), whole(w_second.shape)],
        out_specs=[whole(shape) for shape in shapes],
        out_shape=[jax.ShapeDtypeStruct(shape, BF16) for shape in shapes],
        name="base_rows",
    )(q, p, w_first, w_second)


def tail_rows(heavy_at, arrived, base_p, pos, w_first, w_second):
    emb_width = w_second.shape[1]
    return pl.pallas_call(
        tail_kernel,
        in_specs=[SMEM] + [VMEM] * 5,
        out_specs=[VMEM] * 2,
        out_shape=[
            jax.ShapeDtypeStruct((16, BLOCK, emb_width), BF16),
            jax.ShapeDtypeStruct((2 * UNIT, emb_width + w_first.shape[0]), BF16),
        ],
        name="tail_rows",
    )(heavy_at, arrived, base_p, pos, w_first, w_second)


def hidden_units(blocks, tails, first):
    rows = jax.ShapeDtypeStruct((8 * BLOCK, first.shape[1]), BF16)
    hidden = jax.ShapeDtypeStruct((first.shape[0], 8 * BLOCK), BF16)
    slope = jax.ShapeDtypeStruct((first.shape[0], 8 * BLOCK), F32)
    rows_q, rows_p, hidden_q, hidden_p, slope_q, slope_p = pl.pallas_call(
        units_kernel,
        in_specs=[VMEM] * 11,
        out_specs=[VMEM] * 6,
        out_shape=[rows, rows, hidden, hidden, slope, slope],
        name="hidden_units",
    )(*blocks, *tails, first)
    return ((hidden_q, slope_q, rows_q), (hidden_p, slope_p, rows_p))


def score_stats(sc, qs, ts, p, scale):
    width = p.shape[1]
    rows = 8 * BLOCK
    return pl.pallas_call(
        functools.partial(stats_kernel, scale=scale),
        in_specs=[SMEM] + [VMEM] * 5,
        out_specs=[VMEM] * 3,
        out_shape=[
            jax.ShapeDtypeStruct((rows, width), BF16),
            jax.ShapeDtypeStruct((1, rows), jnp.int32),
            jax.ShapeDtypeStruct((64, rows), F32),
        ],
        scratch_shapes=[pltpu.VMEM((8, LOW, width), BF16), pltpu.VMEM((8, 16, width), BF16)],
        name="score_stats",
    )(sc, *qs, *ts, p)


def score_grads(stats, q, p, place, scale):
    columns, width = p.shape
    rows = q.shape[0]
    steps = columns // PAIR
    return pl.pallas_call(
        functools.partial(grads_kernel, scale=scale),
        in_specs=[VMEM] * 4,
        out_specs=[HBM] * 2,
        out_shape=[
            jax.ShapeDtypeStruct((2 * steps * CHUNK, width), BF16),
            jax.ShapeDtypeStruct((columns, rows), BF16),
        ],
        scratch_shapes=[
            pltpu.VMEM((2 * steps * CHUNK, width), BF16),
            pltpu.VMEM((columns, rows), BF16),
            pltpu.SemaphoreType.DMA((2 * steps,)),
        ],
        name="score_grads",
    )(stats, q, p, place)


def query_grads(sc, p, g, scale):
    width = p.shape[1]
    return pl.pallas_call(
        functools.partial(query_kernel, scale=scale),
        in_specs=[SMEM, VMEM, VMEM],
        out_specs=[VMEM] * 2,
        out_shape=[jax.ShapeDtypeStruct((4, BLOCK, width), F32)] * 2,
        name="query_grads",
    )(sc, p, g)


def weight_grads(dqs, q_units, dps, p_units, second):
    held = [pltpu.VMEM(x.shape, x.dtype) for x in (*q_units, *p_units)]
    return pl.pallas_call(
        weights_kernel,
        in_specs=[VMEM] * 5 + [HBM] * 6,
        out_specs=VMEM,
        out_shape=jax.ShapeDtypeStruct((LOW, 1792), BF16),
        scratch_shapes=[pltpu.VMEM((8 * BLOCK, second.shape[1]), BF16)]
        + held
        + [pltpu.SemaphoreType.DMA((6,))],
        name="weight_grads",
    )(*dqs, *dps, second, *q_units, *p_units)


def body(query_features, passage_features, counts, positives, w_first, w_second):
    width = query_features.shape[1]
    hidden_width, emb_width = w_second.shape
    scale = 2.5 * emb_width ** (-0.5)
    group = lax.axis_index((LINE, CORE))
    pairs = BLOCK * lax.axis_size(DP)

    pos = positives.reshape(2, LOW)
    where = jnp.reshape(group, (1,)).astype(jnp.int32)
    over, heavy_at = pack_overflow(counts, where, query_features, passage_features, pos)
    over = over.reshape(16 * UNIT, -1)
    arrived = plane_exchange(over)

    q_base, p_base, feats = base_rows(query_features, passage_features, w_first, w_second)
    q_parts = along_line(q_base)

    feats = along_line(feats)
    feats = feats + [swap_core(x) for x in feats]

    p_send, q_tail = tail_rows(
        heavy_at, arrived.reshape(16, UNIT, -1), p_base, pos, w_first, w_second
    )
    p_all = plane_exchange(p_send.reshape(16 * BLOCK, emb_width))
    t_parts = along_line(q_tail)
    t_own = jnp.concatenate(t_parts, axis=0)
    ts = (t_own, swap_core(t_own))
    q_parts, _ = lax.optimization_barrier((q_parts, t_parts[1]))
    q_own = jnp.concatenate(q_parts, axis=0)
    qs = (q_own, swap_core(q_own))

    late_counts, group, _ = lax.optimization_barrier((counts, group, q_tail))
    heavy = (late_counts > LOW).astype(jnp.int32)
    devices = jnp.arange(counts.shape[0], dtype=jnp.int32)
    mine = heavy * (devices % 8 == group)
    offsets = jnp.cumsum(late_counts) - late_counts
    over_start = jnp.sum(mine * offsets) + LOW
    group_start = lax.dynamic_slice_in_dim(offsets.reshape(16, 8), group, 1, 1)[:, 0]
    scalars = [heavy_at[0], over_start, lax.axis_index(LINE), lax.axis_index(CORE)]
    scalars = jnp.stack(scalars + [lax.axis_index(PLANE)])
    heavies = jnp.sum(heavy.reshape(16, 8) * jnp.arange(16, dtype=jnp.int32)[:, None], axis=0)
    sc = jnp.concatenate([group_start, scalars, heavies]).astype(jnp.int32)

    each = hidden_width // lax.axis_size(DP)
    unit = jnp.arange(16 * each, dtype=jnp.int32)
    rest = unit - LOW
    unit_of = jnp.where(
        unit < LOW, (unit // 8) * (8 * each) + unit % 8, (rest // 4) * (8 * each) + 8 + rest % 4
    )
    unit_of = unit_of + group * each
    pick = (unit_of[:, None] == jnp.arange(hidden_width, dtype=jnp.int32)[None, :]).astype(BF16)
    first_part = lax.dot_general(
        pick, w_first, (((1,), (1,)), ((), ())), preferred_element_type=F32
    ).astype(BF16)
    second_part = jnp.dot(pick, w_second, preferred_element_type=F32).astype(BF16)
    p_all, first_part = lax.optimization_barrier((p_all, first_part))

    q_all, place, stats = score_stats(sc, qs, ts, p_all, scale)
    stats = stats_exchange(stats)
    q_units, p_units = hidden_units(feats, ts, first_part)
    dp_part, g = score_grads(stats, q_all, p_all, place, scale)
    dp_all = plane_exchange(dp_part)
    dq_own, dq_far = query_grads(sc, p_all, g, scale)

    dq = dq_own + swap_core(dq_far)
    dq_sum = dq[0].astype(BF16).astype(F32)
    arrived = [to_line(dq[k].astype(BF16), k) for k in (1, 2, 3)]
    for part in arrived:
        dq_sum = dq_sum + part.astype(F32)
    dqs = gathered(dq_sum.astype(BF16))

    dp_sum = jnp.sum(dp_all.reshape(16, CHUNK, emb_width).astype(F32), axis=0)
    mean_loss = (dp_sum[BLOCK, 0] + dp_sum[BLOCK + 1, 0] + dp_sum[BLOCK + 2, 0]) / pairs
    dps = gathered(dp_sum[:BLOCK].astype(BF16))
    grads = weight_grads(dqs, q_units, dps, p_units, second_part)
    out = jnp.sum(plane_exchange(grads).reshape(16, 8, -1).astype(F32), axis=0)
    wide = width + emb_width
    tail_out = jnp.concatenate([out[:4, wide:], out[4:, wide : 2 * wide - 640]], axis=1)
    out = jnp.concatenate([out[:, :wide], tail_out], axis=0)
    return (mean_loss, out[:, :width].T, out[:, width:])


def solution(mesh):
    finer = Mesh(mesh.devices.reshape(4, 4, 4, 2), DP)
    placed = (P(DP, None), P(DP, None), P(), P(DP), P(), P())
    return jax.shard_map(
        body,
        mesh=finer,
        in_specs=placed,
        out_specs=(P(), P(None, DP), P(DP, None)),
        check_vma=False,
    )
```
